256 devices in a mesh: expert: 32 (over x, y, z_hi), tok: 8 (over z_lo, core).
Axes of the slice: x: 4, y: 4, z: 8 (z_hi: 2, z_lo: 4; z = z_hi * 4 + z_lo), core: 2. Of those that a mesh axis runs over, the one named last changes fastest.
Arguments:
- tokens: bfloat16 [8192, 7168], P(('tok', 'expert')), may hold values from -6 to 6
- w_gate: bfloat16 [64, 7168, 1024], P('expert', None, 'tok'), may hold values from -0.0625 to 0.0625
- w_up: bfloat16 [64, 7168, 1024], P('expert', None, 'tok'), may hold values from -0.0625 to 0.0625
- w_down: bfloat16 [64, 1024, 7168], P('expert', 'tok'), may hold values from -0.1875 to 0.1875
- gates: float32 [8, 64, 32], replicated, may hold values from 0.2 to 1
- dispatch: int32 [8, 64, 32], replicated, may hold values from 0 to 1023, as said below
Outputs:
- combined: bfloat16 [8192, 7168], P(('tok', 'expert'))
The draws below stay inside these ranges and needn't reach their ends.
Inputs may be any that keep to these rules, and one draw needn't show every extreme that they name: `dispatch`: for each step and expert the 32 indices are different, and at most 2 of them lie in one aligned block of 32 indices (the rows of one device); in every step and for every expert some block holds exactly 2.
All inputs are finite; a program needn't handle non-finite values.
Results may differ from the reference program's by a relative error of at most 0.015.
Values may be sent and summed in bfloat16 or wider, within the bound.
A program may use at most 128 MiB of HBM per device.

```python
import jax
import jax.numpy as jnp
from jax import lax

D = 7168
HID = 1024
ROWS_DEV = 32
EXPERTS = 64
MOST = 2
CAP = 32
GROUP = 1024
STEPS = 8
TOKENS = 8192
N_TOK = 8


def expert_pick(key):
    sources = GROUP // ROWS_DEV
    total_slots = sources * MOST
    key_full, key_order, key_shuffle, key_rows = jax.random.split(key, 4)
    full_source = jax.random.randint(key_full, (), 0, sources)
    ranking = jax.random.permutation(key_order, total_slots)
    owner_of = jnp.arange(total_slots) // MOST
    scores = jnp.where(owner_of == full_source, ranking - total_slots, ranking)
    taken = jnp.argsort(scores)[:CAP]
    taken = taken[jax.random.permutation(key_shuffle, CAP)]
    source = taken // MOST
    within = taken % MOST
    noise = jax.random.randint(key_rows, (sources, ROWS_DEV), 0, 1 << 20) * ROWS_DEV + jnp.arange(ROWS_DEV)[None, :]
    row_order = jnp.argsort(noise, axis=1)
    return (source * ROWS_DEV + row_order[source, within]).astype(jnp.int32)


def draw_dispatch(key, part):
    keys = jax.random.split(jax.random.fold_in(key, 17), STEPS * EXPERTS)
    picks = jax.vmap(expert_pick)(keys)
    return picks.reshape(STEPS, EXPERTS, CAP)


def shard_levels(rng, shape, cuts, smallest, high):
    def one(dim, shards_of):
        steps = jax.random.uniform(jax.random.fold_in(jax.random.fold_in(rng, 6), dim), (shards_of,), jnp.float32, smallest / len(cuts), high / len(cuts))
        return jnp.repeat(jnp.exp(steps), shape[dim] // shards_of).reshape((-1,) + (1,) * (len(shape) - dim - 1))

    factor_of = one(*cuts[0])
    for cut in cuts[1:]:
        factor_of = factor_of * one(*cut)
    return factor_of


def normal_values(own_key, shape, width, bound, pieces=(), dtype=jnp.bfloat16):
    entries = width * jax.random.normal(own_key, shape, jnp.float32)
    if pieces:
        entries = entries * shard_levels(own_key, shape, pieces, -0.22, 0.18)
    return jnp.clip(entries, -bound, bound).astype(dtype)


def setup_inputs(seed: int = 0) -> dict:
    streams_of = jax.random.split(jax.random.key(seed), 7)
    tokens = normal_values(streams_of[0], (TOKENS, D), 1.0, 6.0, ((0, 256),))
    w_gate = normal_values(streams_of[1], (EXPERTS, D, HID), D ** -0.5, 0.0625, ((0, 32), (2, 8)))
    w_up = normal_values(streams_of[2], (EXPERTS, D, HID), D ** -0.5, 0.0625, ((0, 32), (2, 8)))
    w_down = normal_values(streams_of[3], (EXPERTS, HID, D), HID ** -0.5, 0.1875, ((0, 32), (1, 8)))
    gates = jnp.clip(jax.random.uniform(streams_of[4], (STEPS, EXPERTS, CAP), jnp.float32, 0.2, 1.0), 0.2, 1.0)
    dispatch = draw_dispatch(jax.random.fold_in(streams_of[6], 71), 0)
    return dict(tokens=tokens, w_gate=w_gate, w_up=w_up, w_down=w_down, gates=gates, dispatch=dispatch)


def reference(tokens, w_gate, w_up, w_down, gates, dispatch):
    shard_width = HID // N_TOK
    results = []
    for current in range(STEPS):
        group_rows = tokens[current * GROUP:(current + 1) * GROUP]

        def per_expert(packed):
            gate_mat, up_mat, down_mat, chosen, weight = packed
            picked = jnp.take(group_rows, chosen, axis=0)
            gate_pre = jnp.dot(picked, gate_mat, preferred_element_type=jnp.float32)
            up_pre = jnp.dot(picked, up_mat, preferred_element_type=jnp.float32)
            hidden = (jax.nn.silu(gate_pre) * up_pre).astype(jnp.bfloat16)
            hidden_f = hidden.astype(jnp.float32).reshape(CAP, N_TOK, shard_width)
            down_f = down_mat.astype(jnp.float32).reshape(N_TOK, shard_width, D)
            partials = jnp.einsum('cjh,jhd->jcd', hidden_f, down_f)
            partials = (partials * weight[None, :, None]).astype(jnp.bfloat16)
            return jnp.sum(partials.astype(jnp.float32), axis=0).astype(jnp.bfloat16)

        expert_out = lax.map(per_expert, (w_gate, w_up, w_down, dispatch[current], gates[current]))
        combined = jnp.zeros((GROUP, D), jnp.float32)
        combined = combined.at[dispatch[current].reshape(-1)].add(expert_out.reshape(-1, D).astype(jnp.float32))
        results.append(combined.astype(jnp.bfloat16))
    return jnp.concatenate(results, axis=0)
```

```python
import jax
import jax.numpy as jnp
from jax import lax
from jax.experimental import pallas as pl
from jax.experimental.pallas import tpu as pltpu
from jax.sharding import Mesh
from jax.sharding import PartitionSpec as P

NX, NY, NH, NL, NC = 4, 4, 2, 4, 2
NZ = NH * NL
COLS = NX * NY
D1 = 4096
SLOTS = 4
BF = jnp.bfloat16
F32 = jnp.float32
ANY = pl.BlockSpec(memory_space=pl.ANY)
VMEM = pl.BlockSpec(memory_space=pltpu.VMEM)
DMA = pltpu.SemaphoreType.DMA


def z_of(z):
    z = lax.rem(z + NZ, NZ)
    return {"zh": lax.div(z, NL), "zl": lax.rem(z, NL)}


def remote(src, dst, send, recv, device):
    return pltpu.make_async_remote_copy(
        src_ref=src, dst_ref=dst, send_sem=send, recv_sem=recv,
        device_id=device, device_id_type=pl.DeviceIdType.MESH)


def greet(devices):
    barrier = pltpu.get_barrier_semaphore()
    for device in devices:
        pl.semaphore_signal(barrier, inc=1, device_id=device, device_id_type=pl.DeviceIdType.MESH)
    pl.semaphore_wait(barrier, len(devices))


def xy_targets():
    x, y = lax.axis_index("x"), lax.axis_index("y")
    found = []
    for d in range(1, COLS):
        found.append((lax.rem(x + d // NY, NX), lax.rem(y + d % NY, NY)))
    return found


def xy_devices():
    return [{"x": tx, "y": ty} for tx, ty in xy_targets()]


def xy_copies(src, dst, send, recv):
    me = lax.axis_index("x") * NY + lax.axis_index("y")
    return [
        remote(src.at[tx * NY + ty], dst.at[me], send.at[d], recv.at[d], {"x": tx, "y": ty})
        for d, (tx, ty) in enumerate(xy_targets())
    ]


def my_z():
    return lax.axis_index("zh") * NL + lax.axis_index("zl")


def pair_kernel(own_ref, out_ref, relay, send, recv):
    z = my_z()
    rows, width = out_ref.shape
    half = rows // 2
    greet([z_of(z + 2), z_of(z - 2)])
    first = []
    for d, step in enumerate((2, -2)):
        part = pl.ds(d * half, half)
        copy = remote(own_ref.at[part, pl.ds(0, width)], relay.at[d], send.at[d], recv.at[d], z_of(z + step))
        copy.start()
        first.append(copy)
    second = []
    for d, step in enumerate((2, -2)):
        part = pl.ds(d * half, half)
        first[d].wait_recv()
        copy = remote(relay.at[d], out_ref.at[part], send.at[2 + d], recv.at[2 + d], z_of(z + step))
        copy.start()
        second.append(copy)
    for copy in first:
        copy.wait_send()
    for copy in second:
        copy.wait()


def pair_exchange(own, width, cid):
    rows = own.shape[0]
    return pl.pallas_call(
        pair_kernel,
        out_shape=jax.ShapeDtypeStruct((rows, width), BF),
        in_specs=[ANY], out_specs=ANY,
        scratch_shapes=[pltpu.VMEM((2, rows // 2, width), BF), DMA((4,)), DMA((4,))],
        compiler_params=pltpu.CompilerParams(collective_id=cid, has_side_effects=True),
        name="pair_exchange",
    )(own)


def ring_kernel(tok_ref, blk_ref, all_ref, got_ref, xs, xr, us, ur, ds, dr, ls):
    z = my_z()
    rows = tok_ref.shape[0]
    half = rows // 2
    width = all_ref.shape[2]
    start_col = tok_ref.shape[1] - width
    greet(xy_devices() + [z_of(z + 1), z_of(z - 1)])
    me = lax.axis_index("x") * NY + lax.axis_index("y")

    def hop(t, h, up):
        who = lax.rem(z + (-(t - 1) if up else t - 1) + NZ, NZ)
        part = pl.ds(h * half, half)
        if t == 1:
            src = tok_ref.at[part, pl.ds(start_col, width)]
        else:
            src = all_ref.at[who, part]
        send, recv = (us, ur) if up else (ds, dr)
        return remote(src, all_ref.at[who, part], send.at[t - 1, h], recv.at[t - 1, h], z_of(z + (1 if up else -1)))

    last = NZ // 2
    hops = [(t, h, up) for t in range(1, last + 1) for h in range(2) for up in (True, False)
            if t < last or (h == 0) == up]
    for t, h, up in hops:
        if t == 1:
            hop(t, h, up).start()
    blocks = xy_copies(blk_ref, got_ref, xs, xr)
    for copy in blocks:
        copy.start()
    own = [pltpu.make_async_copy(tok_ref.at[:, pl.ds(start_col, width)], all_ref.at[z], ls.at[0]),
           pltpu.make_async_copy(blk_ref.at[me], got_ref.at[me], ls.at[1])]
    for copy in own:
        copy.start()
    for t, h, up in hops:
        hop(t, h, up).wait_recv()
        if (t + 1, h, up) in hops:
            hop(t + 1, h, up).start()
    for t, h, up in hops:
        hop(t, h, up).wait_send()
    for copy in blocks:
        copy.wait()
    for copy in own:
        copy.wait()


def ring_and_plane(tokens, blocks, cid):
    rows = tokens.shape[0]
    width = tokens.shape[1] - D1
    return pl.pallas_call(
        ring_kernel,
        out_shape=(jax.ShapeDtypeStruct((NZ, rows, width), BF), jax.ShapeDtypeStruct(blocks.shape, BF)),
        in_specs=[ANY, ANY], out_specs=(ANY, ANY),
        scratch_shapes=[DMA((COLS - 1,)), DMA((COLS - 1,))] + [DMA((NZ // 2, 2))] * 4 + [DMA((2,))],
        compiler_params=pltpu.CompilerParams(collective_id=cid, has_side_effects=True),
        name="ring_and_plane",
    )(tokens, blocks)


def line_kernel(row_ref, blk_ref, wg_ref, wu_ref, wd_ref, all_ref, got_ref, og_ref, ou_ref, od_ref,
                xs, xr, us, ur, ds, dr, ws, wr, ls):
    zl = lax.axis_index("zl")
    experts = row_ref.shape[0]
    me = lax.axis_index("x") * NY + lax.axis_index("y")
    above, below = lax.rem(zl + 1, NL), lax.rem(zl + NL - 1, NL)
    other = {"c": 1 - lax.axis_index("c")}
    greet(xy_devices() + [{"zl": above}, {"zl": below}, other])

    def hop(i, e, up):
        who = lax.rem(zl + (-i if up else i) + NL, NL)
        src = row_ref.at[e] if i == 0 else all_ref.at[e, who]
        send, recv = (us, ur) if up else (ds, dr)
        return remote(src, all_ref.at[e, who], send.at[i, e], recv.at[i, e], {"zl": above if up else below})

    def sends(i, up):
        return (zl < NL - 1) & (zl >= i) if up else (zl > 0) & (zl + i < NL)

    def gets(i, up):
        return zl - 1 - i >= 0 if up else zl + 1 + i < NL

    for e in range(experts):
        for up in (True, False):
            @pl.when(sends(0, up))
            def _():
                hop(0, e, up).start()
    blocks = xy_copies(blk_ref, got_ref, xs, xr)
    for copy in blocks:
        copy.start()
    weights = [remote(a, b, ws.at[i], wr.at[i], other)
               for i, (a, b) in enumerate(((wg_ref, og_ref), (wu_ref, ou_ref), (wd_ref, od_ref)))]
    for copy in weights:
        copy.start()
    own = [pltpu.make_async_copy(row_ref.at[e], all_ref.at[e, zl], ls.at[e]) for e in range(experts)]
    own.append(pltpu.make_async_copy(blk_ref.at[me], got_ref.at[me], ls.at[experts]))
    for copy in own:
        copy.start()
    for i in range(NL - 1):
        for e in range(experts):
            for up in (True, False):
                @pl.when(gets(i, up))
                def _():
                    hop(i, e, up).wait_recv()
                if i < NL - 2:
                    @pl.when(sends(i + 1, up))
                    def _():
                        hop(i + 1, e, up).start()
    for i in range(NL - 1):
        for e in range(experts):
            for up in (True, False):
                @pl.when(sends(i, up))
                def _():
                    hop(i, e, up).wait_send()
    for copy in blocks + weights:
        copy.wait()
    for copy in own:
        copy.wait()


def line_and_plane(rows, blocks, w_gate, w_up, w_down, cid):
    experts, cap, width = rows.shape
    shapes = [(experts, NL, cap, width), blocks.shape, w_gate.shape, w_up.shape, w_down.shape]
    return pl.pallas_call(
        line_kernel,
        out_shape=tuple(jax.ShapeDtypeStruct(s, BF) for s in shapes),
        in_specs=[ANY] * 5, out_specs=(ANY,) * 5,
        scratch_shapes=[DMA((COLS - 1,)), DMA((COLS - 1,))] + [DMA((NL - 1, experts))] * 4
        + [DMA((3,)), DMA((3,)), DMA((experts + 1,))],
        compiler_params=pltpu.CompilerParams(collective_id=cid, has_side_effects=True),
        name="line_and_plane",
    )(rows, blocks, w_gate, w_up, w_down)


def add_into(dst, a, b, width, extra=None, chunk=512):
    @pl.loop(0, width // chunk)
    def _(i):
        part = pl.ds(pl.multiple_of(i * chunk, chunk), chunk)
        total = a[:, part].astype(F32) + b[:, part].astype(F32)
        if extra is not None:
            total = total + extra[:, part].astype(F32)
        dst[:, part] = total.astype(BF)


def line_sum_kernel(part_ref, blk_ref, out_ref, got_ref, ub, db, xs, xr, us, ur, ds, dr, ls):
    zl = lax.axis_index("zl")
    experts = part_ref.shape[0]
    width = part_ref.shape[3]
    me = lax.axis_index("x") * NY + lax.axis_index("y")
    above, below = lax.rem(zl + 1, NL), lax.rem(zl + NL - 1, NL)
    greet(xy_devices() + [{"zl": above}, {"zl": below}])

    def hop(j, e, up, fresh):
        buf = ub if up else db
        slot = j - 1 if up else j
        send, recv = (us, ur) if up else (ds, dr)
        src = part_ref.at[e, j] if fresh else buf.at[slot, e]
        return remote(src, buf.at[slot, e], send.at[slot, e], recv.at[slot, e], {"zl": above if up else below})

    order = [(NL - 1 - i, i) for i in range(NL - 1)]
    for ju, jd in order:
        for e in range(experts):
            @pl.when(zl == 0)
            def _():
                hop(ju, e, True, True).start()

            @pl.when(zl == NL - 1)
            def _():
                hop(jd, e, False, True).start()
    blocks = xy_copies(blk_ref, got_ref, xs, xr)
    for copy in blocks:
        copy.start()
    own = pltpu.make_async_copy(blk_ref.at[me], got_ref.at[me], ls)
    own.start()
    for ju, jd in order:
        for e in range(experts):
            for up, j in ((True, ju), (False, jd)):
                inner = (zl > 0) & (zl <= j) if up else (zl < NL - 1) & (zl >= j)
                passes = (zl > 0) & (zl < j) if up else (zl < NL - 1) & (zl > j)
                slot = j - 1 if up else j
                buf = ub if up else db

                @pl.when(inner)
                def _():
                    hop(j, e, up, False).wait_recv()

                @pl.when(passes)
                def _():
                    add_into(buf.at[slot, e], buf.at[slot, e], part_ref.at[e, j], width)
                    hop(j, e, up, False).start()
    for e in range(experts):
        @pl.when(zl == 0)
        def _():
            add_into(out_ref.at[e], part_ref.at[e, 0], db.at[0, e], width)

        @pl.when(zl == NL - 1)
        def _():
            add_into(out_ref.at[e], part_ref.at[e, NL - 1], ub.at[NL - 2, e], width)
        for mid in range(1, NL - 1):
            @pl.when(zl == mid)
            def _():
                add_into(out_ref.at[e], part_ref.at[e, mid], ub.at[mid - 1, e], width, db.at[mid, e])
    for ju, jd in order:
        for e in range(experts):
            @pl.when(zl < ju)
            def _():
                hop(ju, e, True, False).wait_send()

            @pl.when(zl > jd)
            def _():
                hop(jd, e, False, False).wait_send()
    for copy in blocks:
        copy.wait()
    own.wait()


def line_sum_and_plane(parts, blocks, cid):
    experts, _, cap, width = parts.shape
    buf = pltpu.VMEM((NL - 1, experts, cap, width), BF)
    return pl.pallas_call(
        line_sum_kernel,
        out_shape=(jax.ShapeDtypeStruct((experts, cap, width), BF), jax.ShapeDtypeStruct(blocks.shape, BF)),
        in_specs=[VMEM, ANY], out_specs=(VMEM, ANY),
        scratch_shapes=[buf, buf, DMA((COLS - 1,)), DMA((COLS - 1,))] + [DMA((NL - 1, experts))] * 4 + [DMA],
        compiler_params=pltpu.CompilerParams(collective_id=cid, has_side_effects=True),
        name="line_sum_and_plane",
    )(parts, blocks)


def ring_sum_kernel(part_ref, blk_ref, out_ref, got_ref, ub, db, xs, xr, us, ur, ds, dr, ls):
    z = my_z()
    rows, width = out_ref.shape
    half = rows // 2
    me = lax.axis_index("x") * NY + lax.axis_index("y")
    greet(xy_devices() + [z_of(z + 1), z_of(z - 1)])
    last = NZ // 2

    def spot(t, up):
        return lax.rem(z + (last - t if up else t - last) + NZ, NZ)

    def rows_of(h):
        return pl.ds(h * half, half)

    def hop(t, h, up, fresh):
        buf = ub if up else db
        send, recv = (us, ur) if up else (ds, dr)
        src = part_ref.at[spot(t, up), rows_of(h)] if fresh else buf.at[t - 1, h]
        return remote(src, buf.at[t, h], send.at[t, h], recv.at[t, h], z_of(z + (1 if up else -1)))

    def fresh_of(t, h, up):
        return t == 0 or (t == 1 and (h == 0) != up)

    hops = [(t, h, up) for t in range(last) for h in range(2) for up in (True, False)
            if t > 0 or (h == 0) == up]
    for t, h, up in hops:
        if fresh_of(t, h, up):
            hop(t, h, up, True).start()
    blocks = xy_copies(blk_ref, got_ref, xs, xr)
    for copy in blocks:
        copy.start()
    own = pltpu.make_async_copy(blk_ref.at[me], got_ref.at[me], ls)
    own.start()
    for t, h, up in hops:
        buf = ub if up else db
        hop(t, h, up, fresh_of(t, h, up)).wait_recv()
        if t < last - 1:
            add_into(buf.at[t, h], buf.at[t, h], part_ref.at[spot(t + 1, up), rows_of(h)], width)
            hop(t + 1, h, up, False).start()
    for h in range(2):
        add_into(out_ref.at[rows_of(h)], part_ref.at[z, rows_of(h)], ub.at[last - 1, h], width, db.at[last - 1, h])
    for t, h, up in hops:
        hop(t, h, up, fresh_of(t, h, up)).wait_send()
    for copy in blocks:
        copy.wait()
    own.wait()


def ring_sum_and_plane(parts, blocks, cid):
    _, rows, width = parts.shape
    buf = pltpu.VMEM((NZ // 2, 2, rows // 2, width), BF)
    return pl.pallas_call(
        ring_sum_kernel,
        out_shape=(jax.ShapeDtypeStruct((rows, width), BF), jax.ShapeDtypeStruct(blocks.shape, BF)),
        in_specs=[VMEM, ANY], out_specs=(VMEM, ANY),
        scratch_shapes=[buf, buf, DMA((COLS - 1,)), DMA((COLS - 1,))] + [DMA((NZ // 2, 2))] * 4 + [DMA],
        compiler_params=pltpu.CompilerParams(collective_id=cid, has_side_effects=True),
        name="ring_sum_and_plane",
    )(parts, blocks)


def mm(a, b, dtype=BF):
    return jnp.dot(a, b, preferred_element_type=F32).astype(dtype)


def body(tokens, w_gate, w_up, w_down, gates, dispatch):
    rows, width = tokens.shape
    experts = w_gate.shape[0]
    cap = dispatch.shape[-1]
    x, y, zh = lax.axis_index("x"), lax.axis_index("y"), lax.axis_index("zh")
    zl, c = lax.axis_index("zl"), lax.axis_index("c")
    col = x * NY + y
    span = NH * rows

    def of_parity(a):
        a = a.reshape(NL, NC, COLS, NH, experts, cap)
        a = lax.dynamic_index_in_dim(a, c, 1, keepdims=False)
        return lax.dynamic_index_in_dim(a, zh, 2, keepdims=False)

    picks = of_parity(dispatch)
    block = picks // span
    earlier = (block[..., :, None] == block[..., None, :]) & (jnp.arange(cap)[None, :] < jnp.arange(cap)[:, None])
    place = jnp.sum(earlier.astype(jnp.int32), axis=-1)

    here = jnp.where(block == col, (picks % span) * SLOTS + place, -1)
    table = here[..., None, None, :] == (jnp.arange(span)[None, :] * SLOTS + jnp.arange(SLOTS)[:, None])[..., None]
    table = jnp.any(table, axis=-1)
    pick1 = lax.dynamic_index_in_dim(table, zl, 0, keepdims=False)
    pick1 = pick1.reshape(COLS * experts * SLOTS, NH, rows).astype(BF)
    pick2 = table.transpose(1, 0, 2, 3, 4).reshape(COLS, NL, experts, SLOTS, NH, 1, rows)
    pick2 = pick2 & (jnp.arange(NL)[:, None, None, None, None, None] == jnp.arange(NL)[:, None])
    pick2 = pick2.reshape(COLS * NL * experts * SLOTS, NZ * rows).astype(BF)

    mine = lax.dynamic_index_in_dim(block * SLOTS + place, col, 1, keepdims=False)
    mine = mine.transpose(1, 0, 2)
    fit = mine[..., None] == jnp.arange(COLS * SLOTS)
    fit = fit.reshape(experts, NL, cap, COLS, SLOTS)
    fit1 = lax.dynamic_index_in_dim(fit, zl, 1, keepdims=False)
    same_e = jnp.eye(experts, dtype=bool)
    fit1 = fit1[:, :, :, None, :] & same_e[:, None, None, :, None]
    fit1 = fit1.reshape(experts * cap, COLS * experts * SLOTS).astype(BF)
    same_k = jnp.eye(NL, dtype=bool)
    fit2 = fit[:, :, :, :, None, None, :] & same_k[None, :, None, None, :, None, None] & same_e[:, None, None, None, None, :, None]
    fit2 = fit2.reshape(experts * NL * cap, COLS * NL * experts * SLOTS).astype(BF)
    weight = lax.dynamic_index_in_dim(of_parity(gates), col, 1, keepdims=False)
    weight = weight.transpose(1, 0, 2).reshape(experts, NL * cap, 1)

    other = pair_exchange(tokens, D1, 1)
    pick_own = lax.dynamic_index_in_dim(pick1, zh, 1, keepdims=False)
    pick_other = lax.dynamic_index_in_dim(pick1, 1 - zh, 1, keepdims=False)
    out1 = (mm(pick_own, tokens[:, :D1], F32) + mm(pick_other, other, F32)).astype(BF)
    everyone, got1 = ring_and_plane(tokens, out1.reshape(COLS, experts * SLOTS, D1), 2)
    rows1 = mm(fit1, got1.reshape(-1, D1)).reshape(experts, cap, D1)
    out2 = mm(pick2, everyone.reshape(NZ * rows, width - D1))
    lines, got2, og, ou, od = line_and_plane(
        rows1, out2.reshape(COLS, NL * experts * SLOTS, width - D1), w_gate, w_up, w_down, 3)
    x1 = lines.reshape(experts, NL * cap, D1)
    x2 = mm(fit2, got2.reshape(-1, width - D1)).reshape(experts, NL * cap, width - D1)
    chosen = jnp.concatenate([x1, x2], axis=2)

    def einsum(a, b):
        return jnp.einsum("eck,ekn->ecn", a, b, preferred_element_type=F32)

    down = 0.0
    for g, u, d in ((w_gate, w_up, w_down), (og, ou, od)):
        hidden = (jax.nn.silu(einsum(chosen, g)) * einsum(chosen, u)).astype(BF)
        down = down + einsum(hidden, d)
    partial = (down * weight).astype(BF)
    back1 = partial[:, :, :D1].reshape(experts, NL, cap, D1)
    back2 = mm(fit2.T, partial[:, :, D1:].reshape(experts * NL * cap, width - D1))
    summed, home2 = line_sum_and_plane(back1, back2.reshape(COLS, NL * experts * SLOTS, width - D1), 4)
    give1 = mm(fit1.T, summed.reshape(experts * cap, D1))
    sums2 = mm(pick2.T, home2.reshape(-1, width - D1)).reshape(NZ, rows, width - D1)
    final2, home1 = ring_sum_and_plane(sums2, give1.reshape(COLS, experts * SLOTS, D1), 5)
    home1 = home1.reshape(-1, D1)
    returned = pair_exchange(mm(pick_other.T, home1), D1, 6)
    final1 = (mm(pick_own.T, home1, F32) + returned.astype(F32)).astype(BF)
    return jnp.concatenate([final1, final2], axis=1)


def solution(mesh):
    split = Mesh(mesh.devices.reshape(NX, NY, NH, NL, NC), ("x", "y", "zh", "zl", "c"))
    expert, tok = ("x", "y", "zh"), ("zl", "c")
    in_specs = (P(tok + expert, None), P(expert, None, tok), P(expert, None, tok), P(expert, tok, None), P(), P())
    return jax.shard_map(body, mesh=split, in_specs=in_specs, out_specs=P(tok + expert, None), check_vma=False)
```

```python
import jax
import jax.numpy as jnp
from jax import lax
from jax.experimental import pallas as pl
from jax.experimental.pallas import tpu as pltpu
from jax.sharding import Mesh
from jax.sharding import PartitionSpec as P

NX, NY, NH, NL, NC = 4, 4, 2, 4, 2
NZ = NH * NL
COLS = NX * NY
D1 = 4096
SLOTS = 4
XY_ORDER = ((2, 2), (1, 1), (3, 3), (1, 3), (3, 1), (2, 1), (1, 2), (2, 3), (3, 2), (2, 0), (0, 2), (1, 0), (3, 0), (0, 1), (0, 3))
BF = jnp.bfloat16
F32 = jnp.float32
ANY = pl.BlockSpec(memory_space=pl.ANY)
VMEM = pl.BlockSpec(memory_space=pltpu.VMEM)
DMA = pltpu.SemaphoreType.DMA


def z_of(z):
    z = lax.rem(z + NZ, NZ)
    return {"zh": lax.div(z, NL), "zl": lax.rem(z, NL)}


def remote(src, dst, send, recv, device):
    return pltpu.make_async_remote_copy(
        src_ref=src, dst_ref=dst, send_sem=send, recv_sem=recv,
        device_id=device, device_id_type=pl.DeviceIdType.MESH)


def greet(devices):
    barrier = pltpu.get_barrier_semaphore()
    for device in devices:
        pl.semaphore_signal(barrier, inc=1, device_id=device, device_id_type=pl.DeviceIdType.MESH)
    pl.semaphore_wait(barrier, len(devices))


def xy_targets():
    x, y = lax.axis_index("x"), lax.axis_index("y")
    return [(lax.rem(x + dx, NX), lax.rem(y + dy, NY)) for dx, dy in XY_ORDER]


def xy_devices():
    return [{"x": tx, "y": ty} for tx, ty in xy_targets()]


def xy_copies(src, dst, send, recv):
    me = lax.axis_index("x") * NY + lax.axis_index("y")
    return [
        remote(src.at[tx * NY + ty], dst.at[me], send.at[d], recv.at[d], {"x": tx, "y": ty})
        for d, (tx, ty) in enumerate(xy_targets())
    ]


def my_z():
    return lax.axis_index("zh") * NL + lax.axis_index("zl")


def pair_kernel(own_ref, out_ref, relay, send, recv):
    z = my_z()
    rows, width = out_ref.shape
    half = rows // 2
    greet([z_of(z + 2), z_of(z - 2)])
    first = []
    for d, step in enumerate((2, -2)):
        part = pl.ds(d * half, half)
        copy = remote(own_ref.at[part, pl.ds(0, width)], relay.at[d], send.at[d], recv.at[d], z_of(z + step))
        copy.start()
        first.append(copy)
    second = []
    for d, step in enumerate((2, -2)):
        part = pl.ds(d * half, half)
        first[d].wait_recv()
        copy = remote(relay.at[d], out_ref.at[part], send.at[2 + d], recv.at[2 + d], z_of(z + step))
        copy.start()
        second.append(copy)
    for copy in first:
        copy.wait_send()
    for copy in second:
        copy.wait()


def pair_exchange(own, width, cid):
    rows = own.shape[0]
    return pl.pallas_call(
        pair_kernel,
        out_shape=jax.ShapeDtypeStruct((rows, width), BF),
        in_specs=[ANY], out_specs=ANY,
        scratch_shapes=[pltpu.VMEM((2, rows // 2, width), BF), DMA((4,)), DMA((4,))],
        compiler_params=pltpu.CompilerParams(collective_id=cid, has_side_effects=True),
        name="pair_exchange",
    )(own)


def sub(q, rows, width, first=0):
    half, wide = rows // 2, width // 2
    return pl.ds(q // 2 * half, half), pl.ds(first + q % 2 * wide, wide)


RING_HOPS = [(t, q, up) for t in range(NZ // 2) for q in range(4) for up in (True, False)]


def ring_kernel(tok_ref, blk_ref, all_ref, got_ref, xs, xr, us, ur, ds, dr, ls):
    z = my_z()
    _, rows, width = all_ref.shape
    start_col = tok_ref.shape[1] - width
    greet(xy_devices() + [z_of(z + 1), z_of(z - 1)])
    me = lax.axis_index("x") * NY + lax.axis_index("y")
    last = NZ // 2 - 1

    def hop(t, q, up):
        who = lax.rem(z + (-t if up else t) + NZ, NZ)
        r, c = sub(q, rows, width)
        src = tok_ref.at[sub(q, rows, width, start_col)] if t == 0 else all_ref.at[who, r, c]
        send, recv = (us, ur) if up else (ds, dr)
        return remote(src, all_ref.at[who, r, c], send.at[t, q], recv.at[t, q], z_of(z + (1 if up else -1)))

    hops = [(t, q, up) for t, q, up in RING_HOPS if t < last or (q < 2) == up]
    for t, q, up in hops:
        if t == 0:
            hop(t, q, up).start()
    blocks = xy_copies(blk_ref, got_ref, xs, xr)
    for copy in blocks:
        copy.start()
    own = pltpu.make_async_copy(blk_ref.at[me], got_ref.at[me], ls)
    own.start()
    all_ref[z] = tok_ref[:, start_col:]
    for t, q, up in hops:
        hop(t, q, up).wait_recv()
        if (t + 1, q, up) in hops:
            hop(t + 1, q, up).start()
    for t, q, up in hops:
        hop(t, q, up).wait_send()
    for copy in blocks:
        copy.wait()
    own.wait()


def ring_and_plane(tokens, blocks, cid):
    rows = tokens.shape[0]
    width = tokens.shape[1] - D1
    return pl.pallas_call(
        ring_kernel,
        out_shape=(jax.ShapeDtypeStruct((NZ, rows, width), BF), jax.ShapeDtypeStruct(blocks.shape, BF)),
        in_specs=[VMEM, ANY], out_specs=(VMEM, ANY),
        scratch_shapes=[DMA((COLS - 1,)), DMA((COLS - 1,))] + [DMA((NZ // 2, 4))] * 4 + [DMA],
        compiler_params=pltpu.CompilerParams(collective_id=cid, has_side_effects=True),
        name="ring_and_plane",
    )(tokens, blocks)


def line_kernel(row_ref, blk_ref, wg_ref, wu_ref, wd_ref, all_ref, got_ref, og_ref, ou_ref, od_ref,
                xs, xr, us, ur, ds, dr, ws, wr, ls):
    zl = lax.axis_index("zl")
    experts = row_ref.shape[0]
    me = lax.axis_index("x") * NY + lax.axis_index("y")
    above, below = lax.rem(zl + 1, NL), lax.rem(zl + NL - 1, NL)
    other = {"c": 1 - lax.axis_index("c")}
    greet(xy_devices() + [{"zl": above}, {"zl": below}, other])

    def hop(i, e, up):
        who = lax.rem(zl + (-i if up else i) + NL, NL)
        src = row_ref.at[e] if i == 0 else all_ref.at[e, who]
        send, recv = (us, ur) if up else (ds, dr)
        return remote(src, all_ref.at[e, who], send.at[i, e], recv.at[i, e], {"zl": above if up else below})

    def sends(i, up):
        return (zl < NL - 1) & (zl >= i) if up else (zl > 0) & (zl + i < NL)

    def gets(i, up):
        return zl - 1 - i >= 0 if up else zl + 1 + i < NL

    for e in range(experts):
        for up in (True, False):
            @pl.when(sends(0, up))
            def _():
                hop(0, e, up).start()
    blocks = xy_copies(blk_ref, got_ref, xs, xr)
    for copy in blocks:
        copy.start()
    weights = [remote(a, b, ws.at[i], wr.at[i], other)
               for i, (a, b) in enumerate(((wg_ref, og_ref), (wu_ref, ou_ref), (wd_ref, od_ref)))]
    for copy in weights:
        copy.start()
    own = [pltpu.make_async_copy(row_ref.at[e], all_ref.at[e, zl], ls.at[e]) for e in range(experts)]
    own.append(pltpu.make_async_copy(blk_ref.at[me], got_ref.at[me], ls.at[experts]))
    for copy in own:
        copy.start()
    for i in range(NL - 1):
        for e in range(experts):
            for up in (True, False):
                @pl.when(gets(i, up))
                def _():
                    hop(i, e, up).wait_recv()
                if i < NL - 2:
                    @pl.when(sends(i + 1, up))
                    def _():
                        hop(i + 1, e, up).start()
    for i in range(NL - 1):
        for e in range(experts):
            for up in (True, False):
                @pl.when(sends(i, up))
                def _():
                    hop(i, e, up).wait_send()
    for copy in blocks + weights:
        copy.wait()
    for copy in own:
        copy.wait()


def line_and_plane(rows, blocks, w_gate, w_up, w_down, cid):
    experts, cap, width = rows.shape
    shapes = [(experts, NL, cap, width), blocks.shape, w_gate.shape, w_up.shape, w_down.shape]
    return pl.pallas_call(
        line_kernel,
        out_shape=tuple(jax.ShapeDtypeStruct(s, BF) for s in shapes),
        in_specs=[ANY] * 5, out_specs=(ANY,) * 5,
        scratch_shapes=[DMA((COLS - 1,)), DMA((COLS - 1,))] + [DMA((NL - 1, experts))] * 4
        + [DMA((3,)), DMA((3,)), DMA((experts + 1,))],
        compiler_params=pltpu.CompilerParams(collective_id=cid, has_side_effects=True),
        name="line_and_plane",
    )(rows, blocks, w_gate, w_up, w_down)


def add_into(dst, a, b, width, extra=None, chunk=512):
    @pl.loop(0, width // chunk)
    def _(i):
        part = pl.ds(pl.multiple_of(i * chunk, chunk), chunk)
        total = a[:, part].astype(F32) + b[:, part].astype(F32)
        if extra is not None:
            total = total + extra[:, part].astype(F32)
        dst[:, part] = total.astype(BF)


def line_sum_kernel(part_ref, blk_ref, out_ref, got_ref, ub, db, xs, xr, us, ur, ds, dr, ls):
    zl = lax.axis_index("zl")
    experts = part_ref.shape[0]
    width = part_ref.shape[3]
    me = lax.axis_index("x") * NY + lax.axis_index("y")
    above, below = lax.rem(zl + 1, NL), lax.rem(zl + NL - 1, NL)
    greet(xy_devices() + [{"zl": above}, {"zl": below}])

    def hop(j, e, up, fresh):
        buf = ub if up else db
        slot = j - 1 if up else j
        send, recv = (us, ur) if up else (ds, dr)
        src = part_ref.at[e, j] if fresh else buf.at[slot, e]
        return remote(src, buf.at[slot, e], send.at[slot, e], recv.at[slot, e], {"zl": above if up else below})

    order = [(NL - 1 - i, i) for i in range(NL - 1)]
    blocks = xy_copies(blk_ref, got_ref, xs, xr)
    for copy in blocks:
        copy.start()
    own = pltpu.make_async_copy(blk_ref.at[me], got_ref.at[me], ls)
    own.start()
    edge = [(i, e) for i in range(NL - 1) for e in range(experts)]
    for up, home in ((True, 0), (False, NL - 1)):
        @pl.when(zl == home)
        def _():
            copies = [hop(NL - 1 - i if up else i, e, up, True) for i, e in edge]
            copies[0].start()
            copies[1].start()
            for n in range(2, len(copies)):
                copies[n - 2].wait_send()
                copies[n].start()
            copies[-2].wait_send()
            copies[-1].wait_send()

    def pass_on(j, e, up):
        slot = j - 1 if up else j
        buf = ub if up else db
        copy = hop(j, e, up, False)
        copy.wait_recv()
        add_into(buf.at[slot, e], buf.at[slot, e], part_ref.at[e, j], width)
        copy.start()

    for home, near in ((1, True), (2, False)):
        far, mid = (3, 2) if near else (0, 1)
        back = 0 if near else 3
        events = [(far, 0, near), (far, 1, near), (back, 0, not near), (mid, 0, near), (back, 1, not near), (mid, 1, near)]

        @pl.when(zl == home)
        def _():
            for event in events:
                pass_on(*event)
            for j, e, up in events:
                hop(j, e, up, False).wait_send()
    for ju, jd in order:
        for e in range(experts):
            @pl.when(zl == ju)
            def _():
                hop(ju, e, True, False).wait_recv()

            @pl.when(zl == jd)
            def _():
                hop(jd, e, False, False).wait_recv()
    for e in range(experts):
        @pl.when(zl == 0)
        def _():
            add_into(out_ref.at[e], part_ref.at[e, 0], db.at[0, e], width)

        @pl.when(zl == NL - 1)
        def _():
            add_into(out_ref.at[e], part_ref.at[e, NL - 1], ub.at[NL - 2, e], width)
        for mid in range(1, NL - 1):
            @pl.when(zl == mid)
            def _():
                add_into(out_ref.at[e], part_ref.at[e, mid], ub.at[mid - 1, e], width, db.at[mid, e])
    for copy in blocks:
        copy.wait()
    own.wait()


def line_sum_and_plane(parts, blocks, cid):
    experts, _, cap, width = parts.shape
    buf = pltpu.VMEM((NL - 1, experts, cap, width), BF)
    return pl.pallas_call(
        line_sum_kernel,
        out_shape=(jax.ShapeDtypeStruct((experts, cap, width), BF), jax.ShapeDtypeStruct(blocks.shape, BF)),
        in_specs=[VMEM, ANY], out_specs=(VMEM, ANY),
        scratch_shapes=[buf, buf, DMA((COLS - 1,)), DMA((COLS - 1,))] + [DMA((NL - 1, experts))] * 4 + [DMA],
        compiler_params=pltpu.CompilerParams(collective_id=cid, has_side_effects=True),
        name="line_sum_and_plane",
    )(parts, blocks)


def ring_sum_kernel(part_ref, blk_ref, out_ref, got_ref, ub, db, xs, xr, us, ur, ds, dr, ls):
    z = my_z()
    rows, width = out_ref.shape
    wide = width // 2
    me = lax.axis_index("x") * NY + lax.axis_index("y")
    greet(xy_devices() + [z_of(z + 1), z_of(z - 1)])
    last = NZ // 2

    def spot(t, up):
        return lax.rem(z + (last - t if up else t - last) + NZ, NZ)

    def hop(t, q, up, fresh):
        buf = ub if up else db
        send, recv = (us, ur) if up else (ds, dr)
        src = part_ref.at[(spot(t, up),) + sub(q, rows, width)] if fresh else buf.at[t - 1, q]
        return remote(src, buf.at[t, q], send.at[t, q], recv.at[t, q], z_of(z + (1 if up else -1)))

    def fresh_of(t, q, up):
        return t == 0 or (t == 1 and (q < 2) != up)

    hops = [(t, q, up) for t, q, up in RING_HOPS if t > 0 or (q < 2) == up]
    for t, q, up in hops:
        if fresh_of(t, q, up):
            hop(t, q, up, True).start()
    blocks = xy_copies(blk_ref, got_ref, xs, xr)
    for copy in blocks:
        copy.start()
    own = pltpu.make_async_copy(blk_ref.at[me], got_ref.at[me], ls)
    own.start()
    for t, q, up in hops:
        buf = ub if up else db
        hop(t, q, up, fresh_of(t, q, up)).wait_recv()
        if t < last - 1:
            add_into(buf.at[t, q], buf.at[t, q], part_ref.at[(spot(t + 1, up),) + sub(q, rows, width)], wide)
            hop(t + 1, q, up, False).start()
    for q in range(4):
        where = sub(q, rows, width)
        add_into(out_ref.at[where], part_ref.at[(z,) + where], ub.at[last - 1, q], wide, db.at[last - 1, q])
    for t, q, up in hops:
        hop(t, q, up, fresh_of(t, q, up)).wait_send()
    for copy in blocks:
        copy.wait()
    own.wait()


def ring_sum_and_plane(parts, blocks, cid):
    _, rows, width = parts.shape
    buf = pltpu.VMEM((NZ // 2, 4, rows // 2, width // 2), BF)
    return pl.pallas_call(
        ring_sum_kernel,
        out_shape=(jax.ShapeDtypeStruct((rows, width), BF), jax.ShapeDtypeStruct(blocks.shape, BF)),
        in_specs=[VMEM, ANY], out_specs=(VMEM, ANY),
        scratch_shapes=[buf, buf, DMA((COLS - 1,)), DMA((COLS - 1,))] + [DMA((NZ // 2, 4))] * 4 + [DMA],
        compiler_params=pltpu.CompilerParams(collective_id=cid, has_side_effects=True),
        name="ring_sum_and_plane",
    )(parts, blocks)


CHUNK = 1024
NEAR = D1 // CHUNK


def hidden_kernel(x1_ref, got_ref, fit_ref, g0_ref, g1_ref, u0_ref, u1_ref, h_ref, acc):
    d = pl.program_id(0)
    experts, rows, half = h_ref.shape

    @pl.when(d == 0)
    def _():
        acc[...] = jnp.zeros(acc.shape, F32)

    def add(e, x):
        both = jnp.concatenate([g0_ref[e], g1_ref[e], u0_ref[e], u1_ref[e]], axis=1)
        acc[e] += jnp.dot(x, both, preferred_element_type=F32)

    @pl.when(d < NEAR)
    def _():
        for e in range(experts):
            add(e, x1_ref[e])

    @pl.when(d >= NEAR)
    def _():
        for e in range(experts):
            fit = fit_ref[e * rows:(e + 1) * rows, :]
            add(e, jnp.dot(fit, got_ref[...], preferred_element_type=F32).astype(BF))

    @pl.when(d == pl.num_programs(0) - 1)
    def _():
        for e in range(experts):
            gate, up = acc[e, :, :half], acc[e, :, half:]
            h_ref[e] = (gate / (1.0 + jnp.exp(-gate)) * up).astype(BF)


def hidden_of(x1, got2, fit2, g0, g1, u0, u1):
    experts, rows, _ = x1.shape
    width, cols = g0.shape[1], g0.shape[2]
    weight = pl.BlockSpec((experts, CHUNK, cols), lambda d: (0, d, 0))
    return pl.pallas_call(
        hidden_kernel,
        grid=(width // CHUNK,),
        out_shape=jax.ShapeDtypeStruct((experts, rows, 2 * cols), BF),
        in_specs=[
            pl.BlockSpec((experts, rows, CHUNK), lambda d: (0, 0, jnp.minimum(d, NEAR - 1))),
            pl.BlockSpec((got2.shape[0], CHUNK), lambda d: (0, jnp.maximum(d - NEAR, 0))),
            pl.BlockSpec(fit2.shape, lambda d: (0, 0)),
            weight, weight, weight, weight],
        out_specs=pl.BlockSpec((experts, rows, 2 * cols), lambda d: (0, 0, 0)),
        scratch_shapes=[pltpu.VMEM((experts, rows, 4 * cols), F32)],
        compiler_params=pltpu.CompilerParams(dimension_semantics=("arbitrary",)),
        name="hidden_units",
    )(x1, got2, fit2, g0, g1, u0, u1)


def down_kernel(h_ref, fit_ref, wt_ref, d0_ref, d1_ref, near_ref, far_ref, padded, scale):
    d = pl.program_id(0)
    experts, rows, units = h_ref.shape
    turn = (((0,), (0,)), ((), ()))

    @pl.when(d == 0)
    def _():
        scale[...] = jnp.zeros(scale.shape, F32)
        for e in range(experts):
            fit = fit_ref[e * rows:(e + 1) * rows, :]
            placed = lax.dot_general(fit, h_ref[e], turn, preferred_element_type=F32)
            padded[:, e * units:(e + 1) * units] = placed.astype(BF)
            wide = jnp.broadcast_to(wt_ref[e], (rows, scale.shape[1]))
            scale[...] += lax.dot_general(fit.astype(F32), wide, turn, precision=lax.Precision.HIGHEST,
                                          preferred_element_type=F32)

    @pl.when(d < NEAR)
    def _():
        for e in range(experts):
            both = jnp.concatenate([d0_ref[e], d1_ref[e]], axis=0)
            y = jnp.dot(h_ref[e], both, preferred_element_type=F32)
            near_ref[e] = (y * wt_ref[e]).astype(BF)

    @pl.when(d >= NEAR)
    def _():
        both = jnp.concatenate([ref[e] for e in range(experts) for ref in (d0_ref, d1_ref)], axis=0)
        y = jnp.dot(padded[...], both, preferred_element_type=F32)
        far_ref[...] = (y * scale[:, :1]).astype(BF)


def down_of(hidden, fit2, weight, d0, d1):
    experts, rows, units = hidden.shape
    cols, width = d0.shape[1], d0.shape[2]
    slots = fit2.shape[1]
    mat = pl.BlockSpec((experts, cols, CHUNK), lambda d: (0, 0, d))
    return pl.pallas_call(
        down_kernel,
        grid=(width // CHUNK,),
        out_shape=(jax.ShapeDtypeStruct((experts, rows, D1), BF), jax.ShapeDtypeStruct((slots, width - D1), BF)),
        in_specs=[
            pl.BlockSpec(hidden.shape, lambda d: (0, 0, 0)),
            pl.BlockSpec(fit2.shape, lambda d: (0, 0)),
            pl.BlockSpec((experts, rows, 1), lambda d: (0, 0, 0)),
            mat, mat],
        out_specs=(
            pl.BlockSpec((experts, rows, CHUNK), lambda d: (0, 0, jnp.minimum(d, NEAR - 1))),
            pl.BlockSpec((slots, CHUNK), lambda d: (0, jnp.maximum(d - NEAR, 0)))),
        scratch_shapes=[pltpu.VMEM((slots, experts * units), BF), pltpu.VMEM((slots, 128), F32)],
        compiler_params=pltpu.CompilerParams(dimension_semantics=("arbitrary",)),
        name="down_units",
    )(hidden, fit2, weight, d0, d1)


def mm(a, b, dtype=BF):
    return jnp.dot(a, b, preferred_element_type=F32).astype(dtype)


def body(tokens, w_gate, w_up, w_down, gates, dispatch):
    rows, width = tokens.shape
    experts = w_gate.shape[0]
    cap = dispatch.shape[-1]
    x, y, zh = lax.axis_index("x"), lax.axis_index("y"), lax.axis_index("zh")
    zl, c = lax.axis_index("zl"), lax.axis_index("c")
    col = x * NY + y
    span = NH * rows

    def of_parity(a):
        a = a.reshape(NL, NC, COLS, NH, experts, cap)
        a = lax.dynamic_index_in_dim(a, c, 1, keepdims=False)
        return lax.dynamic_index_in_dim(a, zh, 2, keepdims=False)

    picks = of_parity(dispatch)
    block = picks // span
    earlier = (block[..., :, None] == block[..., None, :]) & (jnp.arange(cap)[None, :] < jnp.arange(cap)[:, None])
    place = jnp.sum(earlier.astype(jnp.int32), axis=-1)

    here = jnp.where(block == col, (picks % span) * SLOTS + place, -1)
    table = here[..., None, None, :] == (jnp.arange(span)[None, :] * SLOTS + jnp.arange(SLOTS)[:, None])[..., None]
    table = jnp.any(table, axis=-1)
    pick1 = lax.dynamic_index_in_dim(table, zl, 0, keepdims=False)
    pick1 = pick1.reshape(COLS * experts * SLOTS, NH, rows).astype(BF)
    pick2 = table.transpose(1, 0, 2, 3, 4).reshape(COLS, NL, experts, SLOTS, NH, 1, rows)
    pick2 = pick2 & (jnp.arange(NL)[:, None, None, None, None, None] == jnp.arange(NL)[:, None])
    pick2 = pick2.reshape(COLS * NL * experts * SLOTS, NZ * rows).astype(BF)

    mine = lax.dynamic_index_in_dim(block * SLOTS + place, col, 1, keepdims=False)
    mine = mine.transpose(1, 0, 2)
    fit = mine[..., None] == jnp.arange(COLS * SLOTS)
    fit = fit.reshape(experts, NL, cap, COLS, SLOTS)
    fit1 = lax.dynamic_index_in_dim(fit, zl, 1, keepdims=False)
    same_e = jnp.eye(experts, dtype=bool)
    fit1 = fit1[:, :, :, None, :] & same_e[:, None, None, :, None]
    fit1 = fit1.reshape(experts * cap, COLS * experts * SLOTS).astype(BF)
    same_k = jnp.eye(NL, dtype=bool)
    fit2 = fit[:, :, :, :, None, None, :] & same_k[None, :, None, None, :, None, None] & same_e[:, None, None, None, None, :, None]
    fit2 = fit2.reshape(experts * NL * cap, COLS * NL * experts * SLOTS).astype(BF)
    weight = lax.dynamic_index_in_dim(of_parity(gates), col, 1, keepdims=False)
    weight = weight.transpose(1, 0, 2).reshape(experts, NL * cap, 1)

    other = pair_exchange(tokens, D1, 1)
    pick_own = lax.dynamic_index_in_dim(pick1, zh, 1, keepdims=False)
    pick_other = lax.dynamic_index_in_dim(pick1, 1 - zh, 1, keepdims=False)
    out1 = (mm(pick_own, tokens[:, :D1], F32) + mm(pick_other, other, F32)).astype(BF)
    everyone, got1 = ring_and_plane(tokens, out1.reshape(COLS, experts * SLOTS, D1), 2)
    rows1 = mm(fit1, got1.reshape(-1, D1)).reshape(experts, cap, D1)
    out2 = mm(pick2, everyone.reshape(NZ * rows, width - D1))
    lines, got2, og, ou, od = line_and_plane(
        rows1, out2.reshape(COLS, NL * experts * SLOTS, width - D1), w_gate, w_up, w_down, 3)
    x1 = lines.reshape(experts, NL * cap, D1)
    hidden = hidden_of(x1, got2.reshape(-1, width - D1), fit2, w_gate, og, w_up, ou)
    back1, back2 = down_of(hidden, fit2, weight, w_down, od)
    back1 = back1.reshape(experts, NL, cap, D1)
    summed, home2 = line_sum_and_plane(back1, back2.reshape(COLS, NL * experts * SLOTS, width - D1), 4)
    give1 = mm(fit1.T, summed.reshape(experts * cap, D1))
    sums2 = mm(pick2.T, home2.reshape(-1, width - D1)).reshape(NZ, rows, width - D1)
    final2, home1 = ring_sum_and_plane(sums2, give1.reshape(COLS, experts * SLOTS, D1), 5)
    home1 = home1.reshape(-1, D1)
    returned = pair_exchange(mm(pick_other.T, home1), D1, 6)
    final1 = (mm(pick_own.T, home1, F32) + returned.astype(F32)).astype(BF)
    return jnp.concatenate([final1, final2], axis=1)


def solution(mesh):
    split = Mesh(mesh.devices.reshape(NX, NY, NH, NL, NC), ("x", "y", "zh", "zl", "c"))
    expert, tok = ("x", "y", "zh"), ("zl", "c")
    in_specs = (P(tok + expert, None), P(expert, None, tok), P(expert, None, tok), P(expert, tok, None), P(), P())
    return jax.shard_map(body, mesh=split, in_specs=in_specs, out_specs=P(tok + expert, None), check_vma=False)
```

```python
import jax
import jax.numpy as jnp
from jax import lax
from jax.experimental import pallas as pl
from jax.experimental.pallas import tpu as pltpu
from jax.sharding import Mesh
from jax.sharding import PartitionSpec as P

NX, NY, NH, NL, NC = 4, 4, 2, 4, 2
NZ = NH * NL
COLS = NX * NY
D1 = 4096
SLOTS = 4
CHUNK = 1024
NEAR = D1 // CHUNK
XY_ORDER = ((2, 2), (1, 1), (3, 3), (1, 3), (3, 1), (2, 1), (1, 2), (2, 3), (3, 2), (2, 0), (0, 2), (1, 0), (3, 0), (0, 1), (0, 3))
BF = jnp.bfloat16
F32 = jnp.float32
ANY = pl.BlockSpec(memory_space=pl.ANY)
VMEM = pl.BlockSpec(memory_space=pltpu.VMEM)
DMA = pltpu.SemaphoreType.DMA


def z_of(z):
    z = lax.rem(z + NZ, NZ)
    return {"zh": lax.div(z, NL), "zl": lax.rem(z, NL)}


def remote(src, dst, send, recv, device):
    return pltpu.make_async_remote_copy(
        src_ref=src, dst_ref=dst, send_sem=send, recv_sem=recv,
        device_id=device, device_id_type=pl.DeviceIdType.MESH)


def greet(devices):
    barrier = pltpu.get_barrier_semaphore()
    for device in devices:
        pl.semaphore_signal(barrier, inc=1, device_id=device, device_id_type=pl.DeviceIdType.MESH)
    pl.semaphore_wait(barrier, len(devices))


def xy_targets():
    x, y = lax.axis_index("x"), lax.axis_index("y")
    return [(lax.rem(x + dx, NX), lax.rem(y + dy, NY)) for dx, dy in XY_ORDER]


def xy_devices():
    return [{"x": tx, "y": ty} for tx, ty in xy_targets()]


def xy_copies(src, dst, send, recv):
    me = lax.axis_index("x") * NY + lax.axis_index("y")
    return [
        remote(src.at[tx * NY + ty], dst.at[me], send.at[d], recv.at[d], {"x": tx, "y": ty})
        for d, (tx, ty) in enumerate(xy_targets())
    ]


def my_z():
    return lax.axis_index("zh") * NL + lax.axis_index("zl")


def pair_steps(src, relay, dst, send, recv):
    z = my_z()
    half = relay.shape[1]
    first, second = [], []
    for d, step in enumerate((2, -2)):
        part = pl.ds(d * half, half)
        near = z_of(z + step)
        first.append(remote(src.at[part, pl.ds(0, relay.shape[2])], relay.at[d], send.at[d], recv.at[d], near))
        second.append(remote(relay.at[d], dst.at[part], send.at[2 + d], recv.at[2 + d], near))
    return first, second


def sub(q, rows, width, first=0):
    half, wide = rows // 2, width // 2
    return pl.ds(q // 2 * half, half), pl.ds(first + q % 2 * wide, wide)


RING_HOPS = [(t, q, up) for t in range(NZ // 2) for q in range(4) for up in (True, False)]


def head_kernel(tok_ref, mine_ref, theirs_ref, all_ref, got_ref, other, relay, block,
                xs, xr, us, ur, ds, dr, ps, pr, ls):
    z = my_z()
    _, rows, width = all_ref.shape
    cols, wide = block.shape[0], block.shape[2]
    start_col = tok_ref.shape[1] - width
    greet(xy_devices() + [z_of(z + 1), z_of(z - 1), z_of(z + 2), z_of(z - 2)])
    me = lax.axis_index("x") * NY + lax.axis_index("y")
    last = NZ // 2 - 1

    def hop(t, q, up):
        who = lax.rem(z + (-t if up else t) + NZ, NZ)
        r, c = sub(q, rows, width)
        src = tok_ref.at[sub(q, rows, width, start_col)] if t == 0 else all_ref.at[who, r, c]
        send, recv = (us, ur) if up else (ds, dr)
        return remote(src, all_ref.at[who, r, c], send.at[t, q], recv.at[t, q], z_of(z + (1 if up else -1)))

    hops = [(t, q, up) for t, q, up in RING_HOPS if t < last or (q < 2) == up]

    def serve(step):
        for t, q, up in hops:
            if t == step:
                hop(t, q, up).wait_recv()
                if (t + 1, q, up) in hops:
                    hop(t + 1, q, up).start()

    first, second = pair_steps(tok_ref, relay, other, ps, pr)
    for copy in first:
        copy.start()
    for t, q, up in hops:
        if t == 0:
            hop(t, q, up).start()
    all_ref[z] = tok_ref[:, start_col:]
    for d in range(2):
        first[d].wait_recv()
        second[d].start()
    serve(0)
    for copy in second:
        copy.wait_recv()

    @pl.loop(0, wide // CHUNK)
    def _(i):
        part = pl.ds(pl.multiple_of(i * CHUNK, CHUNK), CHUNK)
        y = jnp.dot(mine_ref[...], tok_ref[:, part], preferred_element_type=F32)
        y = y + jnp.dot(theirs_ref[...], other[:, part], preferred_element_type=F32)
        block[:, :, part] = y.reshape(cols, y.shape[0] // cols, CHUNK).astype(BF)

    blocks = xy_copies(block, got_ref, xs, xr)
    for copy in blocks:
        copy.start()
    own = pltpu.make_async_copy(block.at[me], got_ref.at[me], ls)
    own.start()
    for step in range(1, last + 1):
        serve(step)
    for t, q, up in hops:
        hop(t, q, up).wait_send()
    for copy in first + second:
        copy.wait_send()
    for copy in blocks:
        copy.wait()
    own.wait()


def head(tokens, mine, theirs, cid):
    rows = tokens.shape[0]
    width = tokens.shape[1] - D1
    block = (COLS, mine.shape[0] // COLS, D1)
    return pl.pallas_call(
        head_kernel,
        out_shape=(jax.ShapeDtypeStruct((NZ, rows, width), BF), jax.ShapeDtypeStruct(block, BF)),
        in_specs=[VMEM, VMEM, VMEM], out_specs=(VMEM, ANY),
        scratch_shapes=[pltpu.VMEM((rows, D1), BF), pltpu.VMEM((2, rows // 2, D1), BF), pltpu.VMEM(block, BF),
                        DMA((COLS - 1,)), DMA((COLS - 1,))] + [DMA((NZ // 2, 4))] * 4 + [DMA((4,)), DMA((4,)), DMA],
        compiler_params=pltpu.CompilerParams(collective_id=cid, has_side_effects=True),
        name="head",
    )(tokens, mine, theirs)


def line_kernel(row_ref, blk_ref, wg_ref, wu_ref, wd_ref, all_ref, got_ref, og_ref, ou_ref, od_ref,
                xs, xr, us, ur, ds, dr, ws, wr, ls):
    zl = lax.axis_index("zl")
    experts = row_ref.shape[0]
    me = lax.axis_index("x") * NY + lax.axis_index("y")
    above, below = lax.rem(zl + 1, NL), lax.rem(zl + NL - 1, NL)
    other = {"c": 1 - lax.axis_index("c")}
    greet(xy_devices() + [{"zl": above}, {"zl": below}, other])

    def hop(i, e, up):
        who = lax.rem(zl + (-i if up else i) + NL, NL)
        src = row_ref.at[e] if i == 0 else all_ref.at[e, who]
        send, recv = (us, ur) if up else (ds, dr)
        return remote(src, all_ref.at[e, who], send.at[i, e], recv.at[i, e], {"zl": above if up else below})

    def sends(i, up):
        return (zl < NL - 1) & (zl >= i) if up else (zl > 0) & (zl + i < NL)

    def gets(i, up):
        return zl - 1 - i >= 0 if up else zl + 1 + i < NL

    for e in range(experts):
        for up in (True, False):
            @pl.when(sends(0, up))
            def _():
                hop(0, e, up).start()
    blocks = xy_copies(blk_ref, got_ref, xs, xr)
    for copy in blocks:
        copy.start()
    weights = [remote(a, b, ws.at[i], wr.at[i], other)
               for i, (a, b) in enumerate(((wg_ref, og_ref), (wu_ref, ou_ref), (wd_ref, od_ref)))]
    for copy in weights:
        copy.start()
    own = [pltpu.make_async_copy(row_ref.at[e], all_ref.at[e, zl], ls.at[e]) for e in range(experts)]
    own.append(pltpu.make_async_copy(blk_ref.at[me], got_ref.at[me], ls.at[experts]))
    for copy in own:
        copy.start()
    for i in range(NL - 1):
        for e in range(experts):
            for up in (True, False):
                @pl.when(gets(i, up))
                def _():
                    hop(i, e, up).wait_recv()
                if i < NL - 2:
                    @pl.when(sends(i + 1, up))
                    def _():
                        hop(i + 1, e, up).start()
    for i in range(NL - 1):
        for e in range(experts):
            for up in (True, False):
                @pl.when(sends(i, up))
                def _():
                    hop(i, e, up).wait_send()
    for copy in blocks + weights:
        copy.wait()
    for copy in own:
        copy.wait()


def line_and_plane(rows, blocks, w_gate, w_up, w_down, cid):
    experts, cap, width = rows.shape
    shapes = [(experts, NL, cap, width), blocks.shape, w_gate.shape, w_up.shape, w_down.shape]
    return pl.pallas_call(
        line_kernel,
        out_shape=tuple(jax.ShapeDtypeStruct(s, BF) for s in shapes),
        in_specs=[ANY] * 5, out_specs=(ANY,) * 5,
        scratch_shapes=[DMA((COLS - 1,)), DMA((COLS - 1,))] + [DMA((NL - 1, experts))] * 4
        + [DMA((3,)), DMA((3,)), DMA((experts + 1,))],
        compiler_params=pltpu.CompilerParams(collective_id=cid, has_side_effects=True),
        name="line_and_plane",
    )(rows, blocks, w_gate, w_up, w_down)


def add_into(dst, a, b, width, extra=None, chunk=512):
    @pl.loop(0, width // chunk)
    def _(i):
        part = pl.ds(pl.multiple_of(i * chunk, chunk), chunk)
        total = a[:, part].astype(F32) + b[:, part].astype(F32)
        if extra is not None:
            total = total + extra[:, part].astype(F32)
        dst[:, part] = total.astype(BF)


def line_sum_kernel(part_ref, blk_ref, out_ref, got_ref, ub, db, xs, xr, us, ur, ds, dr, ls):
    zl = lax.axis_index("zl")
    experts = part_ref.shape[0]
    width = part_ref.shape[3]
    me = lax.axis_index("x") * NY + lax.axis_index("y")
    above, below = lax.rem(zl + 1, NL), lax.rem(zl + NL - 1, NL)
    greet(xy_devices() + [{"zl": above}, {"zl": below}])

    def hop(j, e, up, fresh):
        buf = ub if up else db
        slot = j - 1 if up else j
        send, recv = (us, ur) if up else (ds, dr)
        src = part_ref.at[e, j] if fresh else buf.at[slot, e]
        return remote(src, buf.at[slot, e], send.at[slot, e], recv.at[slot, e], {"zl": above if up else below})

    order = [(NL - 1 - i, i) for i in range(NL - 1)]
    blocks = xy_copies(blk_ref, got_ref, xs, xr)
    for copy in blocks:
        copy.start()
    own = pltpu.make_async_copy(blk_ref.at[me], got_ref.at[me], ls)
    own.start()
    edge = [(i, e) for i in range(NL - 1) for e in range(experts)]
    for up, home in ((True, 0), (False, NL - 1)):
        @pl.when(zl == home)
        def _():
            copies = [hop(NL - 1 - i if up else i, e, up, True) for i, e in edge]
            copies[0].start()
            copies[1].start()
            for n in range(2, len(copies)):
                copies[n - 2].wait_send()
                copies[n].start()
            copies[-2].wait_send()
            copies[-1].wait_send()

    def pass_on(j, e, up):
        slot = j - 1 if up else j
        buf = ub if up else db
        copy = hop(j, e, up, False)
        copy.wait_recv()
        add_into(buf.at[slot, e], buf.at[slot, e], part_ref.at[e, j], width)
        copy.start()

    for home, near in ((1, True), (2, False)):
        far, mid = (3, 2) if near else (0, 1)
        back = 0 if near else 3
        events = [(far, 0, near), (far, 1, near), (back, 0, not near), (mid, 0, near), (back, 1, not near), (mid, 1, near)]

        @pl.when(zl == home)
        def _():
            for event in events:
                pass_on(*event)
            for j, e, up in events:
                hop(j, e, up, False).wait_send()
    for ju, jd in order:
        for e in range(experts):
            @pl.when(zl == ju)
            def _():
                hop(ju, e, True, False).wait_recv()

            @pl.when(zl == jd)
            def _():
                hop(jd, e, False, False).wait_recv()
    for e in range(experts):
        @pl.when(zl == 0)
        def _():
            add_into(out_ref.at[e], part_ref.at[e, 0], db.at[0, e], width)

        @pl.when(zl == NL - 1)
        def _():
            add_into(out_ref.at[e], part_ref.at[e, NL - 1], ub.at[NL - 2, e], width)
        for mid in range(1, NL - 1):
            @pl.when(zl == mid)
            def _():
                add_into(out_ref.at[e], part_ref.at[e, mid], ub.at[mid - 1, e], width, db.at[mid, e])
    for copy in blocks:
        copy.wait()
    own.wait()


def line_sum_and_plane(parts, blocks, cid):
    experts, _, cap, width = parts.shape
    buf = pltpu.VMEM((NL - 1, experts, cap, width), BF)
    return pl.pallas_call(
        line_sum_kernel,
        out_shape=(jax.ShapeDtypeStruct((experts, cap, width), BF), jax.ShapeDtypeStruct(blocks.shape, BF)),
        in_specs=[VMEM, ANY], out_specs=(VMEM, ANY),
        scratch_shapes=[buf, buf, DMA((COLS - 1,)), DMA((COLS - 1,))] + [DMA((NL - 1, experts))] * 4 + [DMA],
        compiler_params=pltpu.CompilerParams(collective_id=cid, has_side_effects=True),
        name="line_sum_and_plane",
    )(parts, blocks)


def tail_kernel(part_ref, blk_ref, mine_ref, theirs_ref, out_ref, home, away, own, got, relay, ub, db,
                xs, xr, us, ur, ds, dr, ps, pr, ls):
    z = my_z()
    _, rows, width = part_ref.shape
    near = own.shape[1]
    wide = width // 2
    me = lax.axis_index("x") * NY + lax.axis_index("y")
    greet(xy_devices() + [z_of(z + 1), z_of(z - 1), z_of(z + 2), z_of(z - 2)])
    last = NZ // 2

    def spot(t, up):
        return lax.rem(z + (last - t if up else t - last) + NZ, NZ)

    def hop(t, q, up, fresh):
        buf = ub if up else db
        send, recv = (us, ur) if up else (ds, dr)
        src = part_ref.at[(spot(t, up),) + sub(q, rows, width)] if fresh else buf.at[t - 1, q]
        return remote(src, buf.at[t, q], send.at[t, q], recv.at[t, q], z_of(z + (1 if up else -1)))

    def fresh_of(t, q, up):
        return t == 0 or (t == 1 and (q < 2) != up)

    hops = [(t, q, up) for t, q, up in RING_HOPS if t > 0 or (q < 2) == up]

    def serve(step):
        for t, q, up in hops:
            if t == step:
                buf = ub if up else db
                hop(t, q, up, fresh_of(t, q, up)).wait_recv()
                if t < last - 1:
                    add_into(buf.at[t, q], buf.at[t, q], part_ref.at[(spot(t + 1, up),) + sub(q, rows, width)], wide)
                    hop(t + 1, q, up, False).start()

    for t, q, up in hops:
        if fresh_of(t, q, up):
            hop(t, q, up, True).start()
    blocks = xy_copies(blk_ref, home, xs, xr)
    for copy in blocks:
        copy.start()
    keep = pltpu.make_async_copy(blk_ref.at[me], home.at[me], ls)
    keep.start()
    serve(0)
    serve(1)
    for copy in blocks:
        copy.wait_recv()
    keep.wait()
    turn = (((0,), (0,)), ((), ()))

    @pl.loop(0, near // CHUNK)
    def _(i):
        part = pl.ds(pl.multiple_of(i * CHUNK, CHUNK), CHUNK)
        h = home[:, :, part].astype(F32).reshape(mine_ref.shape[0], CHUNK).astype(BF)
        away[:, part] = lax.dot_general(theirs_ref[...], h, turn, preferred_element_type=F32).astype(BF)
        own[:, part] = lax.dot_general(mine_ref[...], h, turn, preferred_element_type=F32)

    first, second = pair_steps(away, relay, got, ps, pr)
    for copy in first:
        copy.start()
    serve(2)
    for d in range(2):
        first[d].wait_recv()
        second[d].start()
    serve(3)
    for q in range(4):
        r, c = sub(q, rows, width)
        there = out_ref.at[sub(q, rows, width, near)]
        add_into(there, part_ref.at[z, r, c], ub.at[last - 1, q], wide, db.at[last - 1, q])
    for copy in second:
        copy.wait_recv()
    add_into(out_ref.at[:, pl.ds(0, near)], own, got, near)
    for t, q, up in hops:
        hop(t, q, up, fresh_of(t, q, up)).wait_send()
    for copy in first + second + blocks:
        copy.wait_send()


def tail(parts, blocks, mine, theirs, cid):
    _, rows, width = parts.shape
    near = blocks.shape[2]
    buf = pltpu.VMEM((NZ // 2, 4, rows // 2, width // 2), BF)
    return pl.pallas_call(
        tail_kernel,
        out_shape=jax.ShapeDtypeStruct((rows, near + width), BF),
        in_specs=[VMEM, ANY, VMEM, VMEM], out_specs=VMEM,
        scratch_shapes=[pltpu.VMEM(blocks.shape, BF), pltpu.VMEM((rows, near), BF), pltpu.VMEM((rows, near), F32),
                        pltpu.VMEM((rows, near), BF), pltpu.VMEM((2, rows // 2, near), BF), buf, buf,
                        DMA((COLS - 1,)), DMA((COLS - 1,))] + [DMA((NZ // 2, 4))] * 4 + [DMA((4,)), DMA((4,)), DMA],
        compiler_params=pltpu.CompilerParams(collective_id=cid, has_side_effects=True),
        name="tail",
    )(parts, blocks, mine, theirs)


def hidden_kernel(x1_ref, got_ref, fit_ref, g0_ref, g1_ref, u0_ref, u1_ref, h_ref, acc):
    d = pl.program_id(0)
    experts, rows, half = h_ref.shape

    @pl.when(d == 0)
    def _():
        acc[...] = jnp.zeros(acc.shape, F32)

    def add(e, x):
        both = jnp.concatenate([g0_ref[e], g1_ref[e], u0_ref[e], u1_ref[e]], axis=1)
        acc[e] += jnp.dot(x, both, preferred_element_type=F32)

    @pl.when(d < NEAR)
    def _():
        for e in range(experts):
            add(e, x1_ref[e])

    @pl.when(d >= NEAR)
    def _():
        for e in range(experts):
            fit = fit_ref[e * rows:(e + 1) * rows, :]
            add(e, jnp.dot(fit, got_ref[...], preferred_element_type=F32).astype(BF))

    @pl.when(d == pl.num_programs(0) - 1)
    def _():
        for e in range(experts):
            gate, up = acc[e, :, :half], acc[e, :, half:]
            h_ref[e] = (gate / (1.0 + jnp.exp(-gate)) * up).astype(BF)


def hidden_of(x1, got2, fit2, g0, g1, u0, u1):
    experts, rows, _ = x1.shape
    width, cols = g0.shape[1], g0.shape[2]
    weight = pl.BlockSpec((experts, CHUNK, cols), lambda d: (0, d, 0))
    return pl.pallas_call(
        hidden_kernel,
        grid=(width // CHUNK,),
        out_shape=jax.ShapeDtypeStruct((experts, rows, 2 * cols), BF),
        in_specs=[
            pl.BlockSpec((experts, rows, CHUNK), lambda d: (0, 0, jnp.minimum(d, NEAR - 1))),
            pl.BlockSpec((got2.shape[0], CHUNK), lambda d: (0, jnp.maximum(d - NEAR, 0))),
            pl.BlockSpec(fit2.shape, lambda d: (0, 0)),
            weight, weight, weight, weight],
        out_specs=pl.BlockSpec((experts, rows, 2 * cols), lambda d: (0, 0, 0)),
        scratch_shapes=[pltpu.VMEM((experts, rows, 4 * cols), F32)],
        compiler_params=pltpu.CompilerParams(dimension_semantics=("arbitrary",)),
        name="hidden_units",
    )(x1, got2, fit2, g0, g1, u0, u1)


def down_kernel(h_ref, fit_ref, wt_ref, d0_ref, d1_ref, near_ref, far_ref, padded, scale):
    d = pl.program_id(0)
    experts, rows, units = h_ref.shape
    turn = (((0,), (0,)), ((), ()))

    @pl.when(d == 0)
    def _():
        scale[...] = jnp.zeros(scale.shape, F32)
        for e in range(experts):
            fit = fit_ref[e * rows:(e + 1) * rows, :]
            placed = lax.dot_general(fit, h_ref[e], turn, preferred_element_type=F32)
            padded[:, e * units:(e + 1) * units] = placed.astype(BF)
            wide = jnp.broadcast_to(wt_ref[e], (rows, scale.shape[1]))
            scale[...] += lax.dot_general(fit.astype(F32), wide, turn, precision=lax.Precision.HIGHEST,
                                          preferred_element_type=F32)

    @pl.when(d < NEAR)
    def _():
        for e in range(experts):
            both = jnp.concatenate([d0_ref[e], d1_ref[e]], axis=0)
            y = jnp.dot(h_ref[e], both, preferred_element_type=F32)
            near_ref[e] = (y * wt_ref[e]).astype(BF)

    @pl.when(d >= NEAR)
    def _():
        both = jnp.concatenate([ref[e] for e in range(experts) for ref in (d0_ref, d1_ref)], axis=0)
        y = jnp.dot(padded[...], both, preferred_element_type=F32)
        far_ref[...] = (y * scale[:, :1]).astype(BF)


def down_of(hidden, fit2, weight, d0, d1):
    experts, rows, units = hidden.shape
    cols, width = d0.shape[1], d0.shape[2]
    slots = fit2.shape[1]
    mat = pl.BlockSpec((experts, cols, CHUNK), lambda d: (0, 0, d))
    return pl.pallas_call(
        down_kernel,
        grid=(width // CHUNK,),
        out_shape=(jax.ShapeDtypeStruct((experts, rows, D1), BF), jax.ShapeDtypeStruct((slots, width - D1), BF)),
        in_specs=[
            pl.BlockSpec(hidden.shape, lambda d: (0, 0, 0)),
            pl.BlockSpec(fit2.shape, lambda d: (0, 0)),
            pl.BlockSpec((experts, rows, 1), lambda d: (0, 0, 0)),
            mat, mat],
        out_specs=(
            pl.BlockSpec((experts, rows, CHUNK), lambda d: (0, 0, jnp.minimum(d, NEAR - 1))),
            pl.BlockSpec((slots, CHUNK), lambda d: (0, jnp.maximum(d - NEAR, 0)))),
        scratch_shapes=[pltpu.VMEM((slots, experts * units), BF), pltpu.VMEM((slots, 128), F32)],
        compiler_params=pltpu.CompilerParams(dimension_semantics=("arbitrary",)),
        name="down_units",
    )(hidden, fit2, weight, d0, d1)


def mm(a, b, dtype=BF):
    return jnp.dot(a, b, preferred_element_type=F32).astype(dtype)


def body(tokens, w_gate, w_up, w_down, gates, dispatch):
    rows, width = tokens.shape
    experts = w_gate.shape[0]
    cap = dispatch.shape[-1]
    x, y, zh = lax.axis_index("x"), lax.axis_index("y"), lax.axis_index("zh")
    zl, c = lax.axis_index("zl"), lax.axis_index("c")
    col = x * NY + y
    span = NH * rows

    def of_parity(a):
        a = a.reshape(NL, NC, COLS, NH, experts, cap)
        a = lax.dynamic_index_in_dim(a, c, 1, keepdims=False)
        return lax.dynamic_index_in_dim(a, zh, 2, keepdims=False)

    picks = of_parity(dispatch)
    block = picks // span
    earlier = (block[..., :, None] == block[..., None, :]) & (jnp.arange(cap)[None, :] < jnp.arange(cap)[:, None])
    place = jnp.sum(earlier.astype(jnp.int32), axis=-1)

    here = jnp.where(block == col, (picks % span) * SLOTS + place, -1)
    table = here[..., None, None, :] == (jnp.arange(span)[None, :] * SLOTS + jnp.arange(SLOTS)[:, None])[..., None]
    table = jnp.any(table, axis=-1)
    pick1 = lax.dynamic_index_in_dim(table, zl, 0, keepdims=False)
    pick1 = pick1.reshape(COLS * experts * SLOTS, NH, rows).astype(BF)
    pick2 = table.transpose(1, 0, 2, 3, 4).reshape(COLS, NL, experts, SLOTS, NH, 1, rows)
    pick2 = pick2 & (jnp.arange(NL)[:, None, None, None, None, None] == jnp.arange(NL)[:, None])
    pick2 = pick2.reshape(COLS * NL * experts * SLOTS, NZ * rows).astype(BF)

    mine = lax.dynamic_index_in_dim(block * SLOTS + place, col, 1, keepdims=False)
    mine = mine.transpose(1, 0, 2)
    fit = mine[..., None] == jnp.arange(COLS * SLOTS)
    fit = fit.reshape(experts, NL, cap, COLS, SLOTS)
    fit1 = lax.dynamic_index_in_dim(fit, zl, 1, keepdims=False)
    same_e = jnp.eye(experts, dtype=bool)
    fit1 = fit1[:, :, :, None, :] & same_e[:, None, None, :, None]
    fit1 = fit1.reshape(experts * cap, COLS * experts * SLOTS).astype(BF)
    same_k = jnp.eye(NL, dtype=bool)
    fit2 = fit[:, :, :, :, None, None, :] & same_k[None, :, None, None, :, None, None] & same_e[:, None, None, None, None, :, None]
    fit2 = fit2.reshape(experts * NL * cap, COLS * NL * experts * SLOTS).astype(BF)
    weight = lax.dynamic_index_in_dim(of_parity(gates), col, 1, keepdims=False)
    weight = weight.transpose(1, 0, 2).reshape(experts, NL * cap, 1)

    pick_own = lax.dynamic_index_in_dim(pick1, zh, 1, keepdims=False)
    pick_other = lax.dynamic_index_in_dim(pick1, 1 - zh, 1, keepdims=False)
    everyone, got1 = head(tokens, pick_own, pick_other, 1)
    rows1 = mm(fit1, got1.reshape(-1, D1)).reshape(experts, cap, D1)
    out2 = mm(pick2, everyone.reshape(NZ * rows, width - D1))
    lines, got2, og, ou, od = line_and_plane(
        rows1, out2.reshape(COLS, NL * experts * SLOTS, width - D1), w_gate, w_up, w_down, 3)
    x1 = lines.reshape(experts, NL * cap, D1)
    hidden = hidden_of(x1, got2.reshape(-1, width - D1), fit2, w_gate, og, w_up, ou)
    back1, back2 = down_of(hidden, fit2, weight, w_down, od)
    back1 = back1.reshape(experts, NL, cap, D1)
    summed, home2 = line_sum_and_plane(back1, back2.reshape(COLS, NL * experts * SLOTS, width - D1), 4)
    give1 = mm(fit1.T, summed.reshape(experts * cap, D1))
    sums2 = mm(pick2.T, home2.reshape(-1, width - D1)).reshape(NZ, rows, width - D1)
    return tail(sums2, give1.reshape(COLS, experts * SLOTS, D1), pick_own, pick_other, 2)


def solution(mesh):
    split = Mesh(mesh.devices.reshape(NX, NY, NH, NL, NC), ("x", "y", "zh", "zl", "c"))
    expert, tok = ("x", "y", "zh"), ("zl", "c")
    in_specs = (P(tok + expert, None), P(expert, None, tok), P(expert, None, tok), P(expert, tok, None), P(), P())
    return jax.shard_map(body, mesh=split, in_specs=in_specs, out_specs=P(tok + expert, None), check_vma=False)
```

```python
import jax
import jax.numpy as jnp
from jax import lax
from jax.experimental import pallas as pl
from jax.experimental.pallas import tpu as pltpu
from jax.sharding import Mesh
from jax.sharding import PartitionSpec as P

NX, NY, NH, NL, NC = 4, 4, 2, 4, 2
NZ = NH * NL
COLS = NX * NY
D1 = 4096
SLOTS = 4
CHUNK = 1024
HALF = 512
NEAR = D1 // CHUNK
XY_ORDER = ((2, 2), (1, 1), (3, 3), (1, 3), (3, 1), (2, 1), (1, 2), (2, 3), (3, 2), (2, 0), (0, 2), (1, 0), (3, 0), (0, 1), (0, 3))
BF = jnp.bfloat16
F32 = jnp.float32
ANY = pl.BlockSpec(memory_space=pl.ANY)
VMEM = pl.BlockSpec(memory_space=pltpu.VMEM)
DMA = pltpu.SemaphoreType.DMA


def z_of(z):
    z = lax.rem(z + NZ, NZ)
    return {"zh": lax.div(z, NL), "zl": lax.rem(z, NL)}


def remote(src, dst, send, recv, device):
    return pltpu.make_async_remote_copy(
        src_ref=src, dst_ref=dst, send_sem=send, recv_sem=recv,
        device_id=device, device_id_type=pl.DeviceIdType.MESH)


def greet(devices):
    barrier = pltpu.get_barrier_semaphore()
    for device in devices:
        pl.semaphore_signal(barrier, inc=1, device_id=device, device_id_type=pl.DeviceIdType.MESH)
    pl.semaphore_wait(barrier, len(devices))


def xy_targets():
    x, y = lax.axis_index("x"), lax.axis_index("y")
    return [(lax.rem(x + dx, NX), lax.rem(y + dy, NY)) for dx, dy in XY_ORDER]


def xy_devices():
    return [{"x": tx, "y": ty} for tx, ty in xy_targets()]


def xy_copies(src, dst, send, recv):
    me = lax.axis_index("x") * NY + lax.axis_index("y")
    return [
        remote(src.at[tx * NY + ty], dst.at[me], send.at[d], recv.at[d], {"x": tx, "y": ty})
        for d, (tx, ty) in enumerate(xy_targets())
    ]


def my_z():
    return lax.axis_index("zh") * NL + lax.axis_index("zl")


def pair_steps(src, relay, dst, send, recv):
    z = my_z()
    half = relay.shape[1]
    first, second = [], []
    for d, step in enumerate((2, -2)):
        part = pl.ds(d * half, half)
        near = z_of(z + step)
        first.append(remote(src.at[part, pl.ds(0, relay.shape[2])], relay.at[d], send.at[d], recv.at[d], near))
        second.append(remote(relay.at[d], dst.at[part], send.at[2 + d], recv.at[2 + d], near))
    return first, second


def sub(q, rows, width, first=0):
    half, wide = rows // 2, width // 2
    return pl.ds(q // 2 * half, half), pl.ds(first + q % 2 * wide, wide)


RING_HOPS = [(t, q, up) for t in range(NZ // 2) for q in range(4) for up in (True, False)]


def front_kernel(tok_ref, mine_ref, theirs_ref, pick_ref, fit_ref, wg_ref, wu_ref, wd_ref,
                 line_ref, got_ref, og_ref, ou_ref, od_ref,
                 ring, other, relay, block, home, far,
                 xs, xr, ys, yr, us, ur, ds, dr, ps, pr, lus, lur, lds, ldr, ws, wr, ls):
    z = my_z()
    zl = lax.axis_index("zl")
    experts = line_ref.shape[0]
    _, rows, width = ring.shape
    cols, wide = block.shape[0], block.shape[2]
    start_col = tok_ref.shape[1] - width
    core = {"c": 1 - lax.axis_index("c")}
    greet(xy_devices() + [z_of(z + 1), z_of(z - 1), z_of(z + 2), z_of(z - 2), core])
    me = lax.axis_index("x") * NY + lax.axis_index("y")
    last = NZ // 2 - 1

    def hop(t, q, up):
        who = lax.rem(z + (-t if up else t) + NZ, NZ)
        r, c = sub(q, rows, width)
        src = tok_ref.at[sub(q, rows, width, start_col)] if t == 0 else ring.at[who, r, c]
        send, recv = (us, ur) if up else (ds, dr)
        return remote(src, ring.at[who, r, c], send.at[t, q], recv.at[t, q], z_of(z + (1 if up else -1)))

    hops = [(t, q, up) for t, q, up in RING_HOPS if t < last or (q < 2) == up]

    def serve(step):
        for t, q, up in hops:
            if t == step:
                hop(t, q, up).wait_recv()
                if (t + 1, q, up) in hops:
                    hop(t + 1, q, up).start()

    def pass_on(i, e, up):
        who = lax.rem(zl + (-i if up else i) + NL, NL)
        send, recv = (lus, lur) if up else (lds, ldr)
        place = line_ref.at[e, who]
        return remote(place, place, send.at[i, e], recv.at[i, e], z_of(z + (1 if up else -1)))

    def sends(i, up):
        return (zl < NL - 1) & (zl >= i) if up else (zl > 0) & (zl + i < NL)

    def gets(i, up):
        return zl - 1 - i >= 0 if up else zl + 1 + i < NL

    first, second = pair_steps(tok_ref, relay, other, ps, pr)
    for copy in first:
        copy.start()
    for t, q, up in hops:
        if t == 0:
            hop(t, q, up).start()
    weights = [remote(a, b, ws.at[i], wr.at[i], core)
               for i, (a, b) in enumerate(((wg_ref, og_ref), (wu_ref, ou_ref), (wd_ref, od_ref)))]
    for copy in weights:
        copy.start()
    ring[z] = tok_ref[:, start_col:]
    for d in range(2):
        first[d].wait_recv()
        second[d].start()
    serve(0)
    for copy in second:
        copy.wait_recv()

    @pl.loop(0, wide // CHUNK)
    def _(i):
        part = pl.ds(pl.multiple_of(i * CHUNK, CHUNK), CHUNK)
        y = jnp.dot(mine_ref[...], tok_ref[:, part], preferred_element_type=F32)
        y = y + jnp.dot(theirs_ref[...], other[:, part], preferred_element_type=F32)
        block[:, :, part] = y.reshape(cols, y.shape[0] // cols, CHUNK).astype(BF)

    blocks = xy_copies(block, home, xs, xr)
    for copy in blocks:
        copy.start()
    home[me] = block[me]
    for step in range(1, last + 1):
        serve(step)
    for copy in blocks:
        copy.wait_recv()

    @pl.loop(0, wide // CHUNK)
    def _(i):
        part = pl.ds(pl.multiple_of(i * CHUNK, CHUNK), CHUNK)
        h = home[:, :, part].astype(F32).reshape(fit_ref.shape[1], CHUNK).astype(BF)
        y = jnp.dot(fit_ref[...], h, preferred_element_type=F32).astype(BF)
        cap = y.shape[0] // experts
        for e in range(experts):
            line_ref[e, zl, :, part] = y[e * cap:(e + 1) * cap]

    for e in range(experts):
        for up in (True, False):
            @pl.when(sends(0, up))
            def _():
                pass_on(0, e, up).start()

    @pl.loop(0, width // HALF)
    def _(i):
        part = pl.ds(pl.multiple_of(i * HALF, HALF), HALF)
        every = ring[:, :, part].reshape(NZ * rows, HALF)
        y = jnp.dot(pick_ref[...], every, preferred_element_type=F32)
        far[:, :, part] = y.reshape(cols, y.shape[0] // cols, HALF).astype(BF)

    fars = xy_copies(far, got_ref, ys, yr)
    for copy in fars:
        copy.start()
    own = pltpu.make_async_copy(far.at[me], got_ref.at[me], ls)
    own.start()
    for i in range(NL - 1):
        for e in range(experts):
            for up in (True, False):
                @pl.when(gets(i, up))
                def _():
                    pass_on(i, e, up).wait_recv()
                if i < NL - 2:
                    @pl.when(sends(i + 1, up))
                    def _():
                        pass_on(i + 1, e, up).start()
    for i in range(NL - 1):
        for e in range(experts):
            for up in (True, False):
                @pl.when(sends(i, up))
                def _():
                    pass_on(i, e, up).wait_send()
    for t, q, up in hops:
        hop(t, q, up).wait_send()
    for copy in first + second + blocks:
        copy.wait_send()
    for copy in fars + weights:
        copy.wait()
    own.wait()


def front(tokens, mine, theirs, pick2, fit1, w_gate, w_up, w_down, cid):
    rows = tokens.shape[0]
    width = tokens.shape[1] - D1
    experts = w_gate.shape[0]
    cap = fit1.shape[0] // experts
    block = (COLS, mine.shape[0] // COLS, D1)
    far = (COLS, pick2.shape[0] // COLS, width)
    shapes = [(experts, NL, cap, D1), far, w_gate.shape, w_up.shape, w_down.shape]
    plane = DMA((COLS - 1,))
    return pl.pallas_call(
        front_kernel,
        out_shape=tuple(jax.ShapeDtypeStruct(shape, BF) for shape in shapes),
        in_specs=[VMEM] * 5 + [ANY] * 3, out_specs=(VMEM, ANY, ANY, ANY, ANY),
        scratch_shapes=[pltpu.VMEM((NZ, rows, width), BF), pltpu.VMEM((rows, D1), BF),
                        pltpu.VMEM((2, rows // 2, D1), BF), pltpu.VMEM(block, BF), pltpu.VMEM(block, BF),
                        pltpu.VMEM(far, BF), plane, plane, plane, plane]
        + [DMA((NZ // 2, 4))] * 4 + [DMA((4,))] * 2 + [DMA((NL - 1, experts))] * 4 + [DMA((3,))] * 2 + [DMA],
        compiler_params=pltpu.CompilerParams(collective_id=cid, has_side_effects=True),
        name="front",
    )(tokens, mine, theirs, pick2, fit1, w_gate, w_up, w_down)


def add_into(dst, a, b, width, extra=None, chunk=512):
    @pl.loop(0, width // chunk)
    def _(i):
        part = pl.ds(pl.multiple_of(i * chunk, chunk), chunk)
        total = a[:, part].astype(F32) + b[:, part].astype(F32)
        if extra is not None:
            total = total + extra[:, part].astype(F32)
        dst[:, part] = total.astype(BF)


def back_kernel(line_ref, far_ref, mine_ref, theirs_ref, pick_ref, fit_ref, out_ref,
                lu, ld, summed, got2, part_ref, block, home, away, own, got, relay, ub, db,
                xs, xr, ys, yr, us, ur, ds, dr, ps, pr, lus, lur, lds, ldr, ls):
    z = my_z()
    zl = lax.axis_index("zl")
    experts = line_ref.shape[0]
    near = line_ref.shape[3]
    _, rows, width = part_ref.shape
    wide = width // 2
    cols = block.shape[0]
    me = lax.axis_index("x") * NY + lax.axis_index("y")
    greet(xy_devices() + [z_of(z + 1), z_of(z - 1), z_of(z + 2), z_of(z - 2)])
    last = NZ // 2
    turn = (((0,), (0,)), ((), ()))

    def send_sum(j, e, up, fresh):
        buf = lu if up else ld
        slot = j - 1 if up else j
        send, recv = (lus, lur) if up else (lds, ldr)
        src = line_ref.at[e, j] if fresh else buf.at[slot, e]
        return remote(src, buf.at[slot, e], send.at[slot, e], recv.at[slot, e], z_of(z + (1 if up else -1)))

    order = [(NL - 1 - i, i) for i in range(NL - 1)]
    fars = xy_copies(far_ref, got2, ys, yr)
    for copy in fars:
        copy.start()
    keep = pltpu.make_async_copy(far_ref.at[me], got2.at[me], ls)
    keep.start()
    edge = [(i, e) for i in range(NL - 1) for e in range(experts)]
    for up, seat in ((True, 0), (False, NL - 1)):
        @pl.when(zl == seat)
        def _():
            copies = [send_sum(NL - 1 - i if up else i, e, up, True) for i, e in edge]
            copies[0].start()
            copies[1].start()
            for n in range(2, len(copies)):
                copies[n - 2].wait_send()
                copies[n].start()
            copies[-2].wait_send()
            copies[-1].wait_send()

    def pass_on(j, e, up):
        slot = j - 1 if up else j
        buf = lu if up else ld
        copy = send_sum(j, e, up, False)
        copy.wait_recv()
        add_into(buf.at[slot, e], buf.at[slot, e], line_ref.at[e, j], near)
        copy.start()

    for seat, up in ((1, True), (2, False)):
        end, inner, start = (3, 2, 0) if up else (0, 1, 3)
        events = [(end, 0, up), (end, 1, up), (start, 0, not up), (inner, 0, up), (start, 1, not up), (inner, 1, up)]

        @pl.when(zl == seat)
        def _():
            for event in events:
                pass_on(*event)
            for j, e, up in events:
                send_sum(j, e, up, False).wait_send()
    for ju, jd in order:
        for e in range(experts):
            @pl.when(zl == ju)
            def _():
                send_sum(ju, e, True, False).wait_recv()

            @pl.when(zl == jd)
            def _():
                send_sum(jd, e, False, False).wait_recv()
    for e in range(experts):
        @pl.when(zl == 0)
        def _():
            add_into(summed.at[e], line_ref.at[e, 0], ld.at[0, e], near)

        @pl.when(zl == NL - 1)
        def _():
            add_into(summed.at[e], line_ref.at[e, NL - 1], lu.at[NL - 2, e], near)
        for mid in range(1, NL - 1):
            @pl.when(zl == mid)
            def _():
                add_into(summed.at[e], line_ref.at[e, mid], lu.at[mid - 1, e], near, ld.at[mid, e])

    @pl.loop(0, near // CHUNK)
    def _(i):
        part = pl.ds(pl.multiple_of(i * CHUNK, CHUNK), CHUNK)
        y = lax.dot_general(fit_ref[...], summed[:, :, part].reshape(fit_ref.shape[0], CHUNK), turn,
                            preferred_element_type=F32)
        block[:, :, part] = y.reshape(cols, y.shape[0] // cols, CHUNK).astype(BF)

    blocks = xy_copies(block, home, xs, xr)
    for copy in blocks:
        copy.start()
    home[me] = block[me]
    for copy in fars:
        copy.wait_recv()
    keep.wait()

    @pl.loop(0, width // HALF)
    def _(i):
        part = pl.ds(pl.multiple_of(i * HALF, HALF), HALF)
        h = got2[:, :, part].reshape(pick_ref.shape[0], HALF)
        y = lax.dot_general(pick_ref[...], h, turn, preferred_element_type=F32)
        part_ref[:, :, part] = y.reshape(NZ, rows, HALF).astype(BF)

    def spot(t, up):
        return lax.rem(z + (last - t if up else t - last) + NZ, NZ)

    def hop(t, q, up, fresh):
        buf = ub if up else db
        send, recv = (us, ur) if up else (ds, dr)
        src = part_ref.at[(spot(t, up),) + sub(q, rows, width)] if fresh else buf.at[t - 1, q]
        return remote(src, buf.at[t, q], send.at[t, q], recv.at[t, q], z_of(z + (1 if up else -1)))

    def fresh_of(t, q, up):
        return t == 0 or (t == 1 and (q < 2) != up)

    hops = [(t, q, up) for t, q, up in RING_HOPS if t > 0 or (q < 2) == up]

    def serve(step):
        for t, q, up in hops:
            if t == step:
                buf = ub if up else db
                hop(t, q, up, fresh_of(t, q, up)).wait_recv()
                if t < last - 1:
                    add_into(buf.at[t, q], buf.at[t, q], part_ref.at[(spot(t + 1, up),) + sub(q, rows, width)], wide)
                    hop(t + 1, q, up, False).start()

    for t, q, up in hops:
        if fresh_of(t, q, up):
            hop(t, q, up, True).start()
    serve(0)
    serve(1)
    for copy in blocks:
        copy.wait_recv()

    @pl.loop(0, near // CHUNK)
    def _(i):
        part = pl.ds(pl.multiple_of(i * CHUNK, CHUNK), CHUNK)
        h = home[:, :, part].astype(F32).reshape(mine_ref.shape[0], CHUNK).astype(BF)
        away[:, part] = lax.dot_general(theirs_ref[...], h, turn, preferred_element_type=F32).astype(BF)
        own[:, part] = lax.dot_general(mine_ref[...], h, turn, preferred_element_type=F32)

    first, second = pair_steps(away, relay, got, ps, pr)
    for copy in first:
        copy.start()
    serve(2)
    for d in range(2):
        first[d].wait_recv()
        second[d].start()
    serve(3)
    for q in range(4):
        r, c = sub(q, rows, width)
        there = out_ref.at[sub(q, rows, width, near)]
        add_into(there, part_ref.at[z, r, c], ub.at[last - 1, q], wide, db.at[last - 1, q])
    for copy in second:
        copy.wait_recv()
    add_into(out_ref.at[:, pl.ds(0, near)], own, got, near)
    for t, q, up in hops:
        hop(t, q, up, fresh_of(t, q, up)).wait_send()
    for copy in first + second + blocks + fars:
        copy.wait_send()


def back(lines, fars, mine, theirs, pick2, fit1, cid):
    experts, _, cap, near = lines.shape
    width = fars.shape[2]
    rows = mine.shape[1]
    block = (COLS, mine.shape[0] // COLS, near)
    buf = pltpu.VMEM((NZ // 2, 4, rows // 2, width // 2), BF)
    line = pltpu.VMEM((NL - 1, experts, cap, near), BF)
    plane = DMA((COLS - 1,))
    return pl.pallas_call(
        back_kernel,
        out_shape=jax.ShapeDtypeStruct((rows, near + width), BF),
        in_specs=[VMEM, ANY, VMEM, VMEM, VMEM, VMEM], out_specs=VMEM,
        scratch_shapes=[line, line, pltpu.VMEM((experts, cap, near), BF), pltpu.VMEM(fars.shape, BF),
                        pltpu.VMEM((NZ, rows, width), BF), pltpu.VMEM(block, BF), pltpu.VMEM(block, BF),
                        pltpu.VMEM((rows, near), BF), pltpu.VMEM((rows, near), F32), pltpu.VMEM((rows, near), BF),
                        pltpu.VMEM((2, rows // 2, near), BF), buf, buf, plane, plane, plane, plane]
        + [DMA((NZ // 2, 4))] * 4 + [DMA((4,))] * 2 + [DMA((NL - 1, experts))] * 4 + [DMA],
        compiler_params=pltpu.CompilerParams(collective_id=cid, has_side_effects=True),
        name="back",
    )(lines, fars, mine, theirs, pick2, fit1)


def hidden_kernel(x1_ref, got_ref, fit_ref, g0_ref, g1_ref, u0_ref, u1_ref, h_ref, acc):
    d = pl.program_id(0)
    experts, rows, half = h_ref.shape

    @pl.when(d == 0)
    def _():
        acc[...] = jnp.zeros(acc.shape, F32)

    def add(e, x):
        both = jnp.concatenate([g0_ref[e], g1_ref[e], u0_ref[e], u1_ref[e]], axis=1)
        acc[e] += jnp.dot(x, both, preferred_element_type=F32)

    @pl.when(d < NEAR)
    def _():
        for e in range(experts):
            add(e, x1_ref[e])

    @pl.when(d >= NEAR)
    def _():
        for e in range(experts):
            fit = fit_ref[e * rows:(e + 1) * rows, :]
            add(e, jnp.dot(fit, got_ref[...], preferred_element_type=F32).astype(BF))

    @pl.when(d == pl.num_programs(0) - 1)
    def _():
        for e in range(experts):
            gate, up = acc[e, :, :half], acc[e, :, half:]
            h_ref[e] = (gate / (1.0 + jnp.exp(-gate)) * up).astype(BF)


def hidden_of(x1, got2, fit2, g0, g1, u0, u1):
    experts, rows, _ = x1.shape
    width, cols = g0.shape[1], g0.shape[2]
    weight = pl.BlockSpec((experts, CHUNK, cols), lambda d: (0, d, 0))
    return pl.pallas_call(
        hidden_kernel,
        grid=(width // CHUNK,),
        out_shape=jax.ShapeDtypeStruct((experts, rows, 2 * cols), BF),
        in_specs=[
            pl.BlockSpec((experts, rows, CHUNK), lambda d: (0, 0, jnp.minimum(d, NEAR - 1))),
            pl.BlockSpec((got2.shape[0], CHUNK), lambda d: (0, jnp.maximum(d - NEAR, 0))),
            pl.BlockSpec(fit2.shape, lambda d: (0, 0)),
            weight, weight, weight, weight],
        out_specs=pl.BlockSpec((experts, rows, 2 * cols), lambda d: (0, 0, 0)),
        scratch_shapes=[pltpu.VMEM((experts, rows, 4 * cols), F32)],
        compiler_params=pltpu.CompilerParams(dimension_semantics=("arbitrary",)),
        name="hidden_units",
    )(x1, got2, fit2, g0, g1, u0, u1)


def down_kernel(h_ref, fit_ref, wt_ref, d0_ref, d1_ref, near_ref, far_ref, padded, scale):
    d = pl.program_id(0)
    experts, rows, units = h_ref.shape
    turn = (((0,), (0,)), ((), ()))

    @pl.when(d == 0)
    def _():
        scale[...] = jnp.zeros(scale.shape, F32)
        for e in range(experts):
            fit = fit_ref[e * rows:(e + 1) * rows, :]
            placed = lax.dot_general(fit, h_ref[e], turn, preferred_element_type=F32)
            padded[:, e * units:(e + 1) * units] = placed.astype(BF)
            wide = jnp.broadcast_to(wt_ref[e], (rows, scale.shape[1]))
            scale[...] += lax.dot_general(fit.astype(F32), wide, turn, precision=lax.Precision.HIGHEST,
                                          preferred_element_type=F32)

    @pl.when(d < NEAR)
    def _():
        for e in range(experts):
            both = jnp.concatenate([d0_ref[e], d1_ref[e]], axis=0)
            y = jnp.dot(h_ref[e], both, preferred_element_type=F32)
            near_ref[e] = (y * wt_ref[e]).astype(BF)

    @pl.when(d >= NEAR)
    def _():
        both = jnp.concatenate([ref[e] for e in range(experts) for ref in (d0_ref, d1_ref)], axis=0)
        y = jnp.dot(padded[...], both, preferred_element_type=F32)
        far_ref[...] = (y * scale[:, :1]).astype(BF)


def down_of(hidden, fit2, weight, d0, d1):
    experts, rows, units = hidden.shape
    cols, width = d0.shape[1], d0.shape[2]
    slots = fit2.shape[1]
    mat = pl.BlockSpec((experts, cols, CHUNK), lambda d: (0, 0, d))
    return pl.pallas_call(
        down_kernel,
        grid=(width // CHUNK,),
        out_shape=(jax.ShapeDtypeStruct((experts, rows, D1), BF), jax.ShapeDtypeStruct((slots, width - D1), BF)),
        in_specs=[
            pl.BlockSpec(hidden.shape, lambda d: (0, 0, 0)),
            pl.BlockSpec(fit2.shape, lambda d: (0, 0)),
            pl.BlockSpec((experts, rows, 1), lambda d: (0, 0, 0)),
            mat, mat],
        out_specs=(
            pl.BlockSpec((experts, rows, CHUNK), lambda d: (0, 0, jnp.minimum(d, NEAR - 1))),
            pl.BlockSpec((slots, CHUNK), lambda d: (0, jnp.maximum(d - NEAR, 0)))),
        scratch_shapes=[pltpu.VMEM((slots, experts * units), BF), pltpu.VMEM((slots, 128), F32)],
        compiler_params=pltpu.CompilerParams(dimension_semantics=("arbitrary",)),
        name="down_units",
    )(hidden, fit2, weight, d0, d1)


def body(tokens, w_gate, w_up, w_down, gates, dispatch):
    rows, width = tokens.shape
    experts = w_gate.shape[0]
    cap = dispatch.shape[-1]
    x, y, zh = lax.axis_index("x"), lax.axis_index("y"), lax.axis_index("zh")
    zl, c = lax.axis_index("zl"), lax.axis_index("c")
    col = x * NY + y
    span = NH * rows

    def of_parity(a):
        a = a.reshape(NL, NC, COLS, NH, experts, cap)
        a = lax.dynamic_index_in_dim(a, c, 1, keepdims=False)
        return lax.dynamic_index_in_dim(a, zh, 2, keepdims=False)

    picks = of_parity(dispatch)
    block = picks // span
    earlier = (block[..., :, None] == block[..., None, :]) & (jnp.arange(cap)[None, :] < jnp.arange(cap)[:, None])
    place = jnp.sum(earlier.astype(jnp.int32), axis=-1)

    here = jnp.where(block == col, (picks % span) * SLOTS + place, -1)
    table = here[..., None, None, :] == (jnp.arange(span)[None, :] * SLOTS + jnp.arange(SLOTS)[:, None])[..., None]
    table = jnp.any(table, axis=-1)
    pick1 = lax.dynamic_index_in_dim(table, zl, 0, keepdims=False)
    pick1 = pick1.reshape(COLS * experts * SLOTS, NH, rows).astype(BF)
    pick2 = table.transpose(1, 0, 2, 3, 4).reshape(COLS, NL, experts, SLOTS, NH, 1, rows)
    pick2 = pick2 & (jnp.arange(NL)[:, None, None, None, None, None] == jnp.arange(NL)[:, None])
    pick2 = pick2.reshape(COLS * NL * experts * SLOTS, NZ * rows).astype(BF)

    mine = lax.dynamic_index_in_dim(block * SLOTS + place, col, 1, keepdims=False)
    mine = mine.transpose(1, 0, 2)
    fit = mine[..., None] == jnp.arange(COLS * SLOTS)
    fit = fit.reshape(experts, NL, cap, COLS, SLOTS)
    fit1 = lax.dynamic_index_in_dim(fit, zl, 1, keepdims=False)
    same_e = jnp.eye(experts, dtype=bool)
    fit1 = fit1[:, :, :, None, :] & same_e[:, None, None, :, None]
    fit1 = fit1.reshape(experts * cap, COLS * experts * SLOTS).astype(BF)
    same_k = jnp.eye(NL, dtype=bool)
    fit2 = fit[:, :, :, :, None, None, :] & same_k[None, :, None, None, :, None, None] & same_e[:, None, None, None, None, :, None]
    fit2 = fit2.reshape(experts * NL * cap, COLS * NL * experts * SLOTS).astype(BF)
    weight = lax.dynamic_index_in_dim(of_parity(gates), col, 1, keepdims=False)
    weight = weight.transpose(1, 0, 2).reshape(experts, NL * cap, 1)

    pick_own = lax.dynamic_index_in_dim(pick1, zh, 1, keepdims=False)
    pick_other = lax.dynamic_index_in_dim(pick1, 1 - zh, 1, keepdims=False)
    lines, got2, og, ou, od = front(tokens, pick_own, pick_other, pick2, fit1, w_gate, w_up, w_down, 1)
    x1 = lines.reshape(experts, NL * cap, D1)
    hidden = hidden_of(x1, got2.reshape(-1, width - D1), fit2, w_gate, og, w_up, ou)
    back1, back2 = down_of(hidden, fit2, weight, w_down, od)
    back1 = back1.reshape(experts, NL, cap, D1)
    back2 = back2.reshape(COLS, NL * experts * SLOTS, width - D1)
    return back(back1, back2, pick_own, pick_other, pick2, fit1, 2)


def solution(mesh):
    split = Mesh(mesh.devices.reshape(NX, NY, NH, NL, NC), ("x", "y", "zh", "zl", "c"))
    expert, tok = ("x", "y", "zh"), ("zl", "c")
    in_specs = (P(tok + expert, None), P(expert, None, tok), P(expert, None, tok), P(expert, tok, None), P(), P())
    return jax.shard_map(body, mesh=split, in_specs=in_specs, out_specs=P(tok + expert, None), check_vma=False)
```

```python
import jax
import jax.numpy as jnp
from jax import lax
from jax.experimental import pallas as pl
from jax.experimental.pallas import tpu as pltpu
from jax.sharding import Mesh
from jax.sharding import PartitionSpec as P

NX, NY, NH, NL, NC = 4, 4, 2, 4, 2
NZ = NH * NL
COLS = NX * NY
D1 = 4096
SLOTS = 4
CHUNK = 1024
HALF = 512
NEAR = D1 // CHUNK
XY_ORDER = ((2, 2), (1, 1), (3, 3), (1, 3), (3, 1), (2, 1), (1, 2), (2, 3), (3, 2), (2, 0), (0, 2), (1, 0), (3, 0), (0, 1), (0, 3))
BF = jnp.bfloat16
F32 = jnp.float32
ANY = pl.BlockSpec(memory_space=pl.ANY)
VMEM = pl.BlockSpec(memory_space=pltpu.VMEM)
DMA = pltpu.SemaphoreType.DMA


def z_of(z):
    z = lax.rem(z + NZ, NZ)
    return {"zh": lax.div(z, NL), "zl": lax.rem(z, NL)}


def remote(src, dst, send, recv, device):
    return pltpu.make_async_remote_copy(
        src_ref=src, dst_ref=dst, send_sem=send, recv_sem=recv,
        device_id=device, device_id_type=pl.DeviceIdType.MESH)


def greet(devices):
    barrier = pltpu.get_barrier_semaphore()
    for device in devices:
        pl.semaphore_signal(barrier, inc=1, device_id=device, device_id_type=pl.DeviceIdType.MESH)
    pl.semaphore_wait(barrier, len(devices))


def xy_targets():
    x, y = lax.axis_index("x"), lax.axis_index("y")
    return [(lax.rem(x + dx, NX), lax.rem(y + dy, NY)) for dx, dy in XY_ORDER]


def xy_devices():
    return [{"x": tx, "y": ty} for tx, ty in xy_targets()]


def xy_copies(src, dst, send, recv):
    me = lax.axis_index("x") * NY + lax.axis_index("y")
    return [
        remote(src.at[tx * NY + ty], dst.at[me], send.at[d], recv.at[d], {"x": tx, "y": ty})
        for d, (tx, ty) in enumerate(xy_targets())
    ]


def my_z():
    return lax.axis_index("zh") * NL + lax.axis_index("zl")


def pair_steps(src, relay, dst, send, recv):
    z = my_z()
    half = relay.shape[1]
    first, second = [], []
    for d, step in enumerate((2, -2)):
        part = pl.ds(d * half, half)
        near = z_of(z + step)
        first.append(remote(src.at[part, pl.ds(0, relay.shape[2])], relay.at[d], send.at[d], recv.at[d], near))
        second.append(remote(relay.at[d], dst.at[part], send.at[2 + d], recv.at[2 + d], near))
    return first, second


def sub(q, rows, width, first=0):
    half, wide = rows // 2, width // 2
    return pl.ds(q // 2 * half, half), pl.ds(first + q % 2 * wide, wide)


RING_HOPS = [(t, q, up) for t in range(NZ // 2) for q in range(4) for up in (True, False)]


def front_kernel(tok_ref, mine_ref, theirs_ref, pick_ref, fit_ref, wg_ref, wu_ref, wd_ref,
                 line_ref, got_ref, og_ref, ou_ref, od_ref,
                 ring, other, relay, block, home, far,
                 xs, xr, ys, yr, us, ur, ds, dr, ps, pr, lus, lur, lds, ldr, ws, wr, ls):
    z = my_z()
    zl = lax.axis_index("zl")
    experts = line_ref.shape[0]
    _, rows, width = ring.shape
    cols, wide = block.shape[0], block.shape[2]
    start_col = tok_ref.shape[1] - width
    core = {"c": 1 - lax.axis_index("c")}
    greet(xy_devices() + [z_of(z + 1), z_of(z - 1), z_of(z + 2), z_of(z - 2), core])
    me = lax.axis_index("x") * NY + lax.axis_index("y")
    last = NZ // 2 - 1

    def hop(t, q, up):
        who = lax.rem(z + (-t if up else t) + NZ, NZ)
        r, c = sub(q, rows, width)
        src = tok_ref.at[sub(q, rows, width, start_col)] if t == 0 else ring.at[who, r, c]
        send, recv = (us, ur) if up else (ds, dr)
        return remote(src, ring.at[who, r, c], send.at[t, q], recv.at[t, q], z_of(z + (1 if up else -1)))

    hops = [(t, q, up) for t, q, up in RING_HOPS if t < last or (q < 2) == up]

    def serve(step):
        for t, q, up in hops:
            if t == step:
                hop(t, q, up).wait_recv()
                if (t + 1, q, up) in hops:
                    hop(t + 1, q, up).start()

    def pass_on(i, e, up):
        who = lax.rem(zl + (-i if up else i) + NL, NL)
        send, recv = (lus, lur) if up else (lds, ldr)
        place = line_ref.at[e, who]
        return remote(place, place, send.at[i, e], recv.at[i, e], z_of(z + (1 if up else -1)))

    def sends(i, up):
        return (zl < NL - 1) & (zl >= i) if up else (zl > 0) & (zl + i < NL)

    def gets(i, up):
        return zl - 1 - i >= 0 if up else zl + 1 + i < NL

    first, second = pair_steps(tok_ref, relay, other, ps, pr)
    for copy in first:
        copy.start()
    for t, q, up in hops:
        if t == 0:
            hop(t, q, up).start()
    weights = [remote(a, b, ws.at[i], wr.at[i], core)
               for i, (a, b) in enumerate(((wg_ref, og_ref), (wu_ref, ou_ref), (wd_ref, od_ref)))]
    for copy in weights:
        copy.start()
    ring[z] = tok_ref[:, start_col:]
    for d in range(2):
        first[d].wait_recv()
        second[d].start()
    serve(0)
    for copy in second:
        copy.wait_recv()

    @pl.loop(0, wide // CHUNK)
    def _(i):
        part = pl.ds(pl.multiple_of(i * CHUNK, CHUNK), CHUNK)
        y = jnp.dot(mine_ref[...], tok_ref[:, part], preferred_element_type=F32)
        y = y + jnp.dot(theirs_ref[...], other[:, part], preferred_element_type=F32)
        block[:, :, part] = y.reshape(cols, y.shape[0] // cols, CHUNK).astype(BF)

    blocks = xy_copies(block, home, xs, xr)
    for copy in blocks:
        copy.start()
    home[me] = block[me]
    for step in range(1, last + 1):
        serve(step)
    for copy in blocks:
        copy.wait_recv()

    @pl.loop(0, wide // CHUNK)
    def _(i):
        part = pl.ds(pl.multiple_of(i * CHUNK, CHUNK), CHUNK)
        h = home[:, :, part].astype(F32).reshape(fit_ref.shape[1], CHUNK).astype(BF)
        y = jnp.dot(fit_ref[...], h, preferred_element_type=F32).astype(BF)
        cap = y.shape[0] // experts
        for e in range(experts):
            line_ref[e, zl, :, part] = y[e * cap:(e + 1) * cap]

    for e in range(experts):
        for up in (True, False):
            @pl.when(sends(0, up))
            def _():
                pass_on(0, e, up).start()

    @pl.loop(0, width // HALF)
    def _(i):
        part = pl.ds(pl.multiple_of(i * HALF, HALF), HALF)
        every = ring[:, :, part].reshape(NZ * rows, HALF)
        y = jnp.dot(pick_ref[...], every, preferred_element_type=F32)
        far[:, :, part] = y.reshape(cols, y.shape[0] // cols, HALF).astype(BF)

    fars = xy_copies(far, got_ref, ys, yr)
    for copy in fars:
        copy.start()
    own = pltpu.make_async_copy(far.at[me], got_ref.at[me], ls)
    own.start()
    for i in range(NL - 1):
        for e in range(experts):
            for up in (True, False):
                @pl.when(gets(i, up))
                def _():
                    pass_on(i, e, up).wait_recv()
                if i < NL - 2:
                    @pl.when(sends(i + 1, up))
                    def _():
                        pass_on(i + 1, e, up).start()
    for i in range(NL - 1):
        for e in range(experts):
            for up in (True, False):
                @pl.when(sends(i, up))
                def _():
                    pass_on(i, e, up).wait_send()
    for t, q, up in hops:
        hop(t, q, up).wait_send()
    for copy in first + second + blocks:
        copy.wait_send()
    for copy in fars + weights:
        copy.wait()
    own.wait()


def front(tokens, mine, theirs, pick2, fit1, w_gate, w_up, w_down, cid):
    rows = tokens.shape[0]
    width = tokens.shape[1] - D1
    experts = w_gate.shape[0]
    cap = fit1.shape[0] // experts
    block = (COLS, mine.shape[0] // COLS, D1)
    far = (COLS, pick2.shape[0] // COLS, width)
    shapes = [(experts, NL, cap, D1), far, w_gate.shape, w_up.shape, w_down.shape]
    plane = DMA((COLS - 1,))
    return pl.pallas_call(
        front_kernel,
        out_shape=tuple(jax.ShapeDtypeStruct(shape, BF) for shape in shapes),
        in_specs=[VMEM] * 5 + [ANY] * 3, out_specs=(VMEM, ANY, ANY, ANY, ANY),
        scratch_shapes=[pltpu.VMEM((NZ, rows, width), BF), pltpu.VMEM((rows, D1), BF),
                        pltpu.VMEM((2, rows // 2, D1), BF), pltpu.VMEM(block, BF), pltpu.VMEM(block, BF),
                        pltpu.VMEM(far, BF), plane, plane, plane, plane]
        + [DMA((NZ // 2, 4))] * 4 + [DMA((4,))] * 2 + [DMA((NL - 1, experts))] * 4 + [DMA((3,))] * 2 + [DMA],
        compiler_params=pltpu.CompilerParams(collective_id=cid, has_side_effects=True),
        name="front",
    )(tokens, mine, theirs, pick2, fit1, w_gate, w_up, w_down)


def add_into(dst, a, b, width, extra=None, chunk=512):
    @pl.loop(0, width // chunk)
    def _(i):
        part = pl.ds(pl.multiple_of(i * chunk, chunk), chunk)
        total = a[:, part].astype(F32) + b[:, part].astype(F32)
        if extra is not None:
            total = total + extra[:, part].astype(F32)
        dst[:, part] = total.astype(BF)


def back_kernel(line_ref, far_ref, mine_ref, theirs_ref, pick_ref, fit_ref, out_ref,
                lu, ld, summed, got2, part_ref, block, home, away, own, got, relay, ub, db,
                xs, xr, ys, yr, us, ur, ds, dr, ps, pr, lus, lur, lds, ldr, ls):
    z = my_z()
    zl = lax.axis_index("zl")
    experts = line_ref.shape[0]
    near = line_ref.shape[3]
    _, rows, width = part_ref.shape
    wide = width // 2
    cols = block.shape[0]
    me = lax.axis_index("x") * NY + lax.axis_index("y")
    greet(xy_devices() + [z_of(z + 1), z_of(z - 1), z_of(z + 2), z_of(z - 2)])
    last = NZ // 2
    turn = (((0,), (0,)), ((), ()))

    def send_sum(j, e, up, fresh):
        buf = lu if up else ld
        slot = j - 1 if up else j
        send, recv = (lus, lur) if up else (lds, ldr)
        src = line_ref.at[e, j] if fresh else buf.at[slot, e]
        return remote(src, buf.at[slot, e], send.at[slot, e], recv.at[slot, e], z_of(z + (1 if up else -1)))

    order = [(NL - 1 - i, i) for i in range(NL - 1)]
    fars = xy_copies(far_ref, got2, ys, yr)
    for copy in fars:
        copy.start()
    keep = pltpu.make_async_copy(far_ref.at[me], got2.at[me], ls)
    keep.start()
    edge = [(i, e) for i in range(NL - 1) for e in range(experts)]
    for up, seat in ((True, 0), (False, NL - 1)):
        @pl.when(zl == seat)
        def _():
            copies = [send_sum(NL - 1 - i if up else i, e, up, True) for i, e in edge]
            copies[0].start()
            copies[1].start()
            for n in range(2, len(copies)):
                copies[n - 2].wait_send()
                copies[n].start()
            copies[-2].wait_send()
            copies[-1].wait_send()

    def pass_on(j, e, up):
        slot = j - 1 if up else j
        buf = lu if up else ld
        copy = send_sum(j, e, up, False)
        copy.wait_recv()
        add_into(buf.at[slot, e], buf.at[slot, e], line_ref.at[e, j], near)
        copy.start()

    for seat, up in ((1, True), (2, False)):
        end, inner, start = (3, 2, 0) if up else (0, 1, 3)
        events = [(end, 0, up), (end, 1, up), (start, 0, not up), (inner, 0, up), (start, 1, not up), (inner, 1, up)]

        @pl.when(zl == seat)
        def _():
            for event in events:
                pass_on(*event)
            for j, e, up in events:
                send_sum(j, e, up, False).wait_send()
    for ju, jd in order:
        for e in range(experts):
            @pl.when(zl == ju)
            def _():
                send_sum(ju, e, True, False).wait_recv()

            @pl.when(zl == jd)
            def _():
                send_sum(jd, e, False, False).wait_recv()
    for e in range(experts):
        @pl.when(zl == 0)
        def _():
            add_into(summed.at[e], line_ref.at[e, 0], ld.at[0, e], near)

        @pl.when(zl == NL - 1)
        def _():
            add_into(summed.at[e], line_ref.at[e, NL - 1], lu.at[NL - 2, e], near)
        for mid in range(1, NL - 1):
            @pl.when(zl == mid)
            def _():
                add_into(summed.at[e], line_ref.at[e, mid], lu.at[mid - 1, e], near, ld.at[mid, e])

    @pl.loop(0, near // CHUNK)
    def _(i):
        part = pl.ds(pl.multiple_of(i * CHUNK, CHUNK), CHUNK)
        y = lax.dot_general(fit_ref[...], summed[:, :, part].reshape(fit_ref.shape[0], CHUNK), turn,
                            preferred_element_type=F32)
        block[:, :, part] = y.reshape(cols, y.shape[0] // cols, CHUNK).astype(BF)

    blocks = xy_copies(block, home, xs, xr)
    for copy in blocks:
        copy.start()
    home[me] = block[me]
    for copy in fars:
        copy.wait_recv()
    keep.wait()

    @pl.loop(0, width // HALF)
    def _(i):
        part = pl.ds(pl.multiple_of(i * HALF, HALF), HALF)
        h = got2[:, :, part].reshape(pick_ref.shape[0], HALF)
        y = lax.dot_general(pick_ref[...], h, turn, preferred_element_type=F32)
        part_ref[:, :, part] = y.reshape(NZ, rows, HALF).astype(BF)

    def spot(t, up):
        return lax.rem(z + (last - t if up else t - last) + NZ, NZ)

    def hop(t, q, up, fresh):
        buf = ub if up else db
        send, recv = (us, ur) if up else (ds, dr)
        src = part_ref.at[(spot(t, up),) + sub(q, rows, width)] if fresh else buf.at[t - 1, q]
        return remote(src, buf.at[t, q], send.at[t, q], recv.at[t, q], z_of(z + (1 if up else -1)))

    def fresh_of(t, q, up):
        return t == 0 or (t == 1 and (q < 2) != up)

    hops = [(t, q, up) for t, q, up in RING_HOPS if t > 0 or (q < 2) == up]

    def serve(step):
        for t, q, up in hops:
            if t == step:
                buf = ub if up else db
                hop(t, q, up, fresh_of(t, q, up)).wait_recv()
                if t < last - 1:
                    add_into(buf.at[t, q], buf.at[t, q], part_ref.at[(spot(t + 1, up),) + sub(q, rows, width)], wide)
                    hop(t + 1, q, up, False).start()

    for t, q, up in hops:
        if fresh_of(t, q, up):
            hop(t, q, up, True).start()
    serve(0)
    serve(1)
    for copy in blocks:
        copy.wait_recv()

    @pl.loop(0, near // CHUNK)
    def _(i):
        part = pl.ds(pl.multiple_of(i * CHUNK, CHUNK), CHUNK)
        h = home[:, :, part].astype(F32).reshape(mine_ref.shape[0], CHUNK).astype(BF)
        away[:, part] = lax.dot_general(theirs_ref[...], h, turn, preferred_element_type=F32).astype(BF)
        own[:, part] = lax.dot_general(mine_ref[...], h, turn, preferred_element_type=F32)

    first, second = pair_steps(away, relay, got, ps, pr)
    for copy in first:
        copy.start()
    serve(2)
    for d in range(2):
        first[d].wait_recv()
        second[d].start()
    serve(3)
    for q in range(4):
        r, c = sub(q, rows, width)
        there = out_ref.at[sub(q, rows, width, near)]
        add_into(there, part_ref.at[z, r, c], ub.at[last - 1, q], wide, db.at[last - 1, q])
    for copy in second:
        copy.wait_recv()
    add_into(out_ref.at[:, pl.ds(0, near)], own, got, near)
    for t, q, up in hops:
        hop(t, q, up, fresh_of(t, q, up)).wait_send()
    for copy in first + second + blocks + fars:
        copy.wait_send()


def back(lines, fars, mine, theirs, pick2, fit1, cid):
    experts, _, cap, near = lines.shape
    width = fars.shape[2]
    rows = mine.shape[1]
    block = (COLS, mine.shape[0] // COLS, near)
    buf = pltpu.VMEM((NZ // 2, 4, rows // 2, width // 2), BF)
    line = pltpu.VMEM((NL - 1, experts, cap, near), BF)
    plane = DMA((COLS - 1,))
    return pl.pallas_call(
        back_kernel,
        out_shape=jax.ShapeDtypeStruct((rows, near + width), BF),
        in_specs=[VMEM, ANY, VMEM, VMEM, VMEM, VMEM], out_specs=VMEM,
        scratch_shapes=[line, line, pltpu.VMEM((experts, cap, near), BF), pltpu.VMEM(fars.shape, BF),
                        pltpu.VMEM((NZ, rows, width), BF), pltpu.VMEM(block, BF), pltpu.VMEM(block, BF),
                        pltpu.VMEM((rows, near), BF), pltpu.VMEM((rows, near), F32), pltpu.VMEM((rows, near), BF),
                        pltpu.VMEM((2, rows // 2, near), BF), buf, buf, plane, plane, plane, plane]
        + [DMA((NZ // 2, 4))] * 4 + [DMA((4,))] * 2 + [DMA((NL - 1, experts))] * 4 + [DMA],
        compiler_params=pltpu.CompilerParams(collective_id=cid, has_side_effects=True),
        name="back",
    )(lines, fars, mine, theirs, pick2, fit1)


def hidden_kernel(x1_ref, got_ref, fit_ref, g0_ref, g1_ref, u0_ref, u1_ref, h_ref, acc):
    d = pl.program_id(0)
    experts, rows, half = h_ref.shape

    @pl.when(d == 0)
    def _():
        acc[...] = jnp.zeros(acc.shape, F32)

    def add(e, x):
        both = jnp.concatenate([g0_ref[e], g1_ref[e], u0_ref[e], u1_ref[e]], axis=1)
        acc[e] += jnp.dot(x, both, preferred_element_type=F32)

    @pl.when(d < NEAR)
    def _():
        for e in range(experts):
            add(e, x1_ref[e])

    @pl.when(d >= NEAR)
    def _():
        for e in range(experts):
            fit = fit_ref[e * rows:(e + 1) * rows, :]
            add(e, jnp.dot(fit, got_ref[...], preferred_element_type=F32).astype(BF))

    @pl.when(d == pl.num_programs(0) - 1)
    def _():
        for e in range(experts):
            gate, up = acc[e, :, :half], acc[e, :, half:]
            h_ref[e] = (gate / (1.0 + jnp.exp(-gate)) * up).astype(BF)


def hidden_of(x1, got2, fit2, g0, g1, u0, u1):
    experts, rows, _ = x1.shape
    width, cols = g0.shape[1], g0.shape[2]
    weight = pl.BlockSpec((experts, CHUNK, cols), lambda d: (0, d, 0))
    return pl.pallas_call(
        hidden_kernel,
        grid=(width // CHUNK,),
        out_shape=jax.ShapeDtypeStruct((experts, rows, 2 * cols), BF),
        in_specs=[
            pl.BlockSpec((experts, rows, CHUNK), lambda d: (0, 0, jnp.minimum(d, NEAR - 1))),
            pl.BlockSpec((got2.shape[0], CHUNK), lambda d: (0, jnp.maximum(d - NEAR, 0))),
            pl.BlockSpec(fit2.shape, lambda d: (0, 0)),
            weight, weight, weight, weight],
        out_specs=pl.BlockSpec((experts, rows, 2 * cols), lambda d: (0, 0, 0)),
        scratch_shapes=[pltpu.VMEM((experts, rows, 4 * cols), F32)],
        compiler_params=pltpu.CompilerParams(dimension_semantics=("arbitrary",)),
        name="hidden_units",
    )(x1, got2, fit2, g0, g1, u0, u1)


def down_kernel(h_ref, fit_ref, wt_ref, d0_ref, d1_ref, near_ref, far_ref, padded, scale):
    d = pl.program_id(0)
    experts, rows, units = h_ref.shape
    turn = (((0,), (0,)), ((), ()))

    @pl.when(d == 0)
    def _():
        scale[...] = jnp.zeros(scale.shape, F32)
        for e in range(experts):
            fit = fit_ref[e * rows:(e + 1) * rows, :]
            placed = lax.dot_general(fit, h_ref[e], turn, preferred_element_type=F32)
            padded[:, e * units:(e + 1) * units] = placed.astype(BF)
            wide = jnp.broadcast_to(wt_ref[e], (rows, scale.shape[1]))
            scale[...] += lax.dot_general(fit.astype(F32), wide, turn, precision=lax.Precision.HIGHEST,
                                          preferred_element_type=F32)

    @pl.when(d < NEAR)
    def _():
        for e in range(experts):
            both = jnp.concatenate([d0_ref[e], d1_ref[e]], axis=0)
            y = jnp.dot(h_ref[e], both, preferred_element_type=F32)
            near_ref[e] = (y * wt_ref[e]).astype(BF)

    @pl.when(d >= NEAR)
    def _():
        both = jnp.concatenate([ref[e] for e in range(experts) for ref in (d0_ref, d1_ref)], axis=0)
        y = jnp.dot(padded[...], both, preferred_element_type=F32)
        far_ref[...] = (y * scale[:, :1]).astype(BF)


def down_of(hidden, fit2, weight, d0, d1):
    experts, rows, units = hidden.shape
    cols, width = d0.shape[1], d0.shape[2]
    slots = fit2.shape[1]
    mat = pl.BlockSpec((experts, cols, CHUNK), lambda d: (0, 0, d))
    return pl.pallas_call(
        down_kernel,
        grid=(width // CHUNK,),
        out_shape=(jax.ShapeDtypeStruct((experts, rows, D1), BF), jax.ShapeDtypeStruct((slots, width - D1), BF)),
        in_specs=[
            pl.BlockSpec(hidden.shape, lambda d: (0, 0, 0)),
            pl.BlockSpec(fit2.shape, lambda d: (0, 0)),
            pl.BlockSpec((experts, rows, 1), lambda d: (0, 0, 0)),
            mat, mat],
        out_specs=(
            pl.BlockSpec((experts, rows, CHUNK), lambda d: (0, 0, jnp.minimum(d, NEAR - 1))),
            pl.BlockSpec((slots, CHUNK), lambda d: (0, jnp.maximum(d - NEAR, 0)))),
        scratch_shapes=[pltpu.VMEM((slots, experts * units), BF), pltpu.VMEM((slots, 128), F32)],
        compiler_params=pltpu.CompilerParams(dimension_semantics=("arbitrary",)),
        name="down_units",
    )(hidden, fit2, weight, d0, d1)


def iota(shape, dim):
    return lax.broadcasted_iota(jnp.int32, shape, dim)


def ones_of(mask):
    return jnp.where(mask, 1.0, 0.0).astype(BF)


def over(a, n):
    return a >> (n.bit_length() - 1)


def rest(a, n):
    return a & (n - 1)


def table_kernel(seat_ref, dispatch_ref, gates_ref, mine_ref, theirs_ref, pick_ref, fit1_ref, fit2_ref, wt_ref):
    col, zh, zl, c = seat_ref[0], seat_ref[1], seat_ref[2], seat_ref[3]
    experts = wt_ref.shape[0]
    total, cap = dispatch_ref.shape[1], dispatch_ref.shape[2]
    lanes = COLS * experts
    span = pick_ref.shape[1] // NL
    rows = span // NH
    turn = (((0,), (0,)), ((), ()))
    level = (((1,), (1,)), ((), ()))

    who, lane = iota((total, lanes), 0), iota((total, lanes), 1)
    chosen = ones_of(who == over(lane, experts) * (NH * experts) + zh * experts + rest(lane, experts))
    blocks, offsets, weights = [], [], []
    for k in range(NL):
        v = dispatch_ref[NC * k + c]
        for out, part in ((blocks, over(v, span)), (offsets, rest(v, span))):
            out.append(lax.dot_general(part.astype(F32).astype(BF), chosen, turn, preferred_element_type=F32))
        weights.append(lax.dot_general(gates_ref[NC * k + c], chosen.astype(F32), turn,
                                       precision=lax.Precision.HIGHEST, preferred_element_type=F32))
    block = jnp.concatenate(blocks, axis=1)
    offset = jnp.concatenate(offsets, axis=1)
    weight = jnp.concatenate(weights, axis=1)
    row = iota(block.shape, 0)
    place = jnp.zeros(block.shape, F32)
    for first in range(cap - 1):
        place = place + jnp.where((block == block[first:first + 1, :]) & (row > first), 1.0, 0.0)

    here = jnp.where(block == col.astype(F32), offset * SLOTS + place, -1.0)
    width = NL * lanes
    slots = width * SLOTS
    wide_row = iota((span, width), 0).astype(F32)
    slot, source = iota((slots, width), 0), iota((slots, width), 1)
    per_k = experts * SLOTS
    slot_lane = rest(over(slot, per_k), NL) * lanes + over(slot, NL * per_k) * experts + rest(over(slot, SLOTS), experts)
    slot_lane = slot_lane * SLOTS + rest(slot, SLOTS) - source * SLOTS
    near, near_source = iota((lanes * SLOTS, width), 0), iota((lanes * SLOTS, width), 1)
    near_lane = zl * (lanes * SLOTS) + near - near_source * SLOTS
    rowed = jnp.zeros((slots, span), F32)
    nearby = jnp.zeros((lanes * SLOTS, span), F32)
    for w in range(SLOTS):
        found = jnp.zeros((span, width), F32)
        for i in range(cap):
            found = found + jnp.where(here[i:i + 1, :] == wide_row * SLOTS + w, 1.0, 0.0)
        found = found.astype(BF)
        rowed = rowed + lax.dot_general(ones_of(slot_lane == w), found, level,
                                        preferred_element_type=F32)
        nearby = nearby + lax.dot_general(ones_of(near_lane == w), found, level,
                                          preferred_element_type=F32)
    rowed, nearby = rowed.astype(BF), nearby.astype(BF)
    r, j = iota((span, NL * span), 0), iota((span, NL * span), 1)
    spread = jnp.dot(rowed, ones_of(r == over(j, NL * rows) * rows + rest(j, rows)), preferred_element_type=F32)
    m, j = iota(spread.shape, 0), iota(spread.shape, 1)
    pick_ref[...] = jnp.where(rest(over(m, per_k), NL) == rest(over(j, rows), NL), spread, 0.0).astype(BF)
    r, o = iota((span, rows), 0), iota((span, rows), 1)
    mine_ref[...] = jnp.dot(nearby, ones_of(r == zh * rows + o), preferred_element_type=F32).astype(BF)
    theirs_ref[...] = jnp.dot(nearby, ones_of(r == (NH - 1 - zh) * rows + o), preferred_element_type=F32).astype(BF)

    def column(a, k, e):
        at = iota((cap, width), 1) == k * lanes + col * experts + e
        return jnp.sum(jnp.where(at, a, 0.0), axis=1, keepdims=True)

    key = block * SLOTS + place
    m = iota((1, slots), 1)
    m_key = (over(m, NL * per_k) * SLOTS + rest(m, SLOTS)).astype(F32)
    n = iota((1, lanes * SLOTS), 1)
    n_key = (over(n, per_k) * SLOTS + rest(n, SLOTS)).astype(F32)
    for e in range(experts):
        for k in range(NL):
            at = (e * NL + k) * cap
            ours = (rest(over(m, per_k), NL) == k) & (rest(over(m, SLOTS), experts) == e)
            fit2_ref[at:at + cap, :] = ones_of(column(key, k, e) == jnp.where(ours, m_key, -1.0))
            wt_ref[e, k * cap:(k + 1) * cap, :] = column(weight, k, e)
        ours = rest(over(n, SLOTS), experts) == e
        fit1_ref[e * cap:(e + 1) * cap, :] = ones_of(column(key, zl, e) == jnp.where(ours, n_key, -1.0))


def tables(seat, dispatch, gates, rows, experts):
    cap = dispatch.shape[2]
    small = COLS * experts * SLOTS
    shapes = [(small, rows), (small, rows), (NL * small, NZ * rows), (experts * cap, small),
              (experts * NL * cap, NL * small)]
    return pl.pallas_call(
        table_kernel,
        out_shape=tuple(jax.ShapeDtypeStruct(shape, BF) for shape in shapes)
        + (jax.ShapeDtypeStruct((experts, NL * cap, 1), F32),),
        in_specs=[pl.BlockSpec(memory_space=pltpu.SMEM), VMEM, VMEM],
        out_specs=(VMEM,) * 6,
        name="tables",
    )(seat, dispatch, gates)


def body(tokens, w_gate, w_up, w_down, gates, dispatch):
    rows, width = tokens.shape
    experts = w_gate.shape[0]
    cap = dispatch.shape[-1]
    col = lax.axis_index("x") * NY + lax.axis_index("y")
    seat = jnp.stack([col, lax.axis_index("zh"), lax.axis_index("zl"), lax.axis_index("c")]).astype(jnp.int32)
    mine, theirs, pick2, fit1, fit2, weight = tables(seat, dispatch, gates, rows, experts)
    lines, got2, og, ou, od = front(tokens, mine, theirs, pick2, fit1, w_gate, w_up, w_down, 1)
    x1 = lines.reshape(experts, NL * cap, D1)
    hidden = hidden_of(x1, got2.reshape(-1, width - D1), fit2, w_gate, og, w_up, ou)
    back1, back2 = down_of(hidden, fit2, weight, w_down, od)
    back1 = back1.reshape(experts, NL, cap, D1)
    back2 = back2.reshape(COLS, NL * experts * SLOTS, width - D1)
    return back(back1, back2, mine, theirs, pick2, fit1, 2)


def solution(mesh):
    split = Mesh(mesh.devices.reshape(NX, NY, NH, NL, NC), ("x", "y", "zh", "zl", "c"))
    expert, tok = ("x", "y", "zh"), ("zl", "c")
    in_specs = (P(tok + expert, None), P(expert, None, tok), P(expert, None, tok), P(expert, tok, None), P(), P())
    return jax.shard_map(body, mesh=split, in_specs=in_specs, out_specs=P(tok + expert, None), check_vma=False)
```

```python
import jax
import jax.numpy as jnp
from jax import lax
from jax.experimental import pallas as pl
from jax.experimental.pallas import tpu as pltpu
from jax.sharding import Mesh
from jax.sharding import PartitionSpec as P

NX, NY, NH, NL, NC = 4, 4, 2, 4, 2
NZ = NH * NL
COLS = NX * NY
D1 = 4096
SLOTS = 4
CHUNK = 1024
HALF = 512
NEAR = D1 // CHUNK
XY_ORDER = ((2, 2), (1, 1), (3, 3), (1, 3), (3, 1), (2, 1), (1, 2), (2, 3), (3, 2), (2, 0), (0, 2), (1, 0), (3, 0), (0, 1), (0, 3))
BF = jnp.bfloat16
F32 = jnp.float32
ANY = pl.BlockSpec(memory_space=pl.ANY)
VMEM = pl.BlockSpec(memory_space=pltpu.VMEM)
DMA = pltpu.SemaphoreType.DMA


def z_of(z):
    z = lax.rem(z + NZ, NZ)
    return {"zh": lax.div(z, NL), "zl": lax.rem(z, NL)}


def remote(src, dst, send, recv, device):
    return pltpu.make_async_remote_copy(
        src_ref=src, dst_ref=dst, send_sem=send, recv_sem=recv,
        device_id=device, device_id_type=pl.DeviceIdType.MESH)


def greet(devices):
    barrier = pltpu.get_barrier_semaphore()
    for device in devices:
        pl.semaphore_signal(barrier, inc=1, device_id=device, device_id_type=pl.DeviceIdType.MESH)
    pl.semaphore_wait(barrier, len(devices))


def xy_targets():
    x, y = lax.axis_index("x"), lax.axis_index("y")
    return [(lax.rem(x + dx, NX), lax.rem(y + dy, NY)) for dx, dy in XY_ORDER]


def xy_devices():
    return [{"x": tx, "y": ty} for tx, ty in xy_targets()]


def xy_copies(src, dst, send, recv, first=0, count=None):
    me = lax.axis_index("x") * NY + lax.axis_index("y")
    part = pl.ds(first, src.shape[1] if count is None else count)
    return [
        remote(src.at[tx * NY + ty, part], dst.at[me, part], send.at[d], recv.at[d], {"x": tx, "y": ty})
        for d, (tx, ty) in enumerate(xy_targets())
    ]


def my_z():
    return lax.axis_index("zh") * NL + lax.axis_index("zl")


def pair_steps(src, relay, dst, send, recv):
    z = my_z()
    half = relay.shape[1]
    first, second = [], []
    for d, step in enumerate((2, -2)):
        part = pl.ds(d * half, half)
        near = z_of(z + step)
        first.append(remote(src.at[part, pl.ds(0, relay.shape[2])], relay.at[d], send.at[d], recv.at[d], near))
        second.append(remote(relay.at[d], dst.at[part], send.at[2 + d], recv.at[2 + d], near))
    return first, second


def sub(q, rows, width, first=0):
    half, wide = rows // 2, width // 2
    return pl.ds(q // 2 * half, half), pl.ds(first + q % 2 * wide, wide)


RING_HOPS = [(t, q, up) for t in range(NZ // 2) for q in range(4) for up in (True, False)]


def front_kernel(tok_ref, mine_ref, theirs_ref, pick_ref, fit_ref, wg_ref, wu_ref, wd_ref,
                 line_ref, got_ref, og_ref, ou_ref, od_ref,
                 ring, other, relay, block, home, far,
                 xs, xr, ys, yr, vs, vr, us, ur, ds, dr, ps, pr, lus, lur, lds, ldr, ws, wr, ls):
    z = my_z()
    zl = lax.axis_index("zl")
    experts = line_ref.shape[0]
    _, rows, width = ring.shape
    cols, wide = block.shape[0], block.shape[2]
    start_col = tok_ref.shape[1] - width
    core = {"c": 1 - lax.axis_index("c")}
    greet(xy_devices() + [z_of(z + 1), z_of(z - 1), z_of(z + 2), z_of(z - 2), core])
    me = lax.axis_index("x") * NY + lax.axis_index("y")
    last = NZ // 2 - 1

    def hop(t, q, up):
        who = lax.rem(z + (-t if up else t) + NZ, NZ)
        r, c = sub(q, rows, width)
        src = tok_ref.at[sub(q, rows, width, start_col)] if t == 0 else ring.at[who, r, c]
        send, recv = (us, ur) if up else (ds, dr)
        return remote(src, ring.at[who, r, c], send.at[t, q], recv.at[t, q], z_of(z + (1 if up else -1)))

    hops = [(t, q, up) for t, q, up in RING_HOPS if t < last or (q < 2) == up]

    def serve(step):
        for t, q, up in hops:
            if t == step:
                hop(t, q, up).wait_recv()
                if (t + 1, q, up) in hops:
                    hop(t + 1, q, up).start()

    def pass_on(i, e, up):
        who = lax.rem(zl + (-i if up else i) + NL, NL)
        send, recv = (lus, lur) if up else (lds, ldr)
        place = line_ref.at[e, who]
        return remote(place, place, send.at[i, e], recv.at[i, e], z_of(z + (1 if up else -1)))

    def sends(i, up):
        return (zl < NL - 1) & (zl >= i) if up else (zl > 0) & (zl + i < NL)

    def gets(i, up):
        return zl - 1 - i >= 0 if up else zl + 1 + i < NL

    first, second = pair_steps(tok_ref, relay, other, ps, pr)
    for copy in first:
        copy.start()
    for t, q, up in hops:
        if t == 0:
            hop(t, q, up).start()
    weights = [remote(a, b, ws.at[i], wr.at[i], core)
               for i, (a, b) in enumerate(((wg_ref, og_ref), (wu_ref, ou_ref), (wd_ref, od_ref)))]
    for copy in weights:
        copy.start()
    ring[z] = tok_ref[:, start_col:]
    for d in range(2):
        first[d].wait_recv()
        second[d].start()
    serve(0)
    for copy in second:
        copy.wait_recv()

    @pl.loop(0, wide // CHUNK)
    def _(i):
        part = pl.ds(pl.multiple_of(i * CHUNK, CHUNK), CHUNK)
        y = jnp.dot(mine_ref[...], tok_ref[:, part], preferred_element_type=F32)
        y = y + jnp.dot(theirs_ref[...], other[:, part], preferred_element_type=F32)
        block[:, :, part] = y.reshape(cols, y.shape[0] // cols, CHUNK).astype(BF)

    blocks = xy_copies(block, home, xs, xr)
    for copy in blocks:
        copy.start()
    home[me] = block[me]
    fars = []

    def far_part(h, send, recv):
        count = far.shape[1] // 2

        @pl.loop(0, width // HALF)
        def _(i):
            part = pl.ds(pl.multiple_of(i * HALF, HALF), HALF)
            found = []
            for p in (2 * h, 2 * h + 1):
                k = lax.rem(zl + p + 1, NL)
                both = jnp.concatenate([ring[k, :, part], ring[k + NL, :, part]], axis=0)
                y = jnp.dot(pick_ref[p], both, preferred_element_type=F32)
                found.append(y.reshape(cols, count // 2, HALF))
            far[:, h * count:(h + 1) * count, part] = jnp.concatenate(found, axis=1).astype(BF)

        copies = xy_copies(far, got_ref, send, recv, h * count, count)
        for copy in copies:
            copy.start()
        fars.extend(copies)

    serve(1)
    serve(2)
    far_part(0, ys, yr)
    for copy in blocks:
        copy.wait_recv()

    @pl.loop(0, wide // CHUNK)
    def _(i):
        part = pl.ds(pl.multiple_of(i * CHUNK, CHUNK), CHUNK)
        h = home[:, :, part].astype(F32).reshape(fit_ref.shape[1], CHUNK).astype(BF)
        y = jnp.dot(fit_ref[...], h, preferred_element_type=F32).astype(BF)
        cap = y.shape[0] // experts
        for e in range(experts):
            line_ref[e, zl, :, part] = y[e * cap:(e + 1) * cap]

    for e in range(experts):
        for up in (True, False):
            @pl.when(sends(0, up))
            def _():
                pass_on(0, e, up).start()

    serve(3)
    far_part(1, vs, vr)
    own = pltpu.make_async_copy(far.at[me], got_ref.at[me], ls)
    own.start()
    for i in range(NL - 1):
        for e in range(experts):
            for up in (True, False):
                @pl.when(gets(i, up))
                def _():
                    pass_on(i, e, up).wait_recv()
                if i < NL - 2:
                    @pl.when(sends(i + 1, up))
                    def _():
                        pass_on(i + 1, e, up).start()
    for i in range(NL - 1):
        for e in range(experts):
            for up in (True, False):
                @pl.when(sends(i, up))
                def _():
                    pass_on(i, e, up).wait_send()
    for t, q, up in hops:
        hop(t, q, up).wait_send()
    for copy in first + second + blocks:
        copy.wait_send()
    for copy in fars + weights:
        copy.wait()
    own.wait()


def front(tokens, mine, theirs, pick2, fit1, w_gate, w_up, w_down, cid):
    rows = tokens.shape[0]
    width = tokens.shape[1] - D1
    experts = w_gate.shape[0]
    cap = fit1.shape[0] // experts
    block = (COLS, mine.shape[0] // COLS, D1)
    far = (COLS, NL * pick2.shape[1] // COLS, width)
    shapes = [(experts, NL, cap, D1), far, w_gate.shape, w_up.shape, w_down.shape]
    plane = DMA((COLS - 1,))
    return pl.pallas_call(
        front_kernel,
        out_shape=tuple(jax.ShapeDtypeStruct(shape, BF) for shape in shapes),
        in_specs=[VMEM] * 5 + [ANY] * 3, out_specs=(VMEM, ANY, ANY, ANY, ANY),
        scratch_shapes=[pltpu.VMEM((NZ, rows, width), BF), pltpu.VMEM((rows, D1), BF),
                        pltpu.VMEM((2, rows // 2, D1), BF), pltpu.VMEM(block, BF), pltpu.VMEM(block, BF),
                        pltpu.VMEM(far, BF)] + [plane] * 6
        + [DMA((NZ // 2, 4))] * 4 + [DMA((4,))] * 2 + [DMA((NL - 1, experts))] * 4 + [DMA((3,))] * 2 + [DMA],
        compiler_params=pltpu.CompilerParams(collective_id=cid, has_side_effects=True),
        name="front",
    )(tokens, mine, theirs, pick2, fit1, w_gate, w_up, w_down)


def add_into(dst, a, b, width, extra=None, chunk=512):
    @pl.loop(0, width // chunk)
    def _(i):
        part = pl.ds(pl.multiple_of(i * chunk, chunk), chunk)
        total = a[:, part].astype(F32) + b[:, part].astype(F32)
        if extra is not None:
            total = total + extra[:, part].astype(F32)
        dst[:, part] = total.astype(BF)


def back_kernel(line_ref, far_ref, mine_ref, theirs_ref, pick_ref, fit_ref, out_ref,
                lu, ld, summed, got2, part_ref, block, home, away, own, got, relay, ub, db,
                xs, xr, ys, yr, vs, vr, us, ur, ds, dr, ps, pr, lus, lur, lds, ldr, ls):
    z = my_z()
    zl = lax.axis_index("zl")
    experts = line_ref.shape[0]
    near = line_ref.shape[3]
    _, rows, width = part_ref.shape
    wide = width // 2
    cols = block.shape[0]
    me = lax.axis_index("x") * NY + lax.axis_index("y")
    greet(xy_devices() + [z_of(z + 1), z_of(z - 1), z_of(z + 2), z_of(z - 2)])
    last = NZ // 2
    turn = (((0,), (0,)), ((), ()))

    def send_sum(j, e, up, fresh):
        buf = lu if up else ld
        slot = j - 1 if up else j
        send, recv = (lus, lur) if up else (lds, ldr)
        src = line_ref.at[e, j] if fresh else buf.at[slot, e]
        return remote(src, buf.at[slot, e], send.at[slot, e], recv.at[slot, e], z_of(z + (1 if up else -1)))

    order = [(NL - 1 - i, i) for i in range(NL - 1)]
    count = got2.shape[1] // 2
    fars = [xy_copies(far_ref, got2, ys, yr, 0, count), xy_copies(far_ref, got2, vs, vr, count, count)]
    for copy in fars[1] + fars[0]:
        copy.start()
    keep = pltpu.make_async_copy(far_ref.at[me], got2.at[me], ls)
    keep.start()
    edge = [(i, e) for i in range(NL - 1) for e in range(experts)]
    for up, seat in ((True, 0), (False, NL - 1)):
        @pl.when(zl == seat)
        def _():
            copies = [send_sum(NL - 1 - i if up else i, e, up, True) for i, e in edge]
            copies[0].start()
            copies[1].start()
            for n in range(2, len(copies)):
                copies[n - 2].wait_send()
                copies[n].start()
            copies[-2].wait_send()
            copies[-1].wait_send()

    def pass_on(j, e, up):
        slot = j - 1 if up else j
        buf = lu if up else ld
        copy = send_sum(j, e, up, False)
        copy.wait_recv()
        add_into(buf.at[slot, e], buf.at[slot, e], line_ref.at[e, j], near)
        copy.start()

    for seat, up in ((1, True), (2, False)):
        end, inner, start = (3, 2, 0) if up else (0, 1, 3)
        events = [(end, 0, up), (end, 1, up), (start, 0, not up), (inner, 0, up), (start, 1, not up), (inner, 1, up)]

        @pl.when(zl == seat)
        def _():
            for event in events:
                pass_on(*event)
            for j, e, up in events:
                send_sum(j, e, up, False).wait_send()
    def spot(t, up):
        return lax.rem(z + (last - t if up else t - last) + NZ, NZ)

    def hop(t, q, up, fresh):
        buf = ub if up else db
        send, recv = (us, ur) if up else (ds, dr)
        src = part_ref.at[(spot(t, up),) + sub(q, rows, width)] if fresh else buf.at[t - 1, q]
        return remote(src, buf.at[t, q], send.at[t, q], recv.at[t, q], z_of(z + (1 if up else -1)))

    def fresh_of(t, q, up):
        return t == 0 or (t == 1 and (q < 2) != up)

    hops = [(t, q, up) for t, q, up in RING_HOPS if t > 0 or (q < 2) == up]

    def serve(step):
        for t, q, up in hops:
            if t == step:
                buf = ub if up else db
                hop(t, q, up, fresh_of(t, q, up)).wait_recv()
                if t < last - 1:
                    add_into(buf.at[t, q], buf.at[t, q], part_ref.at[(spot(t + 1, up),) + sub(q, rows, width)], wide)
                    hop(t + 1, q, up, False).start()

    def sums_of(h):
        for copy in fars[h]:
            copy.wait_recv()

        @pl.loop(0, width // HALF)
        def _(i):
            part = pl.ds(pl.multiple_of(i * HALF, HALF), HALF)
            whole = got2[:, h * count:(h + 1) * count, part].astype(F32)
            for p in (0, 1):
                each = whole[:, p * (count // 2):(p + 1) * (count // 2)].reshape(pick_ref.shape[1], HALF).astype(BF)
                y = lax.dot_general(pick_ref[2 * h + p], each, turn, preferred_element_type=F32).astype(BF)
                k = lax.rem(zl + 2 * h + p + 1, NL)
                part_ref[k, :, part] = y[:rows]
                part_ref[k + NL, :, part] = y[rows:]

    keep.wait()
    sums_of(1)
    for t, q, up in hops:
        if fresh_of(t, q, up) and (t == 0 or up):
            hop(t, q, up, True).start()
    for ju, jd in order:
        for e in range(experts):
            @pl.when(zl == ju)
            def _():
                send_sum(ju, e, True, False).wait_recv()

            @pl.when(zl == jd)
            def _():
                send_sum(jd, e, False, False).wait_recv()
    for e in range(experts):
        @pl.when(zl == 0)
        def _():
            add_into(summed.at[e], line_ref.at[e, 0], ld.at[0, e], near)

        @pl.when(zl == NL - 1)
        def _():
            add_into(summed.at[e], line_ref.at[e, NL - 1], lu.at[NL - 2, e], near)
        for mid in range(1, NL - 1):
            @pl.when(zl == mid)
            def _():
                add_into(summed.at[e], line_ref.at[e, mid], lu.at[mid - 1, e], near, ld.at[mid, e])

    @pl.loop(0, near // CHUNK)
    def _(i):
        part = pl.ds(pl.multiple_of(i * CHUNK, CHUNK), CHUNK)
        y = lax.dot_general(fit_ref[...], summed[:, :, part].reshape(fit_ref.shape[0], CHUNK), turn,
                            preferred_element_type=F32)
        block[:, :, part] = y.reshape(cols, y.shape[0] // cols, CHUNK).astype(BF)

    blocks = xy_copies(block, home, xs, xr)
    for copy in blocks:
        copy.start()
    home[me] = block[me]
    sums_of(0)
    for t, q, up in hops:
        if fresh_of(t, q, up) and t == 1 and not up:
            hop(t, q, up, True).start()
    serve(0)
    serve(1)
    for copy in blocks:
        copy.wait_recv()

    @pl.loop(0, near // CHUNK)
    def _(i):
        part = pl.ds(pl.multiple_of(i * CHUNK, CHUNK), CHUNK)
        h = home[:, :, part].astype(F32).reshape(mine_ref.shape[0], CHUNK).astype(BF)
        away[:, part] = lax.dot_general(theirs_ref[...], h, turn, preferred_element_type=F32).astype(BF)
        own[:, part] = lax.dot_general(mine_ref[...], h, turn, preferred_element_type=F32)

    first, second = pair_steps(away, relay, got, ps, pr)
    for copy in first:
        copy.start()
    serve(2)
    for d in range(2):
        first[d].wait_recv()
        second[d].start()
    serve(3)
    for q in range(4):
        r, c = sub(q, rows, width)
        there = out_ref.at[sub(q, rows, width, near)]
        add_into(there, part_ref.at[z, r, c], ub.at[last - 1, q], wide, db.at[last - 1, q])
    for copy in second:
        copy.wait_recv()
    add_into(out_ref.at[:, pl.ds(0, near)], own, got, near)
    for t, q, up in hops:
        hop(t, q, up, fresh_of(t, q, up)).wait_send()
    for copy in first + second + blocks + fars[0] + fars[1]:
        copy.wait_send()


def back(lines, fars, mine, theirs, pick2, fit1, cid):
    experts, _, cap, near = lines.shape
    width = fars.shape[2]
    rows = mine.shape[1]
    block = (COLS, mine.shape[0] // COLS, near)
    buf = pltpu.VMEM((NZ // 2, 4, rows // 2, width // 2), BF)
    line = pltpu.VMEM((NL - 1, experts, cap, near), BF)
    plane = DMA((COLS - 1,))
    return pl.pallas_call(
        back_kernel,
        out_shape=jax.ShapeDtypeStruct((rows, near + width), BF),
        in_specs=[VMEM, ANY, VMEM, VMEM, VMEM, VMEM], out_specs=VMEM,
        scratch_shapes=[line, line, pltpu.VMEM((experts, cap, near), BF), pltpu.VMEM(fars.shape, BF),
                        pltpu.VMEM((NZ, rows, width), BF), pltpu.VMEM(block, BF), pltpu.VMEM(block, BF),
                        pltpu.VMEM((rows, near), BF), pltpu.VMEM((rows, near), F32), pltpu.VMEM((rows, near), BF),
                        pltpu.VMEM((2, rows // 2, near), BF), buf, buf] + [plane] * 6
        + [DMA((NZ // 2, 4))] * 4 + [DMA((4,))] * 2 + [DMA((NL - 1, experts))] * 4 + [DMA],
        compiler_params=pltpu.CompilerParams(collective_id=cid, has_side_effects=True),
        name="back",
    )(lines, fars, mine, theirs, pick2, fit1)


def hidden_kernel(x1_ref, got_ref, fit_ref, g0_ref, g1_ref, u0_ref, u1_ref, h_ref, acc):
    d = pl.program_id(0)
    experts, rows, half = h_ref.shape

    @pl.when(d == 0)
    def _():
        acc[...] = jnp.zeros(acc.shape, F32)

    def add(e, x):
        both = jnp.concatenate([g0_ref[e], g1_ref[e], u0_ref[e], u1_ref[e]], axis=1)
        acc[e] += jnp.dot(x, both, preferred_element_type=F32)

    @pl.when(d < NEAR)
    def _():
        for e in range(experts):
            add(e, x1_ref[e])

    @pl.when(d >= NEAR)
    def _():
        for e in range(experts):
            fit = fit_ref[e * rows:(e + 1) * rows, :]
            add(e, jnp.dot(fit, got_ref[...], preferred_element_type=F32).astype(BF))

    @pl.when(d == pl.num_programs(0) - 1)
    def _():
        for e in range(experts):
            gate, up = acc[e, :, :half], acc[e, :, half:]
            h_ref[e] = (gate / (1.0 + jnp.exp(-gate)) * up).astype(BF)


def hidden_of(x1, got2, fit2, g0, g1, u0, u1):
    experts, rows, _ = x1.shape
    width, cols = g0.shape[1], g0.shape[2]
    weight = pl.BlockSpec((experts, CHUNK, cols), lambda d: (0, d, 0))
    return pl.pallas_call(
        hidden_kernel,
        grid=(width // CHUNK,),
        out_shape=jax.ShapeDtypeStruct((experts, rows, 2 * cols), BF),
        in_specs=[
            pl.BlockSpec((experts, rows, CHUNK), lambda d: (0, 0, jnp.minimum(d, NEAR - 1))),
            pl.BlockSpec((got2.shape[0], CHUNK), lambda d: (0, jnp.maximum(d - NEAR, 0))),
            pl.BlockSpec(fit2.shape, lambda d: (0, 0)),
            weight, weight, weight, weight],
        out_specs=pl.BlockSpec((experts, rows, 2 * cols), lambda d: (0, 0, 0)),
        scratch_shapes=[pltpu.VMEM((experts, rows, 4 * cols), F32)],
        compiler_params=pltpu.CompilerParams(dimension_semantics=("arbitrary",)),
        name="hidden_units",
    )(x1, got2, fit2, g0, g1, u0, u1)


def down_kernel(h_ref, fit_ref, wt_ref, d0_ref, d1_ref, near_ref, far_ref, padded, scale):
    d = pl.program_id(0)
    experts, rows, units = h_ref.shape
    turn = (((0,), (0,)), ((), ()))

    @pl.when(d == 0)
    def _():
        scale[...] = jnp.zeros(scale.shape, F32)
        for e in range(experts):
            fit = fit_ref[e * rows:(e + 1) * rows, :]
            placed = lax.dot_general(fit, h_ref[e], turn, preferred_element_type=F32)
            padded[:, e * units:(e + 1) * units] = placed.astype(BF)
            wide = jnp.broadcast_to(wt_ref[e], (rows, scale.shape[1]))
            scale[...] += lax.dot_general(fit.astype(F32), wide, turn, precision=lax.Precision.HIGHEST,
                                          preferred_element_type=F32)

    @pl.when(d < NEAR)
    def _():
        for e in range(experts):
            both = jnp.concatenate([d0_ref[e], d1_ref[e]], axis=0)
            y = jnp.dot(h_ref[e], both, preferred_element_type=F32)
            near_ref[e] = (y * wt_ref[e]).astype(BF)

    @pl.when(d >= NEAR)
    def _():
        both = jnp.concatenate([ref[e] for e in range(experts) for ref in (d0_ref, d1_ref)], axis=0)
        y = jnp.dot(padded[...], both, preferred_element_type=F32)
        far_ref[...] = (y * scale[:, :1]).astype(BF)


def down_of(hidden, fit2, weight, d0, d1):
    experts, rows, units = hidden.shape
    cols, width = d0.shape[1], d0.shape[2]
    slots = fit2.shape[1]
    mat = pl.BlockSpec((experts, cols, CHUNK), lambda d: (0, 0, d))
    return pl.pallas_call(
        down_kernel,
        grid=(width // CHUNK,),
        out_shape=(jax.ShapeDtypeStruct((experts, rows, D1), BF), jax.ShapeDtypeStruct((slots, width - D1), BF)),
        in_specs=[
            pl.BlockSpec(hidden.shape, lambda d: (0, 0, 0)),
            pl.BlockSpec(fit2.shape, lambda d: (0, 0)),
            pl.BlockSpec((experts, rows, 1), lambda d: (0, 0, 0)),
            mat, mat],
        out_specs=(
            pl.BlockSpec((experts, rows, CHUNK), lambda d: (0, 0, jnp.minimum(d, NEAR - 1))),
            pl.BlockSpec((slots, CHUNK), lambda d: (0, jnp.maximum(d - NEAR, 0)))),
        scratch_shapes=[pltpu.VMEM((slots, experts * units), BF), pltpu.VMEM((slots, 128), F32)],
        compiler_params=pltpu.CompilerParams(dimension_semantics=("arbitrary",)),
        name="down_units",
    )(hidden, fit2, weight, d0, d1)


def iota(shape, dim):
    return lax.broadcasted_iota(jnp.int32, shape, dim)


def ones_of(mask):
    return jnp.where(mask, 1.0, 0.0).astype(BF)


def over(a, n):
    return a >> (n.bit_length() - 1)


def rest(a, n):
    return a & (n - 1)


def table_kernel(seat_ref, dispatch_ref, gates_ref, mine_ref, theirs_ref, pick_ref, fit1_ref, fit2_ref, wt_ref):
    col, zh, zl, c = seat_ref[0], seat_ref[1], seat_ref[2], seat_ref[3]
    experts = wt_ref.shape[0]
    total, cap = dispatch_ref.shape[1], dispatch_ref.shape[2]
    lanes = COLS * experts
    span = pick_ref.shape[2]
    rows = span // NH
    turn = (((0,), (0,)), ((), ()))
    level = (((1,), (1,)), ((), ()))

    who, lane = iota((total, lanes), 0), iota((total, lanes), 1)
    chosen = ones_of(who == over(lane, experts) * (NH * experts) + zh * experts + rest(lane, experts))
    blocks, offsets, weights = [], [], []
    for k in range(NL):
        v = dispatch_ref[NC * k + c]
        for out, part in ((blocks, over(v, span)), (offsets, rest(v, span))):
            out.append(lax.dot_general(part.astype(F32).astype(BF), chosen, turn, preferred_element_type=F32))
        weights.append(lax.dot_general(gates_ref[NC * k + c], chosen.astype(F32), turn,
                                       precision=lax.Precision.HIGHEST, preferred_element_type=F32))
    block = jnp.concatenate(blocks, axis=1)
    offset = jnp.concatenate(offsets, axis=1)
    weight = jnp.concatenate(weights, axis=1)
    row = iota(block.shape, 0)
    place = jnp.zeros(block.shape, F32)
    for first in range(cap - 1):
        place = place + jnp.where((block == block[first:first + 1, :]) & (row > first), 1.0, 0.0)

    here = jnp.where(block == col.astype(F32), offset * SLOTS + place, -1.0)
    width = NL * lanes
    slots = width * SLOTS
    wide_row = iota((span, width), 0).astype(F32)
    per_k = experts * SLOTS
    near, source = iota((lanes * SLOTS, width), 0), iota((lanes * SLOTS, width), 1)
    lead = near - source * SLOTS
    picked = [jnp.zeros((lanes * SLOTS, span), F32) for _ in range(NL)]
    for w in range(SLOTS):
        found = jnp.zeros((span, width), F32)
        for i in range(cap):
            found = found + jnp.where(here[i:i + 1, :] == wide_row * SLOTS + w, 1.0, 0.0)
        found = found.astype(BF)
        for p in range(NL):
            at = lead + rest(zl + p + 1, NL) * (lanes * SLOTS)
            picked[p] = picked[p] + lax.dot_general(ones_of(at == w), found, level, preferred_element_type=F32)
    for p in range(NL):
        pick_ref[p] = picked[p].astype(BF)
    nearby = picked[NL - 1].astype(BF)
    r, o = iota((span, rows), 0), iota((span, rows), 1)
    mine_ref[...] = jnp.dot(nearby, ones_of(r == zh * rows + o), preferred_element_type=F32).astype(BF)
    theirs_ref[...] = jnp.dot(nearby, ones_of(r == (NH - 1 - zh) * rows + o), preferred_element_type=F32).astype(BF)

    def column(a, k, e):
        at = iota((cap, width), 1) == k * lanes + col * experts + e
        return jnp.sum(jnp.where(at, a, 0.0), axis=1, keepdims=True)

    key = block * SLOTS + place
    m = iota((1, slots), 1)
    m_key = (over(m, NL * per_k) * SLOTS + rest(m, SLOTS)).astype(F32)
    n = iota((1, lanes * SLOTS), 1)
    n_key = (over(n, per_k) * SLOTS + rest(n, SLOTS)).astype(F32)
    for e in range(experts):
        for k in range(NL):
            at = (e * NL + k) * cap
            ours = (rest(over(m, per_k) + zl + 1, NL) == k) & (rest(over(m, SLOTS), experts) == e)
            fit2_ref[at:at + cap, :] = ones_of(column(key, k, e) == jnp.where(ours, m_key, -1.0))
            wt_ref[e, k * cap:(k + 1) * cap, :] = column(weight, k, e)
        ours = rest(over(n, SLOTS), experts) == e
        fit1_ref[e * cap:(e + 1) * cap, :] = ones_of(column(key, zl, e) == jnp.where(ours, n_key, -1.0))


def tables(seat, dispatch, gates, rows, experts):
    cap = dispatch.shape[2]
    small = COLS * experts * SLOTS
    shapes = [(small, rows), (small, rows), (NL, small, NH * rows), (experts * cap, small),
              (experts * NL * cap, NL * small)]
    return pl.pallas_call(
        table_kernel,
        out_shape=tuple(jax.ShapeDtypeStruct(shape, BF) for shape in shapes)
        + (jax.ShapeDtypeStruct((experts, NL * cap, 1), F32),),
        in_specs=[pl.BlockSpec(memory_space=pltpu.SMEM), VMEM, VMEM],
        out_specs=(VMEM,) * 6,
        name="tables",
    )(seat, dispatch, gates)


def body(tokens, w_gate, w_up, w_down, gates, dispatch):
    rows, width = tokens.shape
    experts = w_gate.shape[0]
    cap = dispatch.shape[-1]
    col = lax.axis_index("x") * NY + lax.axis_index("y")
    seat = jnp.stack([col, lax.axis_index("zh"), lax.axis_index("zl"), lax.axis_index("c")]).astype(jnp.int32)
    mine, theirs, pick2, fit1, fit2, weight = tables(seat, dispatch, gates, rows, experts)
    lines, got2, og, ou, od = front(tokens, mine, theirs, pick2, fit1, w_gate, w_up, w_down, 1)
    x1 = lines.reshape(experts, NL * cap, D1)
    hidden = hidden_of(x1, got2.reshape(-1, width - D1), fit2, w_gate, og, w_up, ou)
    back1, back2 = down_of(hidden, fit2, weight, w_down, od)
    back1 = back1.reshape(experts, NL, cap, D1)
    back2 = back2.reshape(COLS, NL * experts * SLOTS, width - D1)
    return back(back1, back2, mine, theirs, pick2, fit1, 2)


def solution(mesh):
    split = Mesh(mesh.devices.reshape(NX, NY, NH, NL, NC), ("x", "y", "zh", "zl", "c"))
    expert, tok = ("x", "y", "zh"), ("zl", "c")
    in_specs = (P(tok + expert, None), P(expert, None, tok), P(expert, None, tok), P(expert, tok, None), P(), P())
    return jax.shard_map(body, mesh=split, in_specs=in_specs, out_specs=P(tok + expert, None), check_vma=False)
```

```python
import jax
import jax.numpy as jnp
from jax import lax
from jax.experimental import pallas as pl
from jax.experimental.pallas import tpu as pltpu
from jax.sharding import Mesh
from jax.sharding import PartitionSpec as P

NX, NY, NH, NL, NC = 4, 4, 2, 4, 2
NZ = NH * NL
COLS = NX * NY
D1 = 4096
SLOTS = 4
CHUNK = 1024
HALF = 512
NEAR = D1 // CHUNK
XY_ORDER = ((2, 2), (1, 1), (3, 3), (1, 3), (3, 1), (2, 1), (1, 2), (2, 3), (3, 2), (2, 0), (0, 2), (1, 0), (3, 0), (0, 1), (0, 3))
BF = jnp.bfloat16
F32 = jnp.float32
ANY = pl.BlockSpec(memory_space=pl.ANY)
VMEM = pl.BlockSpec(memory_space=pltpu.VMEM)
DMA = pltpu.SemaphoreType.DMA


def z_of(z):
    z = lax.rem(z + NZ, NZ)
    return {"zh": lax.div(z, NL), "zl": lax.rem(z, NL)}


def remote(src, dst, send, recv, device):
    return pltpu.make_async_remote_copy(
        src_ref=src, dst_ref=dst, send_sem=send, recv_sem=recv,
        device_id=device, device_id_type=pl.DeviceIdType.MESH)


def greet(devices):
    barrier = pltpu.get_barrier_semaphore()
    for device in devices:
        pl.semaphore_signal(barrier, inc=1, device_id=device, device_id_type=pl.DeviceIdType.MESH)
    pl.semaphore_wait(barrier, len(devices))


def xy_targets():
    x, y = lax.axis_index("x"), lax.axis_index("y")
    return [(lax.rem(x + dx, NX), lax.rem(y + dy, NY)) for dx, dy in XY_ORDER]


def xy_devices():
    return [{"x": tx, "y": ty} for tx, ty in xy_targets()]


def xy_copies(src, dst, send, recv, first=0, count=None):
    me = lax.axis_index("x") * NY + lax.axis_index("y")
    part = pl.ds(first, src.shape[1] if count is None else count)
    return [
        remote(src.at[tx * NY + ty, part], dst.at[me, part], send.at[d], recv.at[d], {"x": tx, "y": ty})
        for d, (tx, ty) in enumerate(xy_targets())
    ]


def my_z():
    return lax.axis_index("zh") * NL + lax.axis_index("zl")


def pair_steps(src, relay, dst, send, recv):
    z = my_z()
    half = relay.shape[1]
    first, second = [], []
    for d, step in enumerate((2, -2)):
        part = pl.ds(d * half, half)
        near = z_of(z + step)
        first.append(remote(src.at[part, pl.ds(0, relay.shape[2])], relay.at[d], send.at[d], recv.at[d], near))
        second.append(remote(relay.at[d], dst.at[part], send.at[2 + d], recv.at[2 + d], near))
    return first, second


def sub(q, rows, width, first=0):
    half, wide = rows // 2, width // 2
    return pl.ds(q // 2 * half, half), pl.ds(first + q % 2 * wide, wide)


RING_HOPS = [(t, q, up) for t in range(NZ // 2) for q in range(4) for up in (True, False)]


def front_kernel(tok_ref, mine_ref, theirs_ref, pick_ref, fit_ref, wg_ref, wu_ref, wd_ref,
                 line_ref, got_ref, og_ref, ou_ref, od_ref,
                 ring, other, relay, block, home, far,
                 xs, xr, ys, yr, vs, vr, us, ur, ds, dr, ps, pr, lus, lur, lds, ldr, ws, wr, ls):
    z = my_z()
    zl = lax.axis_index("zl")
    experts = line_ref.shape[0]
    _, rows, width = ring.shape
    cols, wide = block.shape[0], block.shape[2]
    start_col = tok_ref.shape[1] - width
    core = {"c": 1 - lax.axis_index("c")}
    greet(xy_devices() + [z_of(z + 1), z_of(z - 1), z_of(z + 2), z_of(z - 2), core])
    me = lax.axis_index("x") * NY + lax.axis_index("y")
    last = NZ // 2 - 1

    def hop(t, q, up):
        who = lax.rem(z + (-t if up else t) + NZ, NZ)
        r, c = sub(q, rows, width)
        src = tok_ref.at[sub(q, rows, width, start_col)] if t == 0 else ring.at[who, r, c]
        send, recv = (us, ur) if up else (ds, dr)
        return remote(src, ring.at[who, r, c], send.at[t, q], recv.at[t, q], z_of(z + (1 if up else -1)))

    hops = [(t, q, up) for t, q, up in RING_HOPS if t < last or (q < 2) == up]

    def serve(step):
        for t, q, up in hops:
            if t == step:
                hop(t, q, up).wait_recv()
                if (t + 1, q, up) in hops:
                    hop(t + 1, q, up).start()

    def pass_on(i, e, up):
        who = lax.rem(zl + (-i if up else i) + NL, NL)
        send, recv = (lus, lur) if up else (lds, ldr)
        place = line_ref.at[e, who]
        return remote(place, place, send.at[i, e], recv.at[i, e], z_of(z + (1 if up else -1)))

    def sends(i, up):
        return (zl < NL - 1) & (zl >= i) if up else (zl > 0) & (zl + i < NL)

    def gets(i, up):
        return zl - 1 - i >= 0 if up else zl + 1 + i < NL

    first, second = pair_steps(tok_ref, relay, other, ps, pr)
    for copy in first:
        copy.start()
    for t, q, up in hops:
        if t == 0:
            hop(t, q, up).start()
    weights = [remote(a, b, ws.at[i], wr.at[i], core)
               for i, (a, b) in enumerate(((wg_ref, og_ref), (wu_ref, ou_ref), (wd_ref, od_ref)))]
    for copy in weights:
        copy.start()
    ring[z] = tok_ref[:, start_col:]
    for d in range(2):
        first[d].wait_recv()
        second[d].start()
    serve(0)
    for copy in second:
        copy.wait_recv()

    @pl.loop(0, wide // CHUNK)
    def _(i):
        part = pl.ds(pl.multiple_of(i * CHUNK, CHUNK), CHUNK)
        y = jnp.dot(mine_ref[...], tok_ref[:, part], preferred_element_type=F32)
        y = y + jnp.dot(theirs_ref[...], other[:, part], preferred_element_type=F32)
        block[:, :, part] = y.reshape(cols, y.shape[0] // cols, CHUNK).astype(BF)

    blocks = xy_copies(block, home, xs, xr)
    for copy in blocks:
        copy.start()
    home[me] = block[me]
    fars = []

    def far_part(h, send, recv):
        count = far.shape[1] // 2

        @pl.loop(0, width // HALF)
        def _(i):
            part = pl.ds(pl.multiple_of(i * HALF, HALF), HALF)
            found = []
            for p in (2 * h, 2 * h + 1):
                k = lax.rem(zl + p + 1, NL)
                both = jnp.concatenate([ring[k, :, part], ring[k + NL, :, part]], axis=0)
                y = jnp.dot(pick_ref[p], both, preferred_element_type=F32)
                found.append(y.reshape(cols, count // 2, HALF))
            far[:, h * count:(h + 1) * count, part] = jnp.concatenate(found, axis=1).astype(BF)

        copies = xy_copies(far, got_ref, send, recv, h * count, count)
        for copy in copies:
            copy.start()
        fars.extend(copies)

    serve(1)
    serve(2)
    far_part(0, ys, yr)
    for copy in blocks:
        copy.wait_recv()

    @pl.loop(0, wide // CHUNK)
    def _(i):
        part = pl.ds(pl.multiple_of(i * CHUNK, CHUNK), CHUNK)
        h = home[:, :, part].astype(F32).reshape(fit_ref.shape[1], CHUNK).astype(BF)
        y = jnp.dot(fit_ref[...], h, preferred_element_type=F32).astype(BF)
        cap = y.shape[0] // experts
        for e in range(experts):
            line_ref[e, zl, :, part] = y[e * cap:(e + 1) * cap]

    for e in range(experts):
        for up in (True, False):
            @pl.when(sends(0, up))
            def _():
                pass_on(0, e, up).start()

    serve(3)
    far_part(1, vs, vr)
    own = pltpu.make_async_copy(far.at[me], got_ref.at[me], ls)
    own.start()
    for i in range(NL - 1):
        for e in range(experts):
            for up in (True, False):
                @pl.when(gets(i, up))
                def _():
                    pass_on(i, e, up).wait_recv()
                if i < NL - 2:
                    @pl.when(sends(i + 1, up))
                    def _():
                        pass_on(i + 1, e, up).start()
    for i in range(NL - 1):
        for e in range(experts):
            for up in (True, False):
                @pl.when(sends(i, up))
                def _():
                    pass_on(i, e, up).wait_send()
    for t, q, up in hops:
        hop(t, q, up).wait_send()
    for copy in first + second + blocks:
        copy.wait_send()
    for copy in fars + weights:
        copy.wait()
    own.wait()


def front(tokens, mine, theirs, pick2, fit1, w_gate, w_up, w_down, cid):
    rows = tokens.shape[0]
    width = tokens.shape[1] - D1
    experts = w_gate.shape[0]
    cap = fit1.shape[0] // experts
    block = (COLS, mine.shape[0] // COLS, D1)
    far = (COLS, NL * pick2.shape[1] // COLS, width)
    shapes = [(experts, NL, cap, D1), far, w_gate.shape, w_up.shape, w_down.shape]
    plane = DMA((COLS - 1,))
    return pl.pallas_call(
        front_kernel,
        out_shape=tuple(jax.ShapeDtypeStruct(shape, BF) for shape in shapes),
        in_specs=[VMEM] * 5 + [ANY] * 3, out_specs=(VMEM, ANY, ANY, ANY, ANY),
        scratch_shapes=[pltpu.VMEM((NZ, rows, width), BF), pltpu.VMEM((rows, D1), BF),
                        pltpu.VMEM((2, rows // 2, D1), BF), pltpu.VMEM(block, BF), pltpu.VMEM(block, BF),
                        pltpu.VMEM(far, BF)] + [plane] * 6
        + [DMA((NZ // 2, 4))] * 4 + [DMA((4,))] * 2 + [DMA((NL - 1, experts))] * 4 + [DMA((3,))] * 2 + [DMA],
        compiler_params=pltpu.CompilerParams(collective_id=cid, has_side_effects=True),
        name="front",
    )(tokens, mine, theirs, pick2, fit1, w_gate, w_up, w_down)


def add_into(dst, a, b, width, extra=None, chunk=512):
    @pl.loop(0, width // chunk)
    def _(i):
        part = pl.ds(pl.multiple_of(i * chunk, chunk), chunk)
        total = a[:, part].astype(F32) + b[:, part].astype(F32)
        if extra is not None:
            total = total + extra[:, part].astype(F32)
        dst[:, part] = total.astype(BF)


def back_kernel(line_ref, far_ref, mine_ref, theirs_ref, pick_ref, fit_ref, out_ref,
                lu, ld, summed, got2, part_ref, block, home, away, own, got, relay, ub, db,
                xs, xr, ys, yr, vs, vr, us, ur, ds, dr, ps, pr, lus, lur, lds, ldr, ls):
    z = my_z()
    zl = lax.axis_index("zl")
    experts = line_ref.shape[0]
    near = line_ref.shape[3]
    _, rows, width = part_ref.shape
    wide = width // 2
    cols = block.shape[0]
    me = lax.axis_index("x") * NY + lax.axis_index("y")
    greet(xy_devices() + [z_of(z + 1), z_of(z - 1), z_of(z + 2), z_of(z - 2)])
    last = NZ // 2
    turn = (((0,), (0,)), ((), ()))

    def send_sum(j, e, up, fresh):
        buf = lu if up else ld
        slot = j - 1 if up else j
        send, recv = (lus, lur) if up else (lds, ldr)
        src = line_ref.at[e, j] if fresh else buf.at[slot, e]
        return remote(src, buf.at[slot, e], send.at[slot, e], recv.at[slot, e], z_of(z + (1 if up else -1)))

    order = [(NL - 1 - i, i) for i in range(NL - 1)]
    count = got2.shape[1] // 2
    fars = [xy_copies(far_ref, got2, ys, yr, 0, count), xy_copies(far_ref, got2, vs, vr, count, count)]
    for copy in fars[1] + fars[0]:
        copy.start()
    keep = pltpu.make_async_copy(far_ref.at[me], got2.at[me], ls)
    keep.start()
    edge = [(i, e) for i in range(NL - 1) for e in range(experts)]
    for up, seat in ((True, 0), (False, NL - 1)):
        @pl.when(zl == seat)
        def _():
            copies = [send_sum(NL - 1 - i if up else i, e, up, True) for i, e in edge]
            copies[0].start()
            copies[1].start()
            for n in range(2, len(copies)):
                copies[n - 2].wait_send()
                copies[n].start()
            copies[-2].wait_send()
            copies[-1].wait_send()

    def pass_on(j, e, up):
        slot = j - 1 if up else j
        buf = lu if up else ld
        copy = send_sum(j, e, up, False)
        copy.wait_recv()
        add_into(buf.at[slot, e], buf.at[slot, e], line_ref.at[e, j], near)
        copy.start()

    for seat, up in ((1, True), (2, False)):
        end, inner, start = (3, 2, 0) if up else (0, 1, 3)
        events = [(end, 0, up), (end, 1, up), (start, 0, not up), (inner, 0, up), (start, 1, not up), (inner, 1, up)]

        @pl.when(zl == seat)
        def _():
            for event in events:
                pass_on(*event)
            for j, e, up in events:
                send_sum(j, e, up, False).wait_send()
    def spot(t, up):
        return lax.rem(z + (last - t if up else t - last) + NZ, NZ)

    def hop(t, q, up, fresh):
        buf = ub if up else db
        send, recv = (us, ur) if up else (ds, dr)
        src = part_ref.at[(spot(t, up),) + sub(q, rows, width)] if fresh else buf.at[t - 1, q]
        return remote(src, buf.at[t, q], send.at[t, q], recv.at[t, q], z_of(z + (1 if up else -1)))

    def fresh_of(t, q, up):
        return t == 0 or (t == 1 and (q < 2) != up)

    hops = [(t, q, up) for t, q, up in RING_HOPS if t > 0 or (q < 2) == up]

    def serve(step):
        for t, q, up in hops:
            if t == step:
                buf = ub if up else db
                hop(t, q, up, fresh_of(t, q, up)).wait_recv()
                if t < last - 1:
                    add_into(buf.at[t, q], buf.at[t, q], part_ref.at[(spot(t + 1, up),) + sub(q, rows, width)], wide)
                    hop(t + 1, q, up, False).start()

    def sums_of(h):
        for copy in fars[h]:
            copy.wait_recv()

        @pl.loop(0, width // HALF)
        def _(i):
            part = pl.ds(pl.multiple_of(i * HALF, HALF), HALF)
            whole = got2[:, h * count:(h + 1) * count, part].astype(F32)
            for p in (0, 1):
                each = whole[:, p * (count // 2):(p + 1) * (count // 2)].reshape(pick_ref.shape[1], HALF).astype(BF)
                y = lax.dot_general(pick_ref[2 * h + p], each, turn, preferred_element_type=F32).astype(BF)
                k = lax.rem(zl + 2 * h + p + 1, NL)
                part_ref[k, :, part] = y[:rows]
                part_ref[k + NL, :, part] = y[rows:]

    keep.wait()
    sums_of(1)
    for t, q, up in hops:
        if fresh_of(t, q, up) and (t == 0 or up):
            hop(t, q, up, True).start()
    for ju, jd in order:
        for e in range(experts):
            @pl.when(zl == ju)
            def _():
                send_sum(ju, e, True, False).wait_recv()

            @pl.when(zl == jd)
            def _():
                send_sum(jd, e, False, False).wait_recv()
    for e in range(experts):
        @pl.when(zl == 0)
        def _():
            add_into(summed.at[e], line_ref.at[e, 0], ld.at[0, e], near)

        @pl.when(zl == NL - 1)
        def _():
            add_into(summed.at[e], line_ref.at[e, NL - 1], lu.at[NL - 2, e], near)
        for mid in range(1, NL - 1):
            @pl.when(zl == mid)
            def _():
                add_into(summed.at[e], line_ref.at[e, mid], lu.at[mid - 1, e], near, ld.at[mid, e])

    @pl.loop(0, near // CHUNK)
    def _(i):
        part = pl.ds(pl.multiple_of(i * CHUNK, CHUNK), CHUNK)
        y = lax.dot_general(fit_ref[...], summed[:, :, part].reshape(fit_ref.shape[0], CHUNK), turn,
                            preferred_element_type=F32)
        block[:, :, part] = y.reshape(cols, y.shape[0] // cols, CHUNK).astype(BF)

    blocks = xy_copies(block, home, xs, xr)
    for copy in blocks:
        copy.start()
    home[me] = block[me]
    sums_of(0)
    for t, q, up in hops:
        if fresh_of(t, q, up) and t == 1 and not up:
            hop(t, q, up, True).start()
    serve(0)
    serve(1)
    for copy in blocks:
        copy.wait_recv()

    @pl.loop(0, near // CHUNK)
    def _(i):
        part = pl.ds(pl.multiple_of(i * CHUNK, CHUNK), CHUNK)
        h = home[:, :, part].astype(F32).reshape(mine_ref.shape[0], CHUNK).astype(BF)
        away[:, part] = lax.dot_general(theirs_ref[...], h, turn, preferred_element_type=F32).astype(BF)
        own[:, part] = lax.dot_general(mine_ref[...], h, turn, preferred_element_type=F32)

    first, second = pair_steps(away, relay, got, ps, pr)
    for copy in first:
        copy.start()
    serve(2)
    for d in range(2):
        first[d].wait_recv()
        second[d].start()
    serve(3)
    for q in range(4):
        r, c = sub(q, rows, width)
        there = out_ref.at[sub(q, rows, width, near)]
        add_into(there, part_ref.at[z, r, c], ub.at[last - 1, q], wide, db.at[last - 1, q])
    for copy in second:
        copy.wait_recv()
    add_into(out_ref.at[:, pl.ds(0, near)], own, got, near)
    for t, q, up in hops:
        hop(t, q, up, fresh_of(t, q, up)).wait_send()
    for copy in first + second + blocks + fars[0] + fars[1]:
        copy.wait_send()


def back(lines, fars, mine, theirs, pick2, fit1, cid):
    experts, _, cap, near = lines.shape
    width = fars.shape[2]
    rows = mine.shape[1]
    block = (COLS, mine.shape[0] // COLS, near)
    buf = pltpu.VMEM((NZ // 2, 4, rows // 2, width // 2), BF)
    line = pltpu.VMEM((NL - 1, experts, cap, near), BF)
    plane = DMA((COLS - 1,))
    return pl.pallas_call(
        back_kernel,
        out_shape=jax.ShapeDtypeStruct((rows, near + width), BF),
        in_specs=[VMEM, ANY, VMEM, VMEM, VMEM, VMEM], out_specs=VMEM,
        scratch_shapes=[line, line, pltpu.VMEM((experts, cap, near), BF), pltpu.VMEM(fars.shape, BF),
                        pltpu.VMEM((NZ, rows, width), BF), pltpu.VMEM(block, BF), pltpu.VMEM(block, BF),
                        pltpu.VMEM((rows, near), BF), pltpu.VMEM((rows, near), F32), pltpu.VMEM((rows, near), BF),
                        pltpu.VMEM((2, rows // 2, near), BF), buf, buf] + [plane] * 6
        + [DMA((NZ // 2, 4))] * 4 + [DMA((4,))] * 2 + [DMA((NL - 1, experts))] * 4 + [DMA],
        compiler_params=pltpu.CompilerParams(collective_id=cid, has_side_effects=True),
        name="back",
    )(lines, fars, mine, theirs, pick2, fit1)


def hidden_kernel(x1_ref, got_ref, fit_ref, g0_ref, g1_ref, u0_ref, u1_ref, h_ref, acc):
    d = pl.program_id(0)
    experts, rows, half = h_ref.shape

    @pl.when(d == 0)
    def _():
        acc[...] = jnp.zeros(acc.shape, F32)

    def add(e, x):
        both = jnp.concatenate([g0_ref[e], g1_ref[e], u0_ref[e], u1_ref[e]], axis=1)
        acc[e] += jnp.dot(x, both, preferred_element_type=F32)

    @pl.when(d < NEAR)
    def _():
        for e in range(experts):
            add(e, x1_ref[e])

    @pl.when(d >= NEAR)
    def _():
        for e in range(experts):
            fit = fit_ref[e * rows:(e + 1) * rows, :]
            add(e, jnp.dot(fit, got_ref[...], preferred_element_type=F32).astype(BF))

    @pl.when(d == pl.num_programs(0) - 1)
    def _():
        for e in range(experts):
            gate, up = acc[e, :, :half], acc[e, :, half:]
            h_ref[e] = (gate / (1.0 + jnp.exp(-gate)) * up).astype(BF)


def hidden_of(x1, got2, fit2, g0, g1, u0, u1):
    experts, rows, _ = x1.shape
    width, cols = g0.shape[1], g0.shape[2]
    weight = pl.BlockSpec((experts, CHUNK, cols), lambda d: (0, d, 0))
    return pl.pallas_call(
        hidden_kernel,
        grid=(width // CHUNK,),
        out_shape=jax.ShapeDtypeStruct((experts, rows, 2 * cols), BF),
        in_specs=[
            pl.BlockSpec((experts, rows, CHUNK), lambda d: (0, 0, jnp.minimum(d, NEAR - 1))),
            pl.BlockSpec((got2.shape[0], CHUNK), lambda d: (0, jnp.maximum(d - NEAR, 0))),
            pl.BlockSpec(fit2.shape, lambda d: (0, 0)),
            weight, weight, weight, weight],
        out_specs=pl.BlockSpec((experts, rows, 2 * cols), lambda d: (0, 0, 0)),
        scratch_shapes=[pltpu.VMEM((experts, rows, 4 * cols), F32)],
        compiler_params=pltpu.CompilerParams(dimension_semantics=("arbitrary",)),
        name="hidden_units",
    )(x1, got2, fit2, g0, g1, u0, u1)


def down_kernel(h_ref, fit_ref, wt_ref, d0_ref, d1_ref, near_ref, far_ref, padded, scale):
    d = pl.program_id(0)
    experts, rows, units = h_ref.shape
    turn = (((0,), (0,)), ((), ()))

    @pl.when(d == 0)
    def _():
        held = jnp.zeros((1, scale.shape[0]), F32)
        for e in range(experts):
            fit = fit_ref[e * rows:(e + 1) * rows, :]
            placed = lax.dot_general(fit, h_ref[e], turn, preferred_element_type=F32)
            padded[:, e * units:(e + 1) * units] = placed.astype(BF)
            held = held + jnp.sum(fit.astype(F32) * wt_ref[e], axis=0, keepdims=True)
        scale[...] = jnp.broadcast_to(held, scale.shape[::-1]).T

    @pl.when(d < NEAR)
    def _():
        for e in range(experts):
            both = jnp.concatenate([d0_ref[e], d1_ref[e]], axis=0)
            y = jnp.dot(h_ref[e], both, preferred_element_type=F32)
            near_ref[e] = (y * wt_ref[e]).astype(BF)

    @pl.when(d >= NEAR)
    def _():
        both = jnp.concatenate([ref[e] for e in range(experts) for ref in (d0_ref, d1_ref)], axis=0)
        y = jnp.dot(padded[...], both, preferred_element_type=F32)
        far_ref[...] = (y * scale[:, :1]).astype(BF)


def down_of(hidden, fit2, weight, d0, d1):
    experts, rows, units = hidden.shape
    cols, width = d0.shape[1], d0.shape[2]
    slots = fit2.shape[1]
    mat = pl.BlockSpec((experts, cols, CHUNK), lambda d: (0, 0, d))
    return pl.pallas_call(
        down_kernel,
        grid=(width // CHUNK,),
        out_shape=(jax.ShapeDtypeStruct((experts, rows, D1), BF), jax.ShapeDtypeStruct((slots, width - D1), BF)),
        in_specs=[
            pl.BlockSpec(hidden.shape, lambda d: (0, 0, 0)),
            pl.BlockSpec(fit2.shape, lambda d: (0, 0)),
            pl.BlockSpec((experts, rows, 1), lambda d: (0, 0, 0)),
            mat, mat],
        out_specs=(
            pl.BlockSpec((experts, rows, CHUNK), lambda d: (0, 0, jnp.minimum(d, NEAR - 1))),
            pl.BlockSpec((slots, CHUNK), lambda d: (0, jnp.maximum(d - NEAR, 0)))),
        scratch_shapes=[pltpu.VMEM((slots, experts * units), BF), pltpu.VMEM((slots, 128), F32)],
        compiler_params=pltpu.CompilerParams(dimension_semantics=("arbitrary",)),
        name="down_units",
    )(hidden, fit2, weight, d0, d1)


def iota(shape, dim):
    return lax.broadcasted_iota(jnp.int32, shape, dim)


def ones_of(mask):
    return jnp.where(mask, 1.0, 0.0).astype(BF)


def over(a, n):
    return a >> (n.bit_length() - 1)


def rest(a, n):
    return a & (n - 1)


def table_kernel(seat_ref, dispatch_ref, gates_ref, mine_ref, theirs_ref, pick_ref, fit1_ref, fit2_ref, wt_ref):
    col, zh, zl, c = seat_ref[0], seat_ref[1], seat_ref[2], seat_ref[3]
    experts = wt_ref.shape[0]
    total, cap = dispatch_ref.shape[1], dispatch_ref.shape[2]
    lanes = COLS * experts
    span = pick_ref.shape[2]
    rows = span // NH
    turn = (((0,), (0,)), ((), ()))
    level = (((1,), (1,)), ((), ()))

    who, lane = iota((total, lanes), 0), iota((total, lanes), 1)
    chosen = ones_of(who == over(lane, experts) * (NH * experts) + zh * experts + rest(lane, experts))
    blocks, offsets, weights = [], [], []
    for k in range(NL):
        v = dispatch_ref[NC * k + c]
        for out, part in ((blocks, over(v, span)), (offsets, rest(v, span))):
            out.append(lax.dot_general(part.astype(F32).astype(BF), chosen, turn, preferred_element_type=F32))
        weights.append(lax.dot_general(gates_ref[NC * k + c], chosen.astype(F32), turn,
                                       precision=lax.Precision.HIGHEST, preferred_element_type=F32))
    block = jnp.concatenate(blocks, axis=1)
    offset = jnp.concatenate(offsets, axis=1)
    weight = jnp.concatenate(weights, axis=1)
    row = iota(block.shape, 0)
    place = jnp.zeros(block.shape, F32)
    for first in range(cap - 1):
        place = place + jnp.where((block == block[first:first + 1, :]) & (row > first), 1.0, 0.0)

    here = jnp.where(block == col.astype(F32), offset * SLOTS + place, -1.0)
    width = NL * lanes
    slots = width * SLOTS
    wide_row = iota((span, width), 0).astype(F32)
    per_k = experts * SLOTS
    near, source = iota((lanes * SLOTS, width), 0), iota((lanes * SLOTS, width), 1)
    lead = near - source * SLOTS
    picked = [jnp.zeros((lanes * SLOTS, span), F32) for _ in range(NL)]
    for w in range(SLOTS):
        found = jnp.zeros((span, width), F32)
        for i in range(cap):
            found = found + jnp.where(here[i:i + 1, :] == wide_row * SLOTS + w, 1.0, 0.0)
        found = found.astype(BF)
        for p in range(NL):
            at = lead + rest(zl + p + 1, NL) * (lanes * SLOTS)
            picked[p] = picked[p] + lax.dot_general(ones_of(at == w), found, level, preferred_element_type=F32)
    for p in range(NL):
        pick_ref[p] = picked[p].astype(BF)
    nearby = picked[NL - 1].astype(BF)
    r, o = iota((span, rows), 0), iota((span, rows), 1)
    mine_ref[...] = jnp.dot(nearby, ones_of(r == zh * rows + o), preferred_element_type=F32).astype(BF)
    theirs_ref[...] = jnp.dot(nearby, ones_of(r == (NH - 1 - zh) * rows + o), preferred_element_type=F32).astype(BF)

    def column(a, k, e):
        at = iota((cap, width), 1) == k * lanes + col * experts + e
        return jnp.sum(jnp.where(at, a, 0.0), axis=1, keepdims=True)

    key = block * SLOTS + place
    m = iota((1, slots), 1)
    m_key = (over(m, NL * per_k) * SLOTS + rest(m, SLOTS)).astype(F32)
    n = iota((1, lanes * SLOTS), 1)
    n_key = (over(n, per_k) * SLOTS + rest(n, SLOTS)).astype(F32)
    for e in range(experts):
        for k in range(NL):
            at = (e * NL + k) * cap
            ours = (rest(over(m, per_k) + zl + 1, NL) == k) & (rest(over(m, SLOTS), experts) == e)
            fit2_ref[at:at + cap, :] = ones_of(column(key, k, e) == jnp.where(ours, m_key, -1.0))
            wt_ref[e, k * cap:(k + 1) * cap, :] = column(weight, k, e)
        ours = rest(over(n, SLOTS), experts) == e
        fit1_ref[e * cap:(e + 1) * cap, :] = ones_of(column(key, zl, e) == jnp.where(ours, n_key, -1.0))


def tables(seat, dispatch, gates, rows, experts):
    cap = dispatch.shape[2]
    small = COLS * experts * SLOTS
    shapes = [(small, rows), (small, rows), (NL, small, NH * rows), (experts * cap, small),
              (experts * NL * cap, NL * small)]
    return pl.pallas_call(
        table_kernel,
        out_shape=tuple(jax.ShapeDtypeStruct(shape, BF) for shape in shapes)
        + (jax.ShapeDtypeStruct((experts, NL * cap, 1), F32),),
        in_specs=[pl.BlockSpec(memory_space=pltpu.SMEM), VMEM, VMEM],
        out_specs=(VMEM,) * 6,
        name="tables",
    )(seat, dispatch, gates)


def body(tokens, w_gate, w_up, w_down, gates, dispatch):
    rows, width = tokens.shape
    experts = w_gate.shape[0]
    cap = dispatch.shape[-1]
    col = lax.axis_index("x") * NY + lax.axis_index("y")
    seat = jnp.stack([col, lax.axis_index("zh"), lax.axis_index("zl"), lax.axis_index("c")]).astype(jnp.int32)
    mine, theirs, pick2, fit1, fit2, weight = tables(seat, dispatch, gates, rows, experts)
    lines, got2, og, ou, od = front(tokens, mine, theirs, pick2, fit1, w_gate, w_up, w_down, 1)
    x1 = lines.reshape(experts, NL * cap, D1)
    hidden = hidden_of(x1, got2.reshape(-1, width - D1), fit2, w_gate, og, w_up, ou)
    back1, back2 = down_of(hidden, fit2, weight, w_down, od)
    back1 = back1.reshape(experts, NL, cap, D1)
    back2 = back2.reshape(COLS, NL * experts * SLOTS, width - D1)
    return back(back1, back2, mine, theirs, pick2, fit1, 2)


def solution(mesh):
    split = Mesh(mesh.devices.reshape(NX, NY, NH, NL, NC), ("x", "y", "zh", "zl", "c"))
    expert, tok = ("x", "y", "zh"), ("zl", "c")
    in_specs = (P(tok + expert, None), P(expert, None, tok), P(expert, None, tok), P(expert, tok, None), P(), P())
    return jax.shard_map(body, mesh=split, in_specs=in_specs, out_specs=P(tok + expert, None), check_vma=False)
```
